32 devices in a mesh: data: 1 (over z), pp: 4 (over y), ep: 8 (over x, core).
Axes of the slice: x: 4, y: 4, z: 1, core: 2. Of those that a mesh axis runs over, the one named last changes fastest.
The devices are a block of a 4x4x8 slice.
Arguments:
- expert_out: bfloat16 [4, 1, 64, 320, 2048], P(('data', 'pp'), None, 'ep')
- expert_id: int32 [4, 1, 2048, 8], P(('data', 'pp'), None, 'ep')
- slot_id: int32 [4, 1, 2048, 8], P(('data', 'pp'), None, 'ep')
- gate: float32 [4, 1, 2048, 8], P(('data', 'pp'), None, 'ep')
- resid: bfloat16 [4, 1, 2048, 2048], P(('data', 'pp'), None, 'ep')
- owner: int32 [4, 64], P(('data', 'pp'))
- norm_w: float32 [4, 2048], P('pp')
- w_q: bfloat16 [4, 2048, 2048], P('pp')
- w_k: bfloat16 [4, 2048, 2048], P('pp')
- w_v: bfloat16 [4, 2048, 2048], P('pp')
- w_o: bfloat16 [4, 2048, 2048], P('pp')
Outputs:
- output: bfloat16 [4, 1, 2048, 2048], P(('data', 'pp'), None, 'ep')
All inputs are finite; a program needn't handle non-finite values.
Results may differ from the reference program's by a relative error of at most 0.0140715.
Values are sent between devices in bfloat16 or wider.
A program may use at most 768 MiB of HBM per device.

```python
import jax
import jax.numpy as jnp
from jax import lax

STAGES = 4
EP_DEVICES = 8
MICRO = 1
SEQ_DEV = 8
SEQ_LEN = 32
MODEL_DIM = 2048
EXPERTS = 64
TOP_K = 8
HEADS = 16
HEAD_DIM = 128
CAP_DEV = 40

SEQS = EP_DEVICES * SEQ_DEV
TOKENS = SEQS * SEQ_LEN
TOK_DEV = SEQ_DEV * SEQ_LEN
CAPACITY = EP_DEVICES * CAP_DEV
QKV_WIDTH = HEADS * HEAD_DIM
HOT_COUNT = max(1, EXPERTS // 32)
HOT_BIAS = (2000 * TOP_K) // EXPERTS
NORM_EPS = 1e-6


def draw_routing(rng_key):
    key_hot, key_score = jax.random.split(rng_key)
    hot_rank = jax.random.permutation(key_hot, EXPERTS)
    hot_bias = jnp.where(hot_rank < HOT_COUNT, HOT_BIAS, 0)
    rand_score = jax.random.randint(key_score, (STAGES, MICRO, EP_DEVICES, TOK_DEV, EXPERTS), 0, 1000)
    tok_local = jnp.arange(TOK_DEV)[:, None]
    forced = jnp.where((tok_local < CAP_DEV) & (hot_rank[None, :] == 0), 4000, 0)
    full_score = (rand_score + hot_bias + forced) * EXPERTS + jnp.arange(EXPERTS)
    chosen = lax.top_k(full_score, TOP_K)[1].astype(jnp.int32)
    n_flat = TOK_DEV * TOP_K
    flat_ids = chosen.reshape(STAGES, MICRO, EP_DEVICES, n_flat)
    flat_pos = jnp.arange(n_flat)
    sort_order = jnp.argsort(flat_ids * n_flat + flat_pos, axis=-1)
    sorted_ids = jnp.take_along_axis(flat_ids, sort_order, axis=-1)
    prev_ids = jnp.concatenate([jnp.full_like(sorted_ids[..., :1], -1), sorted_ids[..., :-1]], axis=-1)
    group_start = lax.cummax(jnp.where(sorted_ids != prev_ids, flat_pos, 0), axis=3)
    rank_sorted = flat_pos - group_start
    slot_pos = jnp.take_along_axis(rank_sorted, jnp.argsort(sort_order, axis=-1), axis=-1)
    dev_base = (jnp.arange(EP_DEVICES) * CAP_DEV)[:, None]
    slot_all = jnp.where(slot_pos < CAP_DEV, dev_base + slot_pos, -1).astype(jnp.int32)
    return chosen.reshape(STAGES, MICRO, TOKENS, TOP_K), slot_all.reshape(STAGES, MICRO, TOKENS, TOP_K)


def draw_owner(rng_key):
    key_src, key_dst = jax.random.split(rng_key)
    seq_rows = jnp.broadcast_to(jnp.arange(SEQ_DEV), (STAGES, EP_DEVICES, SEQ_DEV))
    local_perm = jax.random.permutation(key_src, seq_rows, axis=2, independent=True)
    global_ids = local_perm + (jnp.arange(EP_DEVICES) * SEQ_DEV)[:, None]
    per_pair = SEQ_DEV // EP_DEVICES
    global_ids = global_ids.reshape(STAGES, EP_DEVICES, EP_DEVICES, per_pair).transpose(0, 2, 1, 3).reshape(STAGES, EP_DEVICES, SEQ_DEV)
    shuffle = jax.random.permutation(key_dst, seq_rows, axis=2, independent=True)
    owned = jnp.take_along_axis(global_ids, shuffle, axis=2)
    return owned.reshape(STAGES, SEQS).astype(jnp.int32)


def setup_inputs(seed: int = 0, part: int = 0) -> dict:
    part_key = jax.random.fold_in(jax.random.key(seed), part)
    keys_data = jax.random.split(part_key, 8)
    keys_weight = jax.random.split(jax.random.key(seed + 1), 6)
    expert_id, slot_id = draw_routing(keys_data[0])
    owner = draw_owner(keys_data[1])
    expert_scale = jnp.exp(0.7 * jax.random.normal(keys_data[2], (STAGES, MICRO, EXPERTS, 1, 1), jnp.float32))
    expert_out = (jax.random.normal(keys_data[3], (STAGES, MICRO, EXPERTS, CAPACITY, MODEL_DIM), jnp.float32) * expert_scale).astype(jnp.bfloat16)
    gate_raw = jnp.exp(1.2 * jax.random.normal(keys_data[4], (STAGES, MICRO, TOKENS, TOP_K), jnp.float32))
    gate_level = 0.5 + jax.random.uniform(keys_data[5], (STAGES, MICRO, TOKENS, 1), jnp.float32)
    gate = gate_raw / jnp.sum(gate_raw, axis=-1, keepdims=True) * gate_level
    resid = jax.random.normal(keys_data[6], (STAGES, MICRO, TOKENS, MODEL_DIM), jnp.float32).astype(jnp.bfloat16)
    norm_w = jax.random.uniform(keys_weight[0], (STAGES, MODEL_DIM), jnp.float32, 0.5, 1.5)
    qk_scale = 1.5 * MODEL_DIM ** -0.5
    w_q = (jax.random.normal(keys_weight[1], (STAGES, MODEL_DIM, QKV_WIDTH), jnp.float32) * qk_scale).astype(jnp.bfloat16)
    w_k = (jax.random.normal(keys_weight[2], (STAGES, MODEL_DIM, QKV_WIDTH), jnp.float32) * qk_scale).astype(jnp.bfloat16)
    w_v = (jax.random.normal(keys_weight[3], (STAGES, MODEL_DIM, QKV_WIDTH), jnp.float32) * MODEL_DIM ** -0.5).astype(jnp.bfloat16)
    w_o = (jax.random.normal(keys_weight[4], (STAGES, QKV_WIDTH, MODEL_DIM), jnp.float32) * QKV_WIDTH ** -0.5).astype(jnp.bfloat16)
    return dict(expert_out=expert_out, expert_id=expert_id, slot_id=slot_id, gate=gate, resid=resid, owner=owner, norm_w=norm_w, w_q=w_q, w_k=w_k, w_v=w_v, w_o=w_o)


def attend_block(y_seq, norm_scale, w_q_stage, w_k_stage, w_v_stage, w_o_stage):
    y_f32 = y_seq.astype(jnp.float32)
    inv_rms = lax.rsqrt(jnp.mean(y_f32 * y_f32, axis=-1, keepdims=True) + NORM_EPS)
    normed = (y_f32 * inv_rms * norm_scale).astype(jnp.bfloat16)
    queries = jnp.dot(normed, w_q_stage, preferred_element_type=jnp.float32).astype(jnp.bfloat16).reshape(SEQ_LEN, HEADS, HEAD_DIM)
    key_vecs = jnp.dot(normed, w_k_stage, preferred_element_type=jnp.float32).astype(jnp.bfloat16).reshape(SEQ_LEN, HEADS, HEAD_DIM)
    values = jnp.dot(normed, w_v_stage, preferred_element_type=jnp.float32).astype(jnp.bfloat16).reshape(SEQ_LEN, HEADS, HEAD_DIM)
    scores = jnp.einsum('qhe,khe->hqk', queries.astype(jnp.float32), key_vecs.astype(jnp.float32)) * HEAD_DIM ** -0.5
    causal = jnp.arange(SEQ_LEN)[:, None] >= jnp.arange(SEQ_LEN)[None, :]
    attn_probs = jax.nn.softmax(jnp.where(causal, scores, -1e30), axis=-1).astype(jnp.bfloat16)
    head_mix = jnp.einsum('hqk,khe->qhe', attn_probs.astype(jnp.float32), values.astype(jnp.float32)).astype(jnp.bfloat16).reshape(SEQ_LEN, QKV_WIDTH)
    out_proj = jnp.dot(head_mix, w_o_stage, preferred_element_type=jnp.float32).astype(jnp.bfloat16)
    return (y_f32 + out_proj.astype(jnp.float32)).astype(jnp.bfloat16)


def reference(expert_out, expert_id, slot_id, gate, resid, owner, norm_w, w_q, w_k, w_v, w_o):
    from_prev = tuple(jnp.roll(arr_in, 1, axis=0) for arr_in in (expert_out, expert_id, slot_id, gate, resid))

    def per_stage(stage_args):
        out_s, ids_s, slots_s, gate_s, resid_s, owner_s, norm_s, w_q_s, w_k_s, w_v_s, w_o_s = stage_args

        def per_micro(micro_args):
            out_m, ids_m, slots_m, gate_m, resid_m = micro_args
            flat_out = out_m.reshape(EXPERTS * CAPACITY, MODEL_DIM)

            def per_seq(seq_index):
                seq_start = seq_index * SEQ_LEN
                ids_q = lax.dynamic_slice_in_dim(ids_m, seq_start, SEQ_LEN, 0)
                slots_q = lax.dynamic_slice_in_dim(slots_m, seq_start, SEQ_LEN, 0)
                gate_q = lax.dynamic_slice_in_dim(gate_m, seq_start, SEQ_LEN, 0)
                resid_q = lax.dynamic_slice_in_dim(resid_m, seq_start, SEQ_LEN, 0)
                kept_mask = slots_q >= 0
                row_index = ids_q * CAPACITY + jnp.where(kept_mask, slots_q, 0)
                picked = flat_out[row_index].astype(jnp.float32)
                weights = jnp.where(kept_mask, gate_q, 0.0)
                combined = jnp.einsum('lk,lkd->ld', weights, picked)
                y_seq = (resid_q.astype(jnp.float32) + combined).astype(jnp.bfloat16)
                return attend_block(y_seq, norm_s, w_q_s, w_k_s, w_v_s, w_o_s)

            return lax.map(per_seq, owner_s)

        return lax.map(per_micro, (out_s, ids_s, slots_s, gate_s, resid_s))

    result = lax.map(per_stage, from_prev + (owner, norm_w, w_q, w_k, w_v, w_o))
    return result.reshape(STAGES, MICRO, TOKENS, MODEL_DIM)
```

```python
import functools

import jax
import jax.numpy as jnp
from jax import lax
from jax.experimental import pallas as pl
from jax.experimental.pallas import tpu as pltpu
from jax.sharding import PartitionSpec as P

HEAD_DIM = 128
NORM_EPS = 1e-6
MESH = pl.DeviceIdType.MESH
CORES = 2


def attend_local(y_owned, norm_scale, w_q, w_k, w_v, w_o):
    n_micro, n_seqs, seq_len, model_dim = y_owned.shape
    n_heads = w_q.shape[1] // HEAD_DIM
    y_f32 = y_owned.astype(jnp.float32)
    inv_rms = lax.rsqrt(jnp.mean(y_f32 * y_f32, axis=-1, keepdims=True) + NORM_EPS)
    normed = (y_f32 * inv_rms * norm_scale).astype(jnp.bfloat16)

    def project(weight):
        proj_out = jnp.einsum('msld,de->msle', normed, weight, preferred_element_type=jnp.float32)
        return proj_out.astype(jnp.bfloat16).reshape(n_micro, n_seqs, seq_len, n_heads, HEAD_DIM)

    queries = project(w_q)
    key_vecs = project(w_k)
    values = project(w_v)
    scores = jnp.einsum('msqhe,mskhe->mshqk', queries, key_vecs, preferred_element_type=jnp.float32) * (HEAD_DIM ** -0.5)
    causal = jnp.arange(seq_len)[:, None] >= jnp.arange(seq_len)[None, :]
    attn_probs = jax.nn.softmax(jnp.where(causal, scores, -1e30), axis=-1).astype(jnp.bfloat16)
    head_mix = jnp.einsum('mshqk,mskhe->msqhe', attn_probs, values, preferred_element_type=jnp.float32).astype(jnp.bfloat16)
    out_proj = jnp.einsum('msqhe,hed->msqd', head_mix, w_o.reshape(n_heads, HEAD_DIM, model_dim), preferred_element_type=jnp.float32)
    return (y_f32 + out_proj.astype(jnp.bfloat16).astype(jnp.float32)).astype(jnp.bfloat16)


def combine_kernel(dims, route_ref, out_ref, resid_ref, y_ref,
                   obuf, hbuf, routes, table, wterm, p1, p2, p3, r1, r2, r3, own, ysend, yland,
                   o_loc, o_snd, o_rcv, h_loc, h_snd, h_rcv, t_loc, t_snd, t_rcv,
                   s1, s2, s3, q1, q2, q3, ys, yr):
    n_ep, n_st, n_loc, cap, slot_pad, seq_len, top_k, half = dims
    n_chip = n_ep // CORES
    n_half = n_ep // 2
    tok_dev = n_ep * seq_len
    me = lax.axis_index('ep')
    rank = lax.axis_index('pp')
    core = lax.rem(me, CORES)
    chip = me // CORES
    sib = me + 1 - 2 * core
    nxt = lax.rem(rank + 1, n_st)
    prv = lax.rem(rank + n_st - 1, n_st)
    side = [lax.rem(me + n_ep - CORES, n_ep), lax.rem(me + CORES, n_ep)]
    my_cols = pl.ds(pl.multiple_of(core * half, 128), half)
    sib_cols = pl.ds(pl.multiple_of((1 - core) * half, 128), half)

    loc = []
    for h in range(n_ep):
        loc.append(pltpu.make_async_copy(out_ref.at[:, pl.ds(h * cap, cap), my_cols],
                                         obuf.at[h, pl.ds(core * n_loc, n_loc), pl.ds(0, cap)], o_loc.at[h]))
        loc[-1].start()
    h_copy = pltpu.make_async_copy(resid_ref.at[:, my_cols], hbuf.at[core], h_loc)
    h_copy.start()
    t_copy = pltpu.make_async_copy(route_ref, routes.at[me], t_loc)
    t_copy.start()

    barrier = pltpu.get_barrier_semaphore()
    for k in range(1, n_ep):
        pl.semaphore_signal(barrier, inc=1, device_id={'ep': lax.rem(me + k, n_ep)}, device_id_type=MESH)
    for other in (nxt, prv):
        for jc in range(CORES):
            pl.semaphore_signal(barrier, inc=1, device_id={'pp': other, 'ep': chip * CORES + jc}, device_id_type=MESH)
    if slot_pad > cap:
        for h in range(n_ep):
            obuf[h, :, cap:, :] = jnp.zeros((CORES * n_loc, slot_pad - cap, half), jnp.bfloat16)
    pl.semaphore_wait(barrier, n_ep - 1 + 2 * CORES)

    t_out = []
    for k in range(1, n_ep):
        peer = lax.rem(me + k, n_ep)
        t_out.append(pltpu.make_async_remote_copy(route_ref, routes.at[me], t_snd.at[k - 1], t_rcv.at[me],
                                                  device_id={'ep': peer}, device_id_type=MESH))
        t_out[-1].start()
    o_out = []
    for h in range(n_ep):
        o_out.append(pltpu.make_async_remote_copy(out_ref.at[:, pl.ds(h * cap, cap), sib_cols],
                                                  obuf.at[h, pl.ds(core * n_loc, n_loc), pl.ds(0, cap)],
                                                  o_snd.at[h], o_rcv.at[h],
                                                  device_id={'ep': sib}, device_id_type=MESH))
        o_out[-1].start()
    h_out = pltpu.make_async_remote_copy(resid_ref.at[:, sib_cols], hbuf.at[core], h_snd, h_rcv,
                                         device_id={'ep': sib}, device_id_type=MESH)
    h_out.start()

    t_copy.wait()
    for k in range(1, n_ep):
        src = lax.rem(me + k, n_ep)
        pltpu.make_async_remote_copy(route_ref, routes.at[src], t_snd.at[k - 1], t_rcv.at[src],
                                     device_id={'ep': src}, device_id_type=MESH).wait_recv()
    h_copy.wait()
    h_out.wait_recv()

    def o_wait(h):
        pltpu.make_async_copy(out_ref.at[:, pl.ds(0, cap), my_cols],
                              obuf.at[h, pl.ds(core * n_loc, n_loc), pl.ds(0, cap)], o_loc.at[h]).wait()
        pltpu.make_async_remote_copy(out_ref.at[:, pl.ds(0, cap), sib_cols],
                                     obuf.at[h, pl.ds((1 - core) * n_loc, n_loc), pl.ds(0, cap)],
                                     o_snd.at[h], o_rcv.at[h],
                                     device_id={'ep': sib}, device_id_type=MESH).wait_recv()

    depth = CORES * n_loc * slot_pad
    width = min(256, half)
    lane = lax.broadcasted_iota(jnp.int32, (seq_len, depth), 1).astype(jnp.float32)
    block = CORES * seq_len

    def partial(q, ab):
        h = q + n_half * ab
        o_wait(h)
        rows = routes[h]
        rows = jnp.concatenate([rows, jnp.zeros((128 - rows.shape[0], tok_dev), jnp.float32)], axis=0)
        table[...] = rows.T
        step = 1 - 2 * ab
        dest = [chip + 2, chip + n_chip + step, chip + n_chip - step, chip]
        picks = []
        for r in range(n_chip):
            for jc in range(CORES):
                j = lax.rem(dest[r], n_chip) * CORES + jc
                picks.append(pl.multiple_of(j * seq_len, seq_len))
        base = (chip * depth).astype(jnp.float32)
        for b, start in enumerate(picks):
            rt = table[pl.ds(start, seq_len), :]
            w = jnp.zeros((seq_len, depth), jnp.float32)
            for j in range(top_k):
                key = rt[:, j:j + 1] - base
                w = jnp.where(lane == key, rt[:, top_k + j:top_k + j + 1], w)
            hi = w.astype(jnp.bfloat16)
            rest = w - hi.astype(jnp.float32)
            mid = rest.astype(jnp.bfloat16)
            low = (rest - mid.astype(jnp.float32)).astype(jnp.bfloat16)
            for t, term in enumerate((hi, mid, low)):
                wterm[pl.ds(t * tok_dev + b * seq_len, seq_len), :] = term

        dsts = [p1.at[ab, q], p2.at[1 - ab, q], p3.at[ab, q], own.at[ab, q]]

        @pl.loop(0, half // width)
        def _(n):
            cols = pl.ds(pl.multiple_of(n * width, width), width)
            slots = obuf[h, :, :, cols].reshape(depth, width)
            res = jnp.dot(wterm[...], slots, preferred_element_type=jnp.float32)
            res = res[:tok_dev] + (res[tok_dev:2 * tok_dev] + res[2 * tok_dev:])
            for r in range(n_chip):
                dsts[r][:, cols] = res[r * block:(r + 1) * block]

        @pl.when(h // CORES == chip)
        def _():
            hc = lax.rem(h, CORES)
            for b, start in enumerate(picks):
                dst = dsts[b // CORES]
                rs = slice((b % CORES) * seq_len, (b % CORES + 1) * seq_len)
                dst[rs, :] = dst[rs, :] + hbuf[hc, pl.ds(start, seq_len), :].astype(jnp.float32)

    def ring(src, dst, snd, rcv, d, q):
        return pltpu.make_async_remote_copy(src.at[d, q], dst.at[d, q], snd.at[d, q], rcv.at[d, q],
                                            device_id={'ep': side[d]}, device_id_type=MESH)

    def hop(q, jc):
        return pltpu.make_async_remote_copy(ysend.at[q, jc], yland.at[pl.ds(2 * q, 2), :, my_cols],
                                            ys.at[q, jc], yr.at[core, q],
                                            device_id={'pp': nxt, 'ep': chip * CORES + jc}, device_id_type=MESH)

    @pl.loop(0, n_half + 2)
    def _(it):
        @pl.when(it < n_half)
        def _():
            @pl.loop(0, 2)
            def _(ab):
                partial(it, ab)
            for d in range(2):
                ring(p1, r1, s1, q1, d, it).start()

        @pl.when(jnp.logical_and(it >= 1, it <= n_half))
        def _():
            q = it - 1
            for d in range(2):
                ring(p2, r2, s2, q2, d, q).start()
            for d in range(2):
                ring(p1, r1, s1, q1, d, q).wait_recv()
                p3[d, q] = p3[d, q] + r1[d, q]
                ring(p3, r3, s3, q3, d, q).start()

        @pl.when(it >= 2)
        def _():
            q = it - 2
            for d in range(2):
                ring(p2, r2, s2, q2, d, q).wait_recv()
                ring(p3, r3, s3, q3, d, q).wait_recv()
            for ab in range(2):
                total = own[ab, q] + (r3[ab, q] + r2[1 - ab, q])
                rounded = total.astype(jnp.bfloat16)
                for jc in range(CORES):
                    ysend[q, jc, ab] = rounded[jc * seq_len:(jc + 1) * seq_len]
            for jc in range(CORES):
                hop(q, jc).start()

    @pl.loop(0, n_half)
    def _(q):
        for c in range(CORES):
            cols = pl.ds(c * half, half)
            pltpu.make_async_remote_copy(ysend.at[q, 0], yland.at[pl.ds(2 * q, 2), :, cols],
                                         ys.at[q, 0], yr.at[c, q],
                                         device_id={'pp': nxt, 'ep': me}, device_id_type=MESH).wait_recv()
    y_ref[...] = yland[...]

    for k in range(1, n_ep):
        t_out[k - 1].wait_send()
    for h in range(n_ep):
        o_out[h].wait_send()
    h_out.wait_send()

    @pl.loop(0, n_half)
    def _(q):
        for d in range(2):
            ring(p1, r1, s1, q1, d, q).wait_send()
            ring(p2, r2, s2, q2, d, q).wait_send()
            ring(p3, r3, s3, q3, d, q).wait_send()
        for jc in range(CORES):
            hop(q, jc).wait_send()


def solution(mesh):
    n_stages = mesh.shape['pp']
    n_ep = mesh.shape['ep']
    prev_rank = [((src_rank + 1) % n_stages, src_rank) for src_rank in range(n_stages)]
    group_axes = ('data', 'pp')

    def device_step(expert_out, expert_id, slot_id, gate, resid, owner, norm_w, w_q, w_k, w_v, w_o):
        dev_index = lax.axis_index('ep')
        n_loc, capacity, model_dim = expert_out.shape[2:]
        cap = capacity // n_ep
        tok_dev, top_k = expert_id.shape[2:]
        seq_dev = owner.shape[1] // n_ep
        seq_len = tok_dev // seq_dev
        assert expert_out.shape[1] == 1 and seq_dev == n_ep
        half = model_dim // CORES
        slot_pad = -(-cap // 16) * 16
        n_half = n_ep // 2
        block = CORES * seq_len

        grid = owner[0].reshape(n_ep, seq_dev)
        homes = jnp.arange(n_ep)[:, None, None]
        pick = jnp.sum(jnp.where(grid[None] // seq_dev == homes, grid[None] - homes * seq_dev, 0), axis=2)
        pick = lax.ppermute(pick.reshape(-1).astype(jnp.int32), 'pp', prev_rank)
        my_src = lax.dynamic_index_in_dim(grid // seq_dev, dev_index, 0, keepdims=False)
        pos = (my_src % n_half * 2 + my_src // n_half).astype(jnp.int32)

        key = jnp.where(slot_id[0, 0] >= 0, expert_id[0, 0] * slot_pad + slot_id[0, 0] - dev_index * cap, -1)
        leaving = lax.dynamic_index_in_dim(pick.reshape(n_ep, n_ep), dev_index, 0, keepdims=False)
        route = jnp.concatenate([key.astype(jnp.float32), gate[0, 0]], axis=1)
        route = jnp.take(route.reshape(seq_dev, seq_len, 2 * top_k), leaving, axis=0).reshape(tok_dev, 2 * top_k).T
        held = jnp.take(resid[0, 0].reshape(seq_dev, seq_len, model_dim), leaving, axis=0).reshape(tok_dev, model_dim)

        dims = (n_ep, n_stages, n_loc, cap, slot_pad, seq_len, top_k, half)
        f32, bf16 = jnp.float32, jnp.bfloat16
        ringbuf = pltpu.VMEM((2, n_half, block, half), f32)
        dma = pltpu.SemaphoreType.DMA
        y_owned = pl.pallas_call(
            functools.partial(combine_kernel, dims),
            out_shape=jax.ShapeDtypeStruct((n_ep, seq_len, model_dim), bf16),
            in_specs=[pl.BlockSpec(memory_space=pltpu.VMEM)] + [pl.BlockSpec(memory_space=pl.ANY)] * 2,
            out_specs=pl.BlockSpec(memory_space=pltpu.VMEM),
            scratch_shapes=[
                pltpu.VMEM((n_ep, CORES * n_loc, slot_pad, half), bf16),
                pltpu.VMEM((CORES, tok_dev, half), bf16),
                pltpu.VMEM((n_ep, 2 * top_k, tok_dev), f32),
                pltpu.VMEM((tok_dev, 128), f32),
                pltpu.VMEM((3 * tok_dev, CORES * n_loc * slot_pad), bf16),
                ringbuf, ringbuf, ringbuf, ringbuf, ringbuf, ringbuf, ringbuf,
                pltpu.VMEM((n_half, CORES, 2, seq_len, half), bf16),
                pltpu.VMEM((n_ep, seq_len, model_dim), bf16),
                dma((n_ep,)), dma((n_ep,)), dma((n_ep,)),
                dma, dma, dma,
                dma, dma((n_ep - 1,)), dma((n_ep,)),
                dma((2, n_half)), dma((2, n_half)), dma((2, n_half)),
                dma((2, n_half)), dma((2, n_half)), dma((2, n_half)),
                dma((n_half, CORES)), dma((CORES, n_half)),
            ],
            compiler_params=pltpu.CompilerParams(collective_id=0, has_side_effects=True, vmem_limit_bytes=60 * 2 ** 20),
            name='combine',
        )(route, expert_out[0, 0], held)
        y_owned = jnp.take(y_owned, pos, axis=0)
        z_owned = attend_local(y_owned[None], norm_w[0], w_q[0], w_k[0], w_v[0], w_o[0])
        return z_owned.reshape(1, tok_dev, model_dim)[None]

    tok_spec = P(group_axes, None, 'ep', None)
    weight_spec = P('pp', None, None)
    in_specs = (P(group_axes, None, 'ep', None, None), tok_spec, tok_spec, tok_spec, tok_spec, P(group_axes, None), P('pp', None), weight_spec, weight_spec, weight_spec, weight_spec)
    return jax.shard_map(device_step, mesh=mesh, in_specs=in_specs, out_specs=tok_spec, check_vma=False)
```

```python
import functools

import jax
import jax.numpy as jnp
from jax import lax
from jax.experimental import pallas as pl
from jax.experimental.pallas import tpu as pltpu
from jax.sharding import PartitionSpec as P

HEAD_DIM = 128
NORM_EPS = 1e-6
MESH = pl.DeviceIdType.MESH
CORES = 2


def attend_local(y_owned, norm_scale, w_q, w_k, w_v, w_o):
    n_micro, n_seqs, seq_len, model_dim = y_owned.shape
    n_heads = w_q.shape[1] // HEAD_DIM
    y_f32 = y_owned.astype(jnp.float32)
    inv_rms = lax.rsqrt(jnp.mean(y_f32 * y_f32, axis=-1, keepdims=True) + NORM_EPS)
    normed = (y_f32 * inv_rms * norm_scale).astype(jnp.bfloat16)

    def project(weight):
        proj_out = jnp.einsum('msld,de->msle', normed, weight, preferred_element_type=jnp.float32)
        return proj_out.astype(jnp.bfloat16).reshape(n_micro, n_seqs, seq_len, n_heads, HEAD_DIM)

    queries = project(w_q)
    key_vecs = project(w_k)
    values = project(w_v)
    scores = jnp.einsum('msqhe,mskhe->mshqk', queries, key_vecs, preferred_element_type=jnp.float32) * (HEAD_DIM ** -0.5)
    causal = jnp.arange(seq_len)[:, None] >= jnp.arange(seq_len)[None, :]
    attn_probs = jax.nn.softmax(jnp.where(causal, scores, -1e30), axis=-1).astype(jnp.bfloat16)
    head_mix = jnp.einsum('mshqk,mskhe->msqhe', attn_probs, values, preferred_element_type=jnp.float32).astype(jnp.bfloat16)
    out_proj = jnp.einsum('msqhe,hed->msqd', head_mix, w_o.reshape(n_heads, HEAD_DIM, model_dim), preferred_element_type=jnp.float32)
    return (y_f32 + out_proj.astype(jnp.bfloat16).astype(jnp.float32)).astype(jnp.bfloat16)


def combine_kernel(dims, owner_ref, id_ref, slot_ref, gate_ref, out_ref, resid_ref, y_ref,
                   obuf, hbuf, routes, ids, slots, gates, owners, goes, table, wterm,
                   p1, p2, p3, r1, r2, r3, own, ysend, yland,
                   o_loc, o_snd, o_rcv, h_loc, h_snd, h_rcv, t_loc, t_snd, t_rcv, w_snd, w_rcv, w_loc,
                   s1, s2, s3, q1, q2, q3, ys, yr):
    n_ep, n_st, n_loc, cap, slot_pad, seq_len, top_k, half = dims
    n_chip = n_ep // CORES
    n_half = n_ep // 2
    tok_dev = n_ep * seq_len
    me = lax.axis_index('ep')
    rank = lax.axis_index('pp')
    core = lax.rem(me, CORES)
    chip = me // CORES
    sib = me + 1 - 2 * core
    nxt = lax.rem(rank + 1, n_st)
    prv = lax.rem(rank + n_st - 1, n_st)
    side = [lax.rem(me + n_ep - CORES, n_ep), lax.rem(me + CORES, n_ep)]
    my_cols = pl.ds(pl.multiple_of(core * half, 128), half)
    sib_cols = pl.ds(pl.multiple_of((1 - core) * half, 128), half)
    order = [q + n_half * ab for q in range(n_half) for ab in range(2)]

    small = [pltpu.make_async_copy(src, dst, t_loc.at[i])
             for i, (src, dst) in enumerate(((id_ref, ids), (slot_ref, slots), (gate_ref, gates)))]
    for copy in small:
        copy.start()
    barrier = pltpu.get_barrier_semaphore()
    for k in range(1, n_ep):
        pl.semaphore_signal(barrier, inc=1, device_id={'ep': lax.rem(me + k, n_ep)}, device_id_type=MESH)
    for other in (nxt, prv):
        for jc in range(CORES):
            pl.semaphore_signal(barrier, inc=1, device_id={'pp': other, 'ep': chip * CORES + jc}, device_id_type=MESH)
    for h in order:
        pltpu.make_async_copy(out_ref.at[:, pl.ds(h * cap, cap), my_cols],
                              obuf.at[h, pl.ds(core * n_loc, n_loc), pl.ds(0, cap)], o_loc.at[h]).start()
    h_copy = pltpu.make_async_copy(resid_ref.at[:, my_cols], hbuf.at[core], h_loc)
    h_copy.start()
    for copy in small:
        copy.wait()
    key = jnp.where(slots[...] >= 0, ids[...] * slot_pad + slots[...] - me * cap, -1)
    routes[me, :top_k] = key.astype(jnp.float32).T
    routes[me, top_k:] = gates[...].T
    if slot_pad > cap:
        for h in range(n_ep):
            obuf[h, :, cap:, :] = jnp.zeros((CORES * n_loc, slot_pad - cap, half), jnp.bfloat16)
    pl.semaphore_wait(barrier, n_ep - 1 + 2 * CORES)

    w_out = pltpu.make_async_remote_copy(owner_ref, owners, w_snd, w_rcv, device_id={'pp': prv}, device_id_type=MESH)
    w_out.start()
    t_out = []
    for k in (n_chip, n_chip - 1, n_chip + 1, 2, n_ep - 2, 1, n_ep - 1):
        peer = lax.rem(me + k, n_ep)
        t_out.append(pltpu.make_async_remote_copy(routes.at[me], routes.at[me], t_snd.at[k - 1], t_rcv.at[me],
                                                  device_id={'ep': peer}, device_id_type=MESH))
        t_out[-1].start()
    o_out = []
    for h in order:
        o_out.append(pltpu.make_async_remote_copy(out_ref.at[:, pl.ds(h * cap, cap), sib_cols],
                                                  obuf.at[h, pl.ds(core * n_loc, n_loc), pl.ds(0, cap)],
                                                  o_snd.at[h], o_rcv.at[h],
                                                  device_id={'ep': sib}, device_id_type=MESH))
        o_out[-1].start()
    h_out = pltpu.make_async_remote_copy(resid_ref.at[:, sib_cols], hbuf.at[core], h_snd, h_rcv,
                                         device_id={'ep': sib}, device_id_type=MESH)
    h_out.start()

    w_out.wait_recv()
    goes_copy = pltpu.make_async_copy(owners, goes, w_loc)
    goes_copy.start()
    for k in range(1, n_ep):
        src = lax.rem(me + k, n_ep)
        pltpu.make_async_remote_copy(routes.at[src], routes.at[src], t_snd.at[k - 1], t_rcv.at[src],
                                     device_id={'ep': src}, device_id_type=MESH).wait_recv()
    goes_copy.wait()

    def o_wait(h):
        pltpu.make_async_copy(out_ref.at[:, pl.ds(0, cap), my_cols],
                              obuf.at[h, pl.ds(core * n_loc, n_loc), pl.ds(0, cap)], o_loc.at[h]).wait()
        pltpu.make_async_remote_copy(out_ref.at[:, pl.ds(0, cap), sib_cols],
                                     obuf.at[h, pl.ds((1 - core) * n_loc, n_loc), pl.ds(0, cap)],
                                     o_snd.at[h], o_rcv.at[h],
                                     device_id={'ep': sib}, device_id_type=MESH).wait_recv()

    depth = CORES * n_loc * slot_pad
    width = min(256, half)
    lane = lax.broadcasted_iota(jnp.int32, (seq_len, depth), 1).astype(jnp.float32)
    block = CORES * seq_len

    def partial(q, ab):
        h = q + n_half * ab
        rows = routes[h]
        rows = jnp.concatenate([rows, jnp.zeros((128 - rows.shape[0], tok_dev), jnp.float32)], axis=0)
        table[...] = rows.T
        step = 1 - 2 * ab
        dest = [chip + 2, chip + n_chip + step, chip + n_chip - step, chip]
        picks = []
        for r in range(n_chip):
            for jc in range(CORES):
                j = lax.rem(dest[r], n_chip) * CORES + jc
                pick = 0
                for b in range(n_ep):
                    seq = goes[0, j * n_ep + b] - h * n_ep
                    pick = jnp.where(jnp.logical_and(seq >= 0, seq < n_ep), seq, pick)
                picks.append(pick)

        def chosen(pick, load):
            got = load(0)
            for s in range(1, n_ep):
                got = jnp.where(pick == s, load(s), got)
            return got

        base = (chip * depth).astype(jnp.float32)
        for b, pick in enumerate(picks):
            rt = chosen(pick, lambda s: table[s * seq_len:(s + 1) * seq_len, :])
            w = jnp.zeros((seq_len, depth), jnp.float32)
            for j in range(top_k):
                key = rt[:, j:j + 1] - base
                w = jnp.where(lane == key, rt[:, top_k + j:top_k + j + 1], w)
            hi = w.astype(jnp.bfloat16)
            rest = w - hi.astype(jnp.float32)
            mid = rest.astype(jnp.bfloat16)
            low = (rest - mid.astype(jnp.float32)).astype(jnp.bfloat16)
            for t, term in enumerate((hi, mid, low)):
                wterm[pl.ds(t * tok_dev + b * seq_len, seq_len), :] = term

        dsts = [p1.at[ab, q], p2.at[1 - ab, q], p3.at[ab, q], own.at[ab, q]]
        o_wait(h)

        @pl.loop(0, half // width)
        def _(n):
            cols = pl.ds(pl.multiple_of(n * width, width), width)
            slots_in = obuf[h, :, :, cols].reshape(depth, width)
            res = jnp.dot(wterm[...], slots_in, preferred_element_type=jnp.float32)
            res = res[:tok_dev] + (res[tok_dev:2 * tok_dev] + res[2 * tok_dev:])
            for r in range(n_chip):
                dsts[r][:, cols] = res[r * block:(r + 1) * block]

        @pl.when(h // CORES == chip)
        def _():
            hc = lax.rem(h, CORES)

            @pl.loop(0, half // width)
            def _(n):
                cols = pl.ds(pl.multiple_of(n * width, width), width)
                for b, pick in enumerate(picks):
                    dst = dsts[b // CORES]
                    rs = slice((b % CORES) * seq_len, (b % CORES + 1) * seq_len)
                    held = chosen(pick, lambda s: hbuf[hc, s * seq_len:(s + 1) * seq_len, cols].astype(jnp.float32))
                    dst[rs, cols] = dst[rs, cols] + held

    def ring(src, dst, snd, rcv, d, q):
        return pltpu.make_async_remote_copy(src.at[d, q], dst.at[d, q], snd.at[d, q], rcv.at[d, q],
                                            device_id={'ep': side[d]}, device_id_type=MESH)

    def hop(q, jc):
        return pltpu.make_async_remote_copy(ysend.at[q, jc], yland.at[pl.ds(2 * q, 2), :, my_cols],
                                            ys.at[q, jc], yr.at[core, q],
                                            device_id={'pp': nxt, 'ep': chip * CORES + jc}, device_id_type=MESH)

    h_copy.wait()
    h_out.wait_recv()

    @pl.loop(0, n_half + 2)
    def _(it):
        @pl.when(it < n_half)
        def _():
            @pl.loop(0, 2)
            def _(ab):
                partial(it, ab)
                for d in range(2):
                    @pl.when(ab == d)
                    def _():
                        ring(p1, r1, s1, q1, d, it).start()

                        @pl.when(it == 0)
                        def _():
                            ring(p2, r2, s2, q2, 1 - d, it).start()

        @pl.when(jnp.logical_and(it >= 1, it <= n_half))
        def _():
            q = it - 1
            for d in range(2):
                ring(p1, r1, s1, q1, d, q).wait_recv()
                p3[d, q] = p3[d, q] + r1[d, q]
                ring(p3, r3, s3, q3, d, q).start()

        @pl.when(jnp.logical_and(it >= 1, it < n_half))
        def _():
            for d in range(2):
                ring(p2, r2, s2, q2, d, it).start()

        @pl.when(it >= 2)
        def _():
            q = it - 2
            for d in range(2):
                ring(p2, r2, s2, q2, d, q).wait_recv()
                ring(p3, r3, s3, q3, d, q).wait_recv()
            for ab in range(2):
                total = own[ab, q] + (r3[ab, q] + r2[1 - ab, q])
                rounded = total.astype(jnp.bfloat16)
                for jc in range(CORES):
                    ysend[q, jc, ab] = rounded[jc * seq_len:(jc + 1) * seq_len]
            for jc in range(CORES):
                hop(q, jc).start()

    @pl.loop(0, n_half)
    def _(q):
        for c in range(CORES):
            cols = pl.ds(c * half, half)
            pltpu.make_async_remote_copy(ysend.at[q, 0], yland.at[pl.ds(2 * q, 2), :, cols],
                                         ys.at[q, 0], yr.at[c, q],
                                         device_id={'pp': nxt, 'ep': me}, device_id_type=MESH).wait_recv()
    y_ref[...] = yland[...]

    w_out.wait_send()
    for copy in t_out + o_out:
        copy.wait_send()
    h_out.wait_send()

    @pl.loop(0, n_half)
    def _(q):
        for d in range(2):
            ring(p1, r1, s1, q1, d, q).wait_send()
            ring(p2, r2, s2, q2, d, q).wait_send()
            ring(p3, r3, s3, q3, d, q).wait_send()
        for jc in range(CORES):
            hop(q, jc).wait_send()


def solution(mesh):
    n_stages = mesh.shape['pp']
    n_ep = mesh.shape['ep']
    group_axes = ('data', 'pp')

    def device_step(expert_out, expert_id, slot_id, gate, resid, owner, norm_w, w_q, w_k, w_v, w_o):
        dev_index = lax.axis_index('ep')
        n_loc, capacity, model_dim = expert_out.shape[2:]
        cap = capacity // n_ep
        tok_dev, top_k = expert_id.shape[2:]
        seq_dev = owner.shape[1] // n_ep
        seq_len = tok_dev // seq_dev
        assert expert_out.shape[1] == 1 and seq_dev == n_ep
        half = model_dim // CORES
        slot_pad = -(-cap // 16) * 16
        n_half = n_ep // 2
        block = CORES * seq_len

        dims = (n_ep, n_stages, n_loc, cap, slot_pad, seq_len, top_k, half)
        f32, bf16 = jnp.float32, jnp.bfloat16
        ringbuf = pltpu.VMEM((2, n_half, block, half), f32)
        dma = pltpu.SemaphoreType.DMA
        y_owned = pl.pallas_call(
            functools.partial(combine_kernel, dims),
            out_shape=jax.ShapeDtypeStruct((n_ep, seq_len, model_dim), bf16),
            in_specs=[pl.BlockSpec(memory_space=pl.ANY)] * 6,
            out_specs=pl.BlockSpec(memory_space=pltpu.VMEM),
            scratch_shapes=[
                pltpu.VMEM((n_ep, CORES * n_loc, slot_pad, half), bf16),
                pltpu.VMEM((CORES, tok_dev, half), bf16),
                pltpu.VMEM((n_ep, 2 * top_k, tok_dev), f32),
                pltpu.VMEM((tok_dev, top_k), jnp.int32),
                pltpu.VMEM((tok_dev, top_k), jnp.int32),
                pltpu.VMEM((tok_dev, top_k), f32),
                pltpu.VMEM((1, n_ep * seq_dev), jnp.int32),
                pltpu.SMEM((1, n_ep * seq_dev), jnp.int32),
                pltpu.VMEM((tok_dev, 128), f32),
                pltpu.VMEM((3 * tok_dev, CORES * n_loc * slot_pad), bf16),
                ringbuf, ringbuf, ringbuf, ringbuf, ringbuf, ringbuf, ringbuf,
                pltpu.VMEM((n_half, CORES, 2, seq_len, half), bf16),
                pltpu.VMEM((n_ep, seq_len, model_dim), bf16),
                dma((n_ep,)), dma((n_ep,)), dma((n_ep,)),
                dma, dma, dma,
                dma((3,)), dma((n_ep - 1,)), dma((n_ep,)),
                dma, dma, dma,
                dma((2, n_half)), dma((2, n_half)), dma((2, n_half)),
                dma((2, n_half)), dma((2, n_half)), dma((2, n_half)),
                dma((n_half, CORES)), dma((CORES, n_half)),
            ],
            compiler_params=pltpu.CompilerParams(collective_id=0, has_side_effects=True, vmem_limit_bytes=60 * 2 ** 20),
            name='combine',
        )(owner, expert_id[0, 0], slot_id[0, 0], gate[0, 0], expert_out[0, 0], resid[0, 0])
        source = lax.dynamic_slice_in_dim(owner[0], dev_index * seq_dev, seq_dev) // seq_dev
        y_owned = jnp.take(y_owned, source % n_half * 2 + source // n_half, axis=0)
        z_owned = attend_local(y_owned[None], norm_w[0], w_q[0], w_k[0], w_v[0], w_o[0])
        return z_owned.reshape(1, tok_dev, model_dim)[None]

    tok_spec = P(group_axes, None, 'ep', None)
    weight_spec = P('pp', None, None)
    in_specs = (P(group_axes, None, 'ep', None, None), tok_spec, tok_spec, tok_spec, tok_spec, P(group_axes, None), P('pp', None), weight_spec, weight_spec, weight_spec, weight_spec)
    return jax.shard_map(device_step, mesh=mesh, in_specs=in_specs, out_specs=tok_spec, check_vma=False)
```

```python
import functools

import jax
import jax.numpy as jnp
from jax import lax
from jax.experimental import pallas as pl
from jax.experimental.pallas import tpu as pltpu
from jax.sharding import PartitionSpec as P

HEAD_DIM = 128
NORM_EPS = 1e-6
MESH = pl.DeviceIdType.MESH
CORES = 2


def stage_kernel(dims, owner_ref, id_ref, slot_ref, gate_ref, out_ref, resid_ref, norm_ref, q_ref, k_ref, v_ref, o_ref, z_ref,
                   obuf, hbuf, routes, ids, slots, gates, owners, goes, table, wterm,
                   p1, p2, p3, r1, r2, r3, own, ysend, yland, norm, wq, wk, wv, wo, xs, mix,
                   o_loc, o_snd, o_rcv, h_loc, h_snd, h_rcv, t_loc, t_snd, t_rcv, w_snd, w_rcv, w_loc,
                   s1, s2, s3, q1, q2, q3, ys, yr, wt, zs):
    n_ep, n_st, n_loc, cap, slot_pad, seq_len, top_k, half = dims
    n_chip = n_ep // CORES
    n_half = n_ep // 2
    tok_dev = n_ep * seq_len
    me = lax.axis_index('ep')
    rank = lax.axis_index('pp')
    core = lax.rem(me, CORES)
    chip = me // CORES
    sib = me + 1 - 2 * core
    nxt = lax.rem(rank + 1, n_st)
    prv = lax.rem(rank + n_st - 1, n_st)
    side = [lax.rem(me + n_ep - CORES, n_ep), lax.rem(me + CORES, n_ep)]
    my_cols = pl.ds(pl.multiple_of(core * half, 128), half)
    sib_cols = pl.ds(pl.multiple_of((1 - core) * half, 128), half)
    order = [q + n_half * ab for q in range(n_half) for ab in range(2)]

    small = [pltpu.make_async_copy(src, dst, t_loc.at[i])
             for i, (src, dst) in enumerate(((id_ref, ids), (slot_ref, slots), (gate_ref, gates)))]
    for copy in small:
        copy.start()
    barrier = pltpu.get_barrier_semaphore()
    for k in range(1, n_ep):
        pl.semaphore_signal(barrier, inc=1, device_id={'ep': lax.rem(me + k, n_ep)}, device_id_type=MESH)
    for other in (nxt, prv):
        for jc in range(CORES):
            pl.semaphore_signal(barrier, inc=1, device_id={'pp': other, 'ep': chip * CORES + jc}, device_id_type=MESH)
    for h in order:
        pltpu.make_async_copy(out_ref.at[:, pl.ds(h * cap, cap), my_cols],
                              obuf.at[h, pl.ds(core * n_loc, n_loc), pl.ds(0, cap)], o_loc.at[h]).start()
    h_copy = pltpu.make_async_copy(resid_ref.at[:, my_cols], hbuf.at[core], h_loc)
    h_copy.start()
    for copy in small:
        copy.wait()
    key = jnp.where(slots[...] >= 0, ids[...] * slot_pad + slots[...] - me * cap, -1)
    routes[me, :top_k] = key.astype(jnp.float32)
    routes[me, top_k:] = gates[...]
    if slot_pad > cap:
        for h in range(n_ep):
            obuf[h, :, cap:, :] = jnp.zeros((CORES * n_loc, slot_pad - cap, half), jnp.bfloat16)
    pl.semaphore_wait(barrier, n_ep - 1 + 2 * CORES)

    w_out = pltpu.make_async_remote_copy(owner_ref, owners, w_snd, w_rcv, device_id={'pp': prv}, device_id_type=MESH)
    w_out.start()
    t_out = []
    for k in (n_chip, n_chip - 1, n_chip + 1, 2, n_ep - 2, 1, n_ep - 1):
        peer = lax.rem(me + k, n_ep)
        t_out.append(pltpu.make_async_remote_copy(routes.at[me], routes.at[me], t_snd.at[k - 1], t_rcv.at[me],
                                                  device_id={'ep': peer}, device_id_type=MESH))
        t_out[-1].start()
    o_out = []
    for h in order:
        o_out.append(pltpu.make_async_remote_copy(out_ref.at[:, pl.ds(h * cap, cap), sib_cols],
                                                  obuf.at[h, pl.ds(core * n_loc, n_loc), pl.ds(0, cap)],
                                                  o_snd.at[h], o_rcv.at[h],
                                                  device_id={'ep': sib}, device_id_type=MESH))
        o_out[-1].start()
    h_out = pltpu.make_async_remote_copy(resid_ref.at[:, sib_cols], hbuf.at[core], h_snd, h_rcv,
                                         device_id={'ep': sib}, device_id_type=MESH)
    h_out.start()

    w_out.wait_recv()
    goes_copy = pltpu.make_async_copy(owners, goes, w_loc)
    goes_copy.start()
    for k in range(1, n_ep):
        src = lax.rem(me + k, n_ep)
        pltpu.make_async_remote_copy(routes.at[src], routes.at[src], t_snd.at[k - 1], t_rcv.at[src],
                                     device_id={'ep': src}, device_id_type=MESH).wait_recv()
    goes_copy.wait()

    def o_wait(h):
        pltpu.make_async_copy(out_ref.at[:, pl.ds(0, cap), my_cols],
                              obuf.at[h, pl.ds(core * n_loc, n_loc), pl.ds(0, cap)], o_loc.at[h]).wait()
        pltpu.make_async_remote_copy(out_ref.at[:, pl.ds(0, cap), sib_cols],
                                     obuf.at[h, pl.ds((1 - core) * n_loc, n_loc), pl.ds(0, cap)],
                                     o_snd.at[h], o_rcv.at[h],
                                     device_id={'ep': sib}, device_id_type=MESH).wait_recv()

    depth = CORES * n_loc * slot_pad
    width = min(256, half)
    n_sub = half // width
    model = CORES * half
    tile = min(512, model)
    weights = [pltpu.make_async_copy(src, dst, wt.at[i])
               for i, (src, dst) in enumerate(((q_ref, wq), (k_ref, wk), (v_ref, wv), (o_ref, wo), (norm_ref, norm)))]
    lane = lax.broadcasted_iota(jnp.int32, (seq_len, depth), 1).astype(jnp.float32)
    block = CORES * seq_len

    def partial(q, ab):
        h = q + n_half * ab
        rows = routes[h]
        rows = jnp.concatenate([rows, jnp.zeros((128 - rows.shape[0], tok_dev), jnp.float32)], axis=0)
        table[...] = rows.T
        step = 1 - 2 * ab
        dest = [chip + 2, chip + n_chip + step, chip + n_chip - step, chip]
        picks = []
        for r in range(n_chip):
            for jc in range(CORES):
                j = lax.rem(dest[r], n_chip) * CORES + jc
                pick = 0
                for b in range(n_ep):
                    seq = goes[0, j * n_ep + b] - h * n_ep
                    pick = jnp.where(jnp.logical_and(seq >= 0, seq < n_ep), seq, pick)
                picks.append(pick)

        def chosen(pick, load):
            got = load(0)
            for s in range(1, n_ep):
                got = jnp.where(pick == s, load(s), got)
            return got

        base = (chip * depth).astype(jnp.float32)
        for b, pick in enumerate(picks):
            rt = chosen(pick, lambda s: table[s * seq_len:(s + 1) * seq_len, :])
            w = jnp.zeros((seq_len, depth), jnp.float32)
            for j in range(top_k):
                key = rt[:, j:j + 1] - base
                w = jnp.where(lane == key, rt[:, top_k + j:top_k + j + 1], w)
            hi = w.astype(jnp.bfloat16)
            rest = w - hi.astype(jnp.float32)
            mid = rest.astype(jnp.bfloat16)
            low = (rest - mid.astype(jnp.float32)).astype(jnp.bfloat16)
            for t, term in enumerate((hi, mid, low)):
                wterm[pl.ds(t * tok_dev + b * seq_len, seq_len), :] = term

        dsts = [p1.at[ab, q], p2.at[1 - ab, q], p3.at[ab, lax.rem(q, 2)], own.at[ab, lax.rem(q, 3)]]
        o_wait(h)

        @pl.loop(0, half // width)
        def _(n):
            cols = pl.ds(pl.multiple_of(n * width, width), width)
            slots_in = obuf[h, :, :, cols].reshape(depth, width)
            res = jnp.dot(wterm[...], slots_in, preferred_element_type=jnp.float32)
            res = res[:tok_dev] + (res[tok_dev:2 * tok_dev] + res[2 * tok_dev:])
            for r in range(n_chip):
                dsts[r][:, cols] = res[r * block:(r + 1) * block]

        @pl.when(h // CORES == chip)
        def _():
            hc = lax.rem(h, CORES)

            @pl.loop(0, half // width)
            def _(n):
                cols = pl.ds(pl.multiple_of(n * width, width), width)
                for b, pick in enumerate(picks):
                    dst = dsts[b // CORES]
                    rs = slice((b % CORES) * seq_len, (b % CORES + 1) * seq_len)
                    held = chosen(pick, lambda s: hbuf[hc, s * seq_len:(s + 1) * seq_len, cols].astype(jnp.float32))
                    dst[rs, cols] = dst[rs, cols] + held

    def ring(src, dst, snd, rcv, d, q):
        return pltpu.make_async_remote_copy(src.at[d, q], dst.at[d, q], snd.at[d, q], rcv.at[d, q],
                                            device_id={'ep': side[d]}, device_id_type=MESH)

    def sub(n):
        return pl.ds(pl.multiple_of(n * width, width), width)

    def last_leg(d, q, n):
        return pltpu.make_async_remote_copy(r1.at[d, q, :, sub(n)], r3.at[d, q, :, sub(n)], s3.at[d, q, n], q3.at[d, q, n],
                                            device_id={'ep': side[d]}, device_id_type=MESH)

    def hop(q, jc, n, c, to):
        cols = pl.ds(pl.multiple_of(c * half + n * width, width), width)
        return pltpu.make_async_remote_copy(ysend.at[q, jc, :, :, sub(n)], yland.at[pl.ds(2 * q, 2), :, cols],
                                            ys.at[q, jc, n], yr.at[c, q, n],
                                            device_id={'pp': nxt, 'ep': to}, device_id_type=MESH)

    def finish(q, n):
        @pl.when(n == 0)
        def _():
            for d in range(2):
                ring(p2, r2, s2, q2, d, q).wait_recv()
        cols = sub(n)
        for d in range(2):
            last_leg(d, q, n).wait_recv()
        for ab in range(2):
            total = own[ab, lax.rem(q, 3), :, cols] + (r3[ab, q, :, cols] + r2[1 - ab, q, :, cols])
            rounded = total.astype(jnp.bfloat16)
            for jc in range(CORES):
                ysend[q, jc, ab, :, cols] = rounded[jc * seq_len:(jc + 1) * seq_len]
        for jc in range(CORES):
            hop(q, jc, n, core, chip * CORES + jc).start()

    n_tok = 2 * seq_len
    row = lax.broadcasted_iota(jnp.int32, (n_tok, n_tok), 0)
    col = lax.broadcasted_iota(jnp.int32, (n_tok, n_tok), 1)
    causal = jnp.logical_and(row >= col, row // seq_len == col // seq_len)

    def normalise(q):
        for c in range(CORES):
            for n in range(n_sub):
                hop(q, 0, n, c, me).wait_recv()
        for ab in range(2):
            y = yland[2 * q + ab].astype(jnp.float32)
            inv = lax.rsqrt(jnp.mean(y * y, axis=-1, keepdims=True) + NORM_EPS)
            xs[ab * seq_len:(ab + 1) * seq_len, :] = (y * inv * norm[...]).astype(jnp.bfloat16)

    def attend(n):
        cols = pl.ds(pl.multiple_of(n * tile, tile), tile)
        x = xs[...]
        qt, kt, vt = (jnp.dot(x, w[:, cols], preferred_element_type=jnp.float32).astype(jnp.bfloat16) for w in (wq, wk, wv))
        for hd in range(tile // HEAD_DIM):
            hs = slice(hd * HEAD_DIM, (hd + 1) * HEAD_DIM)
            scores = lax.dot_general(qt[:, hs], kt[:, hs], (((1,), (1,)), ((), ())), preferred_element_type=jnp.float32)
            scores = jnp.where(causal, scores * (HEAD_DIM ** -0.5), -1e30)
            raised = jnp.exp(scores - jnp.max(scores, axis=-1, keepdims=True))
            probs = (raised / jnp.sum(raised, axis=-1, keepdims=True)).astype(jnp.bfloat16)
            mixed = jnp.dot(probs, vt[:, hs], preferred_element_type=jnp.float32).astype(jnp.bfloat16)
            mix[:, pl.ds(pl.multiple_of(n * tile + hd * HEAD_DIM, HEAD_DIM), HEAD_DIM)] = mixed

    def project(q):
        @pl.loop(0, model // tile)
        def _(n):
            cols = pl.ds(pl.multiple_of(n * tile, tile), tile)
            out = jnp.dot(mix[...], wo[:, cols], preferred_element_type=jnp.float32).astype(jnp.bfloat16).astype(jnp.float32)
            for ab in range(2):
                y = yland[2 * q + ab, :, cols].astype(jnp.float32)
                yland[2 * q + ab, :, cols] = (y + out[ab * seq_len:(ab + 1) * seq_len]).astype(jnp.bfloat16)

    def store(q):
        return pltpu.make_async_copy(yland.at[pl.ds(2 * q, 2)], z_ref.at[pl.ds(2 * q, 2)], zs.at[q])

    h_copy.wait()
    h_out.wait_recv()

    @pl.loop(0, n_half + 3)
    def _(it):
        @pl.when(it < n_half)
        def _():
            @pl.loop(0, 2)
            def _(ab):
                partial(it, ab)
                for d in range(2):
                    @pl.when(ab == d)
                    def _():
                        ring(p1, r1, s1, q1, d, it).start()

                        @pl.when(it == 0)
                        def _():
                            ring(p2, r2, s2, q2, 1 - d, it).start()

        @pl.when(it == 0)
        def _():
            for copy in weights:
                copy.start()

        @pl.when(jnp.logical_and(it >= 1, it <= n_half))
        def _():
            q = it - 1
            for d in range(2):
                ring(p1, r1, s1, q1, d, q).wait_recv()
                r1[d, q] = p3[d, lax.rem(q, 2)] + r1[d, q]
                for n in range(n_sub):
                    last_leg(d, q, n).start()

        @pl.when(jnp.logical_and(it >= 1, it < n_half))
        def _():
            for d in range(2):
                ring(p2, r2, s2, q2, d, it).start()

        @pl.when(it == 3)
        def _():
            for copy in weights:
                copy.wait()

        @pl.when(it >= 3)
        def _():
            normalise(it - 3)

        @pl.loop(0, n_sub)
        def _(n):
            @pl.when(it >= 3)
            def _():
                attend(n)

            @pl.when(jnp.logical_and(it >= 2, it < n_half + 2))
            def _():
                finish(it - 2, n)

        @pl.when(it >= 3)
        def _():
            project(it - 3)
            store(it - 3).start()

    w_out.wait_send()
    for copy in t_out + o_out:
        copy.wait_send()
    h_out.wait_send()

    @pl.loop(0, n_half)
    def _(q):
        for d in range(2):
            ring(p1, r1, s1, q1, d, q).wait_send()
            ring(p2, r2, s2, q2, d, q).wait_send()
            for n in range(n_sub):
                last_leg(d, q, n).wait_send()
        for jc in range(CORES):
            for n in range(n_sub):
                hop(q, jc, n, core, chip * CORES + jc).wait_send()
        store(q).wait()


def solution(mesh):
    n_stages = mesh.shape['pp']
    n_ep = mesh.shape['ep']
    group_axes = ('data', 'pp')

    def device_step(expert_out, expert_id, slot_id, gate, resid, owner, norm_w, w_q, w_k, w_v, w_o):
        dev_index = lax.axis_index('ep')
        n_loc, capacity, model_dim = expert_out.shape[2:]
        cap = capacity // n_ep
        tok_dev, top_k = expert_id.shape[2:]
        seq_dev = owner.shape[1] // n_ep
        seq_len = tok_dev // seq_dev
        assert expert_out.shape[1] == 1 and seq_dev == n_ep
        half = model_dim // CORES
        slot_pad = -(-cap // 16) * 16
        n_half = n_ep // 2
        block = CORES * seq_len

        dims = (n_ep, n_stages, n_loc, cap, slot_pad, seq_len, top_k, half)
        f32, bf16 = jnp.float32, jnp.bfloat16
        n_sub = half // min(256, half)
        assert model_dim // min(512, model_dim) == n_sub and n_half > 3

        def ringbuf(slots):
            return pltpu.VMEM((2, slots, block, half), f32)

        square = pltpu.VMEM((model_dim, model_dim), bf16)
        dma = pltpu.SemaphoreType.DMA
        z_pairs = pl.pallas_call(
            functools.partial(stage_kernel, dims),
            out_shape=jax.ShapeDtypeStruct((n_ep, seq_len, model_dim), bf16),
            in_specs=[pl.BlockSpec(memory_space=pl.ANY)] * 11,
            out_specs=pl.BlockSpec(memory_space=pl.ANY),
            scratch_shapes=[
                pltpu.VMEM((n_ep, CORES * n_loc, slot_pad, half), bf16),
                pltpu.VMEM((CORES, tok_dev, half), bf16),
                pltpu.VMEM((n_ep, 2 * top_k, tok_dev), f32),
                pltpu.VMEM((top_k, tok_dev), jnp.int32),
                pltpu.VMEM((top_k, tok_dev), jnp.int32),
                pltpu.VMEM((top_k, tok_dev), f32),
                pltpu.VMEM((1, n_ep * seq_dev), jnp.int32),
                pltpu.SMEM((1, n_ep * seq_dev), jnp.int32),
                pltpu.VMEM((tok_dev, 128), f32),
                pltpu.VMEM((3 * tok_dev, CORES * n_loc * slot_pad), bf16),
                ringbuf(n_half), ringbuf(n_half), ringbuf(2), ringbuf(n_half), ringbuf(n_half), ringbuf(n_half), ringbuf(3),
                pltpu.VMEM((n_half, CORES, 2, seq_len, half), bf16),
                pltpu.VMEM((n_ep, seq_len, model_dim), bf16),
                pltpu.VMEM((1, model_dim), f32),
                square, square, square, square,
                pltpu.VMEM((2 * seq_len, model_dim), bf16),
                pltpu.VMEM((2 * seq_len, model_dim), bf16),
                dma((n_ep,)), dma((n_ep,)), dma((n_ep,)),
                dma, dma, dma,
                dma((3,)), dma((n_ep - 1,)), dma((n_ep,)),
                dma, dma, dma,
                dma((2, n_half)), dma((2, n_half)), dma((2, n_half, n_sub)),
                dma((2, n_half)), dma((2, n_half)), dma((2, n_half, n_sub)),
                dma((n_half, CORES, n_sub)), dma((CORES, n_half, n_sub)), dma((5,)), dma((n_half,)),
            ],
            compiler_params=pltpu.CompilerParams(collective_id=0, has_side_effects=True, vmem_limit_bytes=67043328),
            name='stage',
        )(owner, expert_id[0, 0].T, slot_id[0, 0].T, gate[0, 0].T, expert_out[0, 0], resid[0, 0],
          norm_w, w_q[0], w_k[0], w_v[0], w_o[0])
        source = lax.dynamic_slice_in_dim(owner[0], dev_index * seq_dev, seq_dev) // seq_dev
        z_owned = jnp.take(z_pairs, source % n_half * 2 + source // n_half, axis=0)
        return z_owned.reshape(1, 1, tok_dev, model_dim)

    tok_spec = P(group_axes, None, 'ep', None)
    weight_spec = P('pp', None, None)
    in_specs = (P(group_axes, None, 'ep', None, None), tok_spec, tok_spec, tok_spec, tok_spec, P(group_axes, None), P('pp', None), weight_spec, weight_spec, weight_spec, weight_spec)
    return jax.shard_map(device_step, mesh=mesh, in_specs=in_specs, out_specs=tok_spec, check_vma=False)
```

```python
import functools

import jax
import jax.numpy as jnp
from jax import lax
from jax.experimental import pallas as pl
from jax.experimental.pallas import tpu as pltpu
from jax.sharding import PartitionSpec as P

HEAD_DIM = 128
NORM_EPS = 1e-6
MESH = pl.DeviceIdType.MESH
CORES = 2


def stage_kernel(dims, owner_ref, id_ref, slot_ref, gate_ref, out_ref, resid_ref, norm_ref, q_ref, k_ref, v_ref, o_ref, z_ref,
                   obuf, hbuf, routes, ids, slots, gates, owners, goes, table, wterm,
                   p1, p2, p3, r1, r2, r3, own, ysend, yland, norm, wq, wk, wv, wo, xs, mix,
                   o_loc, o_snd, o_rcv, h_loc, h_snd, h_rcv, t_loc, t_snd, t_rcv, w_snd, w_rcv, w_loc,
                   s1, s2, s3, q1, q2, q3, ys, yr, wt, zs, n_loc_sem):
    n_ep, n_st, n_loc, cap, slot_pad, seq_len, top_k, half = dims
    n_chip = n_ep // CORES
    n_half = n_ep // 2
    tok_dev = n_ep * seq_len
    me = lax.axis_index('ep')
    rank = lax.axis_index('pp')
    core = lax.rem(me, CORES)
    chip = me // CORES
    sib = me + 1 - 2 * core
    nxt = lax.rem(rank + 1, n_st)
    prv = lax.rem(rank + n_st - 1, n_st)
    side = [lax.rem(me + n_ep - CORES, n_ep), lax.rem(me + CORES, n_ep)]
    my_cols = pl.ds(pl.multiple_of(core * half, 128), half)
    sib_cols = pl.ds(pl.multiple_of((1 - core) * half, 128), half)
    order = [q + n_half * ab for q in range(n_half) for ab in range(2)]

    small = [pltpu.make_async_copy(src, dst, t_loc.at[i])
             for i, (src, dst) in enumerate(((id_ref, ids), (slot_ref, slots), (gate_ref, gates)))]
    for copy in small:
        copy.start()
    barrier = pltpu.get_barrier_semaphore()
    for k in range(1, n_ep):
        pl.semaphore_signal(barrier, inc=1, device_id={'ep': lax.rem(me + k, n_ep)}, device_id_type=MESH)
    for other in (nxt, prv):
        for jc in range(CORES):
            pl.semaphore_signal(barrier, inc=1, device_id={'pp': other, 'ep': chip * CORES + jc}, device_id_type=MESH)
    for h in order:
        pltpu.make_async_copy(out_ref.at[:, pl.ds(h * cap, cap), my_cols],
                              obuf.at[h, pl.ds(core * n_loc, n_loc), pl.ds(0, cap)], o_loc.at[h]).start()
    h_copy = pltpu.make_async_copy(resid_ref.at[:, my_cols], hbuf.at[core], h_loc)
    h_copy.start()
    model = CORES * half
    strip = model // n_half

    def weight(i, part):
        src, dst = ((q_ref, wq), (k_ref, wk), (v_ref, wv), (o_ref, wo))[i]
        rows = pl.ds(part * strip, strip)
        return pltpu.make_async_copy(src.at[rows], dst.at[rows], wt.at[i, part])

    norm_copy = pltpu.make_async_copy(norm_ref, norm, n_loc_sem)
    norm_copy.start()
    for part in range(n_half):
        weight(0, part).start()
    for copy in small:
        copy.wait()
    key = jnp.where(slots[...] >= 0, ids[...] * slot_pad + slots[...] - me * cap, -1)
    routes[me, :top_k] = key.astype(jnp.float32)
    routes[me, top_k:] = gates[...]
    if slot_pad > cap:
        for h in range(n_ep):
            obuf[h, :, cap:, :] = jnp.zeros((CORES * n_loc, slot_pad - cap, half), jnp.bfloat16)
    pl.semaphore_wait(barrier, n_ep - 1 + 2 * CORES)

    w_out = pltpu.make_async_remote_copy(owner_ref, owners, w_snd, w_rcv, device_id={'pp': prv}, device_id_type=MESH)
    w_out.start()
    t_out = []
    for k in (n_chip, n_chip - 1, n_chip + 1, 2, n_ep - 2, 1, n_ep - 1):
        peer = lax.rem(me + k, n_ep)
        t_out.append(pltpu.make_async_remote_copy(routes.at[me], routes.at[me], t_snd.at[k - 1], t_rcv.at[me],
                                                  device_id={'ep': peer}, device_id_type=MESH))
        t_out[-1].start()

    def o_out(h):
        return pltpu.make_async_remote_copy(out_ref.at[:, pl.ds(h * cap, cap), sib_cols],
                                            obuf.at[h, pl.ds(core * n_loc, n_loc), pl.ds(0, cap)],
                                            o_snd.at[h], o_rcv.at[h],
                                            device_id={'ep': sib}, device_id_type=MESH)

    h_out = pltpu.make_async_remote_copy(resid_ref.at[:, sib_cols], hbuf.at[core], h_snd, h_rcv,
                                         device_id={'ep': sib}, device_id_type=MESH)
    for i, h in enumerate(order):
        o_out(h).start()
        if i == 1:
            h_out.start()

    w_out.wait_recv()
    goes_copy = pltpu.make_async_copy(owners, goes, w_loc)
    goes_copy.start()
    goes_copy.wait()

    def o_wait(h):
        pltpu.make_async_copy(out_ref.at[:, pl.ds(0, cap), my_cols],
                              obuf.at[h, pl.ds(core * n_loc, n_loc), pl.ds(0, cap)], o_loc.at[h]).wait()
        pltpu.make_async_remote_copy(out_ref.at[:, pl.ds(0, cap), sib_cols],
                                     obuf.at[h, pl.ds((1 - core) * n_loc, n_loc), pl.ds(0, cap)],
                                     o_snd.at[h], o_rcv.at[h],
                                     device_id={'ep': sib}, device_id_type=MESH).wait_recv()

    depth = CORES * n_loc * slot_pad
    width = min(256, half)
    n_sub = half // width
    tile = min(512, model)
    lane = lax.broadcasted_iota(jnp.int32, (seq_len, depth), 1).astype(jnp.float32)
    block = CORES * seq_len

    def partial(q, ab):
        h = q + n_half * ab

        @pl.when(h != me)
        def _():
            pltpu.make_async_remote_copy(routes.at[h], routes.at[h], t_snd.at[0], t_rcv.at[h],
                                         device_id={'ep': h}, device_id_type=MESH).wait_recv()
        rows = routes[h]
        rows = jnp.concatenate([rows, jnp.zeros((128 - rows.shape[0], tok_dev), jnp.float32)], axis=0)
        table[...] = rows.T
        step = 1 - 2 * ab
        dest = [chip + 2, chip + n_chip + step, chip + n_chip - step, chip]
        picks = []
        for r in range(n_chip):
            for jc in range(CORES):
                j = lax.rem(dest[r], n_chip) * CORES + jc
                pick = 0
                for b in range(n_ep):
                    seq = goes[0, j * n_ep + b] - h * n_ep
                    pick = jnp.where(jnp.logical_and(seq >= 0, seq < n_ep), seq, pick)
                picks.append(pick)

        def chosen(pick, load):
            got = load(0)
            for s in range(1, n_ep):
                got = jnp.where(pick == s, load(s), got)
            return got

        base = (chip * depth).astype(jnp.float32)
        for b, pick in enumerate(picks):
            rt = chosen(pick, lambda s: table[s * seq_len:(s + 1) * seq_len, :])
            w = jnp.zeros((seq_len, depth), jnp.float32)
            for j in range(top_k):
                key = rt[:, j:j + 1] - base
                w = jnp.where(lane == key, rt[:, top_k + j:top_k + j + 1], w)
            hi = w.astype(jnp.bfloat16)
            rest = w - hi.astype(jnp.float32)
            mid = rest.astype(jnp.bfloat16)
            low = (rest - mid.astype(jnp.float32)).astype(jnp.bfloat16)
            for t, term in enumerate((hi, mid, low)):
                wterm[pl.ds(t * tok_dev + b * seq_len, seq_len), :] = term

        dsts = [p1.at[ab, q], p2.at[1 - ab, q], p3.at[ab, lax.rem(q, 2)], own.at[ab, lax.rem(q, 3)]]
        o_wait(h)

        @pl.loop(0, half // width)
        def _(n):
            cols = pl.ds(pl.multiple_of(n * width, width), width)
            slots_in = obuf[h, :, :, cols].reshape(depth, width)
            res = jnp.dot(wterm[...], slots_in, preferred_element_type=jnp.float32)
            res = res[:tok_dev] + (res[tok_dev:2 * tok_dev] + res[2 * tok_dev:])
            for r in range(n_chip):
                dsts[r][:, cols] = res[r * block:(r + 1) * block]

        @pl.when(h // CORES == chip)
        def _():
            hc = lax.rem(h, CORES)

            @pl.when(hc == 0)
            def _():
                h_copy.wait()
                h_out.wait_recv()

            @pl.loop(0, half // width)
            def _(n):
                cols = pl.ds(pl.multiple_of(n * width, width), width)
                for b, pick in enumerate(picks):
                    dst = dsts[b // CORES]
                    rs = slice((b % CORES) * seq_len, (b % CORES + 1) * seq_len)
                    held = chosen(pick, lambda s: hbuf[hc, s * seq_len:(s + 1) * seq_len, cols].astype(jnp.float32))
                    dst[rs, cols] = dst[rs, cols] + held

    def o_out_wait(h):
        pltpu.make_async_remote_copy(out_ref.at[:, pl.ds(0, cap), sib_cols],
                                     obuf.at[h, pl.ds(core * n_loc, n_loc), pl.ds(0, cap)],
                                     o_snd.at[h], o_rcv.at[h],
                                     device_id={'ep': sib}, device_id_type=MESH).wait_send()

    def ring(src, dst, snd, rcv, d, q):
        return pltpu.make_async_remote_copy(src.at[d, q], dst.at[d, q], snd.at[d, q], rcv.at[d, q],
                                            device_id={'ep': side[d]}, device_id_type=MESH)

    def sub(n):
        return pl.ds(pl.multiple_of(n * width, width), width)

    def last_leg(d, q, n):
        return pltpu.make_async_remote_copy(r1.at[d, q, :, sub(n)], r3.at[d, q, :, sub(n)], s3.at[d, q, n], q3.at[d, q, n],
                                            device_id={'ep': side[d]}, device_id_type=MESH)

    def hop(q, jc, n, c, to):
        cols = pl.ds(pl.multiple_of(c * half + n * width, width), width)
        return pltpu.make_async_remote_copy(ysend.at[q, jc, :, :, sub(n)], yland.at[pl.ds(2 * q, 2), :, cols],
                                            ys.at[q, jc, n], yr.at[c, q, n],
                                            device_id={'pp': nxt, 'ep': to}, device_id_type=MESH)

    def finish(q, n):
        @pl.when(n == 0)
        def _():
            for d in range(2):
                ring(p2, r2, s2, q2, d, q).wait_recv()
        cols = sub(n)
        for d in range(2):
            last_leg(d, q, n).wait_recv()
        for ab in range(2):
            total = own[ab, lax.rem(q, 3), :, cols] + (r3[ab, q, :, cols] + r2[1 - ab, q, :, cols])
            rounded = total.astype(jnp.bfloat16)
            for jc in range(CORES):
                ysend[q, jc, ab, :, cols] = rounded[jc * seq_len:(jc + 1) * seq_len]
        for jc in range(CORES):
            hop(q, jc, n, core, chip * CORES + jc).start()

    n_tok = 2 * seq_len
    row = lax.broadcasted_iota(jnp.int32, (n_tok, n_tok), 0)
    col = lax.broadcasted_iota(jnp.int32, (n_tok, n_tok), 1)
    causal = jnp.logical_and(row >= col, row // seq_len == col // seq_len)

    def normalise(q):
        for c in range(CORES):
            for n in range(n_sub):
                hop(q, 0, n, c, me).wait_recv()
        for ab in range(2):
            y = yland[2 * q + ab].astype(jnp.float32)
            inv = lax.rsqrt(jnp.mean(y * y, axis=-1, keepdims=True) + NORM_EPS)
            xs[ab * seq_len:(ab + 1) * seq_len, :] = (y * inv * norm[...]).astype(jnp.bfloat16)

    def attend(n):
        cols = pl.ds(pl.multiple_of(n * tile, tile), tile)
        x = xs[...]
        qt, kt, vt = (jnp.dot(x, w[:, cols], preferred_element_type=jnp.float32).astype(jnp.bfloat16) for w in (wq, wk, wv))
        for hd in range(tile // HEAD_DIM):
            hs = slice(hd * HEAD_DIM, (hd + 1) * HEAD_DIM)
            scores = lax.dot_general(qt[:, hs], kt[:, hs], (((1,), (1,)), ((), ())), preferred_element_type=jnp.float32)
            scores = jnp.where(causal, scores * (HEAD_DIM ** -0.5), -1e30)
            raised = jnp.exp(scores - jnp.max(scores, axis=-1, keepdims=True))
            probs = (raised / jnp.sum(raised, axis=-1, keepdims=True)).astype(jnp.bfloat16)
            mixed = jnp.dot(probs, vt[:, hs], preferred_element_type=jnp.float32).astype(jnp.bfloat16)
            mix[:, pl.ds(pl.multiple_of(n * tile + hd * HEAD_DIM, HEAD_DIM), HEAD_DIM)] = mixed

    def project(q):
        @pl.loop(0, model // tile)
        def _(n):
            cols = pl.ds(pl.multiple_of(n * tile, tile), tile)
            out = jnp.dot(mix[...], wo[:, cols], preferred_element_type=jnp.float32).astype(jnp.bfloat16).astype(jnp.float32)
            for ab in range(2):
                y = yland[2 * q + ab, :, cols].astype(jnp.float32)
                yland[2 * q + ab, :, cols] = (y + out[ab * seq_len:(ab + 1) * seq_len]).astype(jnp.bfloat16)

    def store(q):
        return pltpu.make_async_copy(yland.at[pl.ds(2 * q, 2)], z_ref.at[pl.ds(2 * q, 2)], zs.at[q])

    @pl.loop(0, n_half + 3)
    def _(it):
        @pl.when(it < n_half)
        def _():
            @pl.loop(0, 2)
            def _(ab):
                partial(it, ab)
                for d in range(2):
                    @pl.when(ab == d)
                    def _():
                        ring(p1, r1, s1, q1, d, it).start()

                        @pl.when(it == 0)
                        def _():
                            ring(p2, r2, s2, q2, 1 - d, it).start()

        @pl.when(jnp.logical_and(it >= 1, it <= n_half))
        def _():
            q = it - 1
            for d in range(2):
                ring(p1, r1, s1, q1, d, q).wait_recv()
                r1[d, q] = p3[d, lax.rem(q, 2)] + r1[d, q]
                for n in range(n_sub):
                    last_leg(d, q, n).start()

        @pl.when(jnp.logical_and(it >= 1, it < n_half))
        def _():
            for d in range(2):
                ring(p2, r2, s2, q2, d, it).start()

        for i in range(1, 4):
            @pl.when(it == i - 1)
            def _():
                for part in range(n_half):
                    weight(i, part).start()

        @pl.when(it == 3)
        def _():
            norm_copy.wait()
            for i in range(3):
                for part in range(n_half):
                    weight(i, part).wait()

        @pl.when(it >= 3)
        def _():
            normalise(it - 3)

        @pl.loop(0, n_sub)
        def _(n):
            @pl.when(it >= 3)
            def _():
                attend(n)

            @pl.when(jnp.logical_and(it >= 2, it < n_half + 2))
            def _():
                finish(it - 2, n)

        @pl.when(it == 3)
        def _():
            for part in range(n_half):
                weight(3, part).wait()

        @pl.when(it == n_half)
        def _():
            w_out.wait_send()
            h_out.wait_send()
            for copy in t_out:
                copy.wait_send()

            @pl.loop(0, n_ep)
            def _(h):
                o_out_wait(h)

        @pl.when(it >= 3)
        def _():
            project(it - 3)
            store(it - 3).start()

    @pl.loop(0, n_half)
    def _(q):
        for d in range(2):
            ring(p1, r1, s1, q1, d, q).wait_send()
            ring(p2, r2, s2, q2, d, q).wait_send()
            for n in range(n_sub):
                last_leg(d, q, n).wait_send()
        for jc in range(CORES):
            for n in range(n_sub):
                hop(q, jc, n, core, chip * CORES + jc).wait_send()
        store(q).wait()


def solution(mesh):
    n_stages = mesh.shape['pp']
    n_ep = mesh.shape['ep']
    group_axes = ('data', 'pp')

    def device_step(expert_out, expert_id, slot_id, gate, resid, owner, norm_w, w_q, w_k, w_v, w_o):
        dev_index = lax.axis_index('ep')
        n_loc, capacity, model_dim = expert_out.shape[2:]
        cap = capacity // n_ep
        tok_dev, top_k = expert_id.shape[2:]
        seq_dev = owner.shape[1] // n_ep
        seq_len = tok_dev // seq_dev
        assert expert_out.shape[1] == 1 and seq_dev == n_ep
        half = model_dim // CORES
        slot_pad = -(-cap // 16) * 16
        n_half = n_ep // 2
        block = CORES * seq_len

        dims = (n_ep, n_stages, n_loc, cap, slot_pad, seq_len, top_k, half)
        f32, bf16 = jnp.float32, jnp.bfloat16
        n_sub = half // min(256, half)
        assert model_dim // min(512, model_dim) == n_sub and n_half > 3

        def ringbuf(slots):
            return pltpu.VMEM((2, slots, block, half), f32)

        square = pltpu.VMEM((model_dim, model_dim), bf16)
        dma = pltpu.SemaphoreType.DMA
        z_pairs = pl.pallas_call(
            functools.partial(stage_kernel, dims),
            out_shape=jax.ShapeDtypeStruct((n_ep, seq_len, model_dim), bf16),
            in_specs=[pl.BlockSpec(memory_space=pl.ANY)] * 11,
            out_specs=pl.BlockSpec(memory_space=pl.ANY),
            scratch_shapes=[
                pltpu.VMEM((n_ep, CORES * n_loc, slot_pad, half), bf16),
                pltpu.VMEM((CORES, tok_dev, half), bf16),
                pltpu.VMEM((n_ep, 2 * top_k, tok_dev), f32),
                pltpu.VMEM((top_k, tok_dev), jnp.int32),
                pltpu.VMEM((top_k, tok_dev), jnp.int32),
                pltpu.VMEM((top_k, tok_dev), f32),
                pltpu.VMEM((1, n_ep * seq_dev), jnp.int32),
                pltpu.SMEM((1, n_ep * seq_dev), jnp.int32),
                pltpu.VMEM((tok_dev, 128), f32),
                pltpu.VMEM((3 * tok_dev, CORES * n_loc * slot_pad), bf16),
                ringbuf(n_half), ringbuf(n_half), ringbuf(2), ringbuf(n_half), ringbuf(n_half), ringbuf(n_half), ringbuf(3),
                pltpu.VMEM((n_half, CORES, 2, seq_len, half), bf16),
                pltpu.VMEM((n_ep, seq_len, model_dim), bf16),
                pltpu.VMEM((1, model_dim), f32),
                square, square, square, square,
                pltpu.VMEM((2 * seq_len, model_dim), bf16),
                pltpu.VMEM((2 * seq_len, model_dim), bf16),
                dma((n_ep,)), dma((n_ep,)), dma((n_ep,)),
                dma, dma, dma,
                dma((3,)), dma((n_ep - 1,)), dma((n_ep,)),
                dma, dma, dma,
                dma((2, n_half)), dma((2, n_half)), dma((2, n_half, n_sub)),
                dma((2, n_half)), dma((2, n_half)), dma((2, n_half, n_sub)),
                dma((n_half, CORES, n_sub)), dma((CORES, n_half, n_sub)), dma((4, n_half)), dma((n_half,)), dma,
            ],
            compiler_params=pltpu.CompilerParams(collective_id=0, has_side_effects=True, vmem_limit_bytes=67043328),
            name='stage',
        )(owner, expert_id[0, 0].T, slot_id[0, 0].T, gate[0, 0].T, expert_out[0, 0], resid[0, 0],
          norm_w, w_q[0], w_k[0], w_v[0], w_o[0])
        source = lax.dynamic_slice_in_dim(owner[0], dev_index * seq_dev, seq_dev) // seq_dev
        z_owned = z_pairs.at[source % n_half * 2 + source // n_half].get(mode='promise_in_bounds', unique_indices=True)
        return z_owned.reshape(1, 1, tok_dev, model_dim)

    tok_spec = P(group_axes, None, 'ep', None)
    weight_spec = P('pp', None, None)
    in_specs = (P(group_axes, None, 'ep', None, None), tok_spec, tok_spec, tok_spec, tok_spec, P(group_axes, None), P('pp', None), weight_spec, weight_spec, weight_spec, weight_spec)
    return jax.shard_map(device_step, mesh=mesh, in_specs=in_specs, out_specs=tok_spec, check_vma=False)
```

```python
import functools

import jax
import jax.numpy as jnp
from jax import lax
from jax.experimental import pallas as pl
from jax.experimental.pallas import tpu as pltpu
from jax.sharding import PartitionSpec as P

HEAD_DIM = 128
NORM_EPS = 1e-6
MESH = pl.DeviceIdType.MESH
CORES = 2
LEGS = 1


def stage_kernel(dims, owner_ref, id_ref, slot_ref, gate_ref, out_ref, resid_ref, norm_ref, q_ref, k_ref, v_ref, o_ref, z_ref,
                   obuf, hbuf, routes, ids, slots, gates, owners, goes, table, wterm,
                   p1, p2, p3, r1, r2, r3, own, ysend, yland, norm, wq, wk, wv, wo, xs, mix,
                   o_loc, o_snd, o_rcv, h_loc, h_snd, h_rcv, t_loc, t_snd, t_rcv, w_snd, w_rcv, w_loc,
                   s1, s2, s3, q1, q2, q3, ys, yr, wt, zs, n_loc_sem):
    n_ep, n_st, n_loc, cap, slot_pad, seq_len, top_k, half = dims
    n_chip = n_ep // CORES
    n_half = n_ep // 2
    tok_dev = n_ep * seq_len
    me = lax.axis_index('ep')
    rank = lax.axis_index('pp')
    core = lax.rem(me, CORES)
    chip = me // CORES
    sib = me + 1 - 2 * core
    nxt = lax.rem(rank + 1, n_st)
    prv = lax.rem(rank + n_st - 1, n_st)
    side = [lax.rem(me + n_ep - CORES, n_ep), lax.rem(me + CORES, n_ep)]
    my_cols = pl.ds(pl.multiple_of(core * half, 128), half)
    sib_cols = pl.ds(pl.multiple_of((1 - core) * half, 128), half)
    order = [q + n_half * ab for q in range(n_half) for ab in range(2)]

    small = [pltpu.make_async_copy(src, dst, t_loc.at[i])
             for i, (src, dst) in enumerate(((id_ref, ids), (slot_ref, slots), (gate_ref, gates)))]
    for copy in small:
        copy.start()
    barrier = pltpu.get_barrier_semaphore()
    for k in range(1, n_ep):
        pl.semaphore_signal(barrier, inc=1, device_id={'ep': lax.rem(me + k, n_ep)}, device_id_type=MESH)
    for other in (nxt, prv):
        for jc in range(CORES):
            pl.semaphore_signal(barrier, inc=1, device_id={'pp': other, 'ep': chip * CORES + jc}, device_id_type=MESH)
    for h in order:
        pltpu.make_async_copy(out_ref.at[:, pl.ds(h * cap, cap), my_cols],
                              obuf.at[h, pl.ds(core * n_loc, n_loc), pl.ds(0, cap)], o_loc.at[h]).start()
    h_copy = pltpu.make_async_copy(resid_ref.at[:, my_cols], hbuf.at[core], h_loc)
    h_copy.start()
    model = CORES * half
    strip = model // n_half

    def weight(i, part):
        src, dst = ((q_ref, wq), (k_ref, wk), (v_ref, wv), (o_ref, wo))[i]
        rows = pl.ds(part * strip, strip)
        return pltpu.make_async_copy(src.at[rows], dst.at[rows], wt.at[i, part])

    norm_copy = pltpu.make_async_copy(norm_ref, norm, n_loc_sem)
    norm_copy.start()
    for part in range(n_half):
        weight(0, part).start()
    for copy in small:
        copy.wait()
    key = jnp.where(slots[...] >= 0, ids[...] * slot_pad + slots[...] - me * cap, -1)
    routes[me, :top_k] = key.astype(jnp.float32)
    routes[me, top_k:] = gates[...]
    if slot_pad > cap:
        for h in range(n_ep):
            obuf[h, :, cap:, :] = jnp.zeros((CORES * n_loc, slot_pad - cap, half), jnp.bfloat16)
    pl.semaphore_wait(barrier, n_ep - 1 + 2 * CORES)

    w_out = pltpu.make_async_remote_copy(owner_ref, owners, w_snd, w_rcv, device_id={'pp': prv}, device_id_type=MESH)
    w_out.start()
    t_out = []
    for k in (n_chip, n_chip - 1, n_chip + 1, 2, n_ep - 2, 1, n_ep - 1):
        peer = lax.rem(me + k, n_ep)
        t_out.append(pltpu.make_async_remote_copy(routes.at[me], routes.at[me], t_snd.at[k - 1], t_rcv.at[me],
                                                  device_id={'ep': peer}, device_id_type=MESH))
        t_out[-1].start()

    def o_out(h):
        return pltpu.make_async_remote_copy(out_ref.at[:, pl.ds(h * cap, cap), sib_cols],
                                            obuf.at[h, pl.ds(core * n_loc, n_loc), pl.ds(0, cap)],
                                            o_snd.at[h], o_rcv.at[h],
                                            device_id={'ep': sib}, device_id_type=MESH)

    h_out = pltpu.make_async_remote_copy(resid_ref.at[:, sib_cols], hbuf.at[core], h_snd, h_rcv,
                                         device_id={'ep': sib}, device_id_type=MESH)
    for i, h in enumerate(order):
        o_out(h).start()
        if i == 1:
            h_out.start()

    w_out.wait_recv()
    goes_copy = pltpu.make_async_copy(owners, goes, w_loc)
    goes_copy.start()
    goes_copy.wait()

    def o_wait(h):
        pltpu.make_async_copy(out_ref.at[:, pl.ds(0, cap), my_cols],
                              obuf.at[h, pl.ds(core * n_loc, n_loc), pl.ds(0, cap)], o_loc.at[h]).wait()
        pltpu.make_async_remote_copy(out_ref.at[:, pl.ds(0, cap), sib_cols],
                                     obuf.at[h, pl.ds((1 - core) * n_loc, n_loc), pl.ds(0, cap)],
                                     o_snd.at[h], o_rcv.at[h],
                                     device_id={'ep': sib}, device_id_type=MESH).wait_recv()

    depth = CORES * n_loc * slot_pad
    width = min(256, half)
    leg = half // LEGS
    tile = min(512, model)
    lane = lax.broadcasted_iota(jnp.int32, (seq_len, depth), 1).astype(jnp.float32)
    block = CORES * seq_len

    def partial(q, ab):
        h = q + n_half * ab

        @pl.when(h != me)
        def _():
            pltpu.make_async_remote_copy(routes.at[h], routes.at[h], t_snd.at[0], t_rcv.at[h],
                                         device_id={'ep': h}, device_id_type=MESH).wait_recv()
        rows = routes[h]
        rows = jnp.concatenate([rows, jnp.zeros((128 - rows.shape[0], tok_dev), jnp.float32)], axis=0)
        table[...] = rows.T
        step = 1 - 2 * ab
        dest = [chip + 2, chip + n_chip + step, chip + n_chip - step, chip]
        picks = []
        for r in range(n_chip):
            for jc in range(CORES):
                j = lax.rem(dest[r], n_chip) * CORES + jc
                pick = 0
                for b in range(n_ep):
                    seq = goes[0, j * n_ep + b] - h * n_ep
                    pick = jnp.where(jnp.logical_and(seq >= 0, seq < n_ep), seq, pick)
                picks.append(pick)

        def chosen(pick, load):
            got = load(0)
            for s in range(1, n_ep):
                got = jnp.where(pick == s, load(s), got)
            return got

        base = (chip * depth).astype(jnp.float32)
        for b, pick in enumerate(picks):
            rt = chosen(pick, lambda s: table[s * seq_len:(s + 1) * seq_len, :])
            w = jnp.zeros((seq_len, depth), jnp.float32)
            for j in range(top_k):
                key = rt[:, j:j + 1] - base
                w = jnp.where(lane == key, rt[:, top_k + j:top_k + j + 1], w)
            hi = w.astype(jnp.bfloat16)
            rest = w - hi.astype(jnp.float32)
            mid = rest.astype(jnp.bfloat16)
            low = (rest - mid.astype(jnp.float32)).astype(jnp.bfloat16)
            for t, term in enumerate((hi, mid, low)):
                wterm[pl.ds(t * tok_dev + b * seq_len, seq_len), :] = term

        dsts = [p1.at[ab, q], p2.at[1 - ab, q], p3.at[ab, lax.rem(q, 2)], own.at[ab, lax.rem(q, 3)]]
        o_wait(h)

        @pl.loop(0, half // width)
        def _(n):
            cols = pl.ds(pl.multiple_of(n * width, width), width)
            slots_in = obuf[h, :, :, cols].reshape(depth, width)
            res = jnp.dot(wterm[...], slots_in, preferred_element_type=jnp.float32)
            res = res[:tok_dev] + (res[tok_dev:2 * tok_dev] + res[2 * tok_dev:])
            for r in range(n_chip):
                dsts[r][:, cols] = res[r * block:(r + 1) * block]

        @pl.when(h // CORES == chip)
        def _():
            hc = lax.rem(h, CORES)

            @pl.when(hc == 0)
            def _():
                h_copy.wait()
                h_out.wait_recv()

            @pl.loop(0, half // width)
            def _(n):
                cols = pl.ds(pl.multiple_of(n * width, width), width)
                for b, pick in enumerate(picks):
                    dst = dsts[b // CORES]
                    rs = slice((b % CORES) * seq_len, (b % CORES + 1) * seq_len)
                    held = chosen(pick, lambda s: hbuf[hc, s * seq_len:(s + 1) * seq_len, cols].astype(jnp.float32))
                    dst[rs, cols] = dst[rs, cols] + held

    def o_out_wait(h):
        pltpu.make_async_remote_copy(out_ref.at[:, pl.ds(0, cap), sib_cols],
                                     obuf.at[h, pl.ds(core * n_loc, n_loc), pl.ds(0, cap)],
                                     o_snd.at[h], o_rcv.at[h],
                                     device_id={'ep': sib}, device_id_type=MESH).wait_send()

    def ring(src, dst, snd, rcv, d, q):
        return pltpu.make_async_remote_copy(src.at[d, q], dst.at[d, q], snd.at[d, q], rcv.at[d, q],
                                            device_id={'ep': side[d]}, device_id_type=MESH)

    def sub(n):
        return pl.ds(pl.multiple_of(n * leg, leg), leg)

    def last_leg(d, q, n):
        return pltpu.make_async_remote_copy(r1.at[d, q, :, sub(n)], r3.at[d, q, :, sub(n)], s3.at[d, q, n], q3.at[d, q, n],
                                            device_id={'ep': side[d]}, device_id_type=MESH)

    def hop(q, jc, n, c, to):
        cols = pl.ds(pl.multiple_of(c * half + n * leg, leg), leg)
        return pltpu.make_async_remote_copy(ysend.at[q, jc, :, :, sub(n)], yland.at[pl.ds(2 * q, 2), :, cols],
                                            ys.at[q, jc, n], yr.at[c, q, n],
                                            device_id={'pp': nxt, 'ep': to}, device_id_type=MESH)

    def finish(q, n):
        @pl.when(n == 0)
        def _():
            for d in range(2):
                ring(p2, r2, s2, q2, d, q).wait_recv()
        cols = sub(n)
        for d in range(2):
            last_leg(d, q, n).wait_recv()
        for ab in range(2):
            total = own[ab, lax.rem(q, 3), :, cols] + (r3[ab, q, :, cols] + r2[1 - ab, q, :, cols])
            rounded = total.astype(jnp.bfloat16)
            for jc in range(CORES):
                ysend[q, jc, ab, :, cols] = rounded[jc * seq_len:(jc + 1) * seq_len]
        for jc in range(CORES):
            hop(q, jc, n, core, chip * CORES + jc).start()

    n_tok = 2 * seq_len
    row = lax.broadcasted_iota(jnp.int32, (n_tok, n_tok), 0)
    col = lax.broadcasted_iota(jnp.int32, (n_tok, n_tok), 1)
    causal = jnp.logical_and(row >= col, row // seq_len == col // seq_len)

    def normalise(q):
        for c in range(CORES):
            for n in range(LEGS):
                hop(q, 0, n, c, me).wait_recv()
        for ab in range(2):
            y = yland[2 * q + ab].astype(jnp.float32)
            inv = lax.rsqrt(jnp.mean(y * y, axis=-1, keepdims=True) + NORM_EPS)
            xs[ab * seq_len:(ab + 1) * seq_len, :] = (y * inv * norm[...]).astype(jnp.bfloat16)

    def attend(n):
        cols = pl.ds(pl.multiple_of(n * tile, tile), tile)
        x = xs[...]
        qt, kt, vt = (jnp.dot(x, w[:, cols], preferred_element_type=jnp.float32).astype(jnp.bfloat16) for w in (wq, wk, wv))
        for hd in range(tile // HEAD_DIM):
            hs = slice(hd * HEAD_DIM, (hd + 1) * HEAD_DIM)
            scores = lax.dot_general(qt[:, hs], kt[:, hs], (((1,), (1,)), ((), ())), preferred_element_type=jnp.float32)
            scores = jnp.where(causal, scores * (HEAD_DIM ** -0.5), -1e30)
            raised = jnp.exp(scores - jnp.max(scores, axis=-1, keepdims=True))
            probs = (raised / jnp.sum(raised, axis=-1, keepdims=True)).astype(jnp.bfloat16)
            mixed = jnp.dot(probs, vt[:, hs], preferred_element_type=jnp.float32).astype(jnp.bfloat16)
            mix[:, pl.ds(pl.multiple_of(n * tile + hd * HEAD_DIM, HEAD_DIM), HEAD_DIM)] = mixed

    def project(q):
        @pl.loop(0, model // tile)
        def _(n):
            cols = pl.ds(pl.multiple_of(n * tile, tile), tile)
            out = jnp.dot(mix[...], wo[:, cols], preferred_element_type=jnp.float32).astype(jnp.bfloat16).astype(jnp.float32)
            for ab in range(2):
                y = yland[2 * q + ab, :, cols].astype(jnp.float32)
                yland[2 * q + ab, :, cols] = (y + out[ab * seq_len:(ab + 1) * seq_len]).astype(jnp.bfloat16)

    def store(q):
        return pltpu.make_async_copy(yland.at[pl.ds(2 * q, 2)], z_ref.at[pl.ds(2 * q, 2)], zs.at[q])

    @pl.loop(0, n_half + 3)
    def _(it):
        @pl.when(it < n_half)
        def _():
            @pl.loop(0, 2)
            def _(ab):
                partial(it, ab)
                for d in range(2):
                    @pl.when(ab == d)
                    def _():
                        ring(p1, r1, s1, q1, d, it).start()

                        @pl.when(it == 0)
                        def _():
                            ring(p2, r2, s2, q2, 1 - d, it).start()

        @pl.when(jnp.logical_and(it >= 1, it <= n_half))
        def _():
            q = it - 1
            for d in range(2):
                ring(p1, r1, s1, q1, d, q).wait_recv()
                r1[d, q] = p3[d, lax.rem(q, 2)] + r1[d, q]
                for n in range(LEGS):
                    last_leg(d, q, n).start()

        @pl.when(jnp.logical_and(it >= 1, it < n_half))
        def _():
            for d in range(2):
                ring(p2, r2, s2, q2, d, it).start()

        for i in range(1, 4):
            @pl.when(it == i - 1)
            def _():
                for part in range(n_half):
                    weight(i, part).start()

        @pl.when(it == 3)
        def _():
            norm_copy.wait()
            for i in range(3):
                for part in range(n_half):
                    weight(i, part).wait()

        @pl.when(it >= 3)
        def _():
            normalise(it - 3)

        @pl.when(it >= 3)
        def _():
            @pl.loop(0, model // tile)
            def _(n):
                attend(n)

        @pl.when(jnp.logical_and(it >= 2, it < n_half + 2))
        def _():
            @pl.loop(0, LEGS)
            def _(n):
                finish(it - 2, n)

        @pl.when(it == 3)
        def _():
            for part in range(n_half):
                weight(3, part).wait()

        @pl.when(it == n_half)
        def _():
            w_out.wait_send()
            h_out.wait_send()
            for copy in t_out:
                copy.wait_send()

            @pl.loop(0, n_ep)
            def _(h):
                o_out_wait(h)

        @pl.when(it >= 3)
        def _():
            project(it - 3)
            store(it - 3).start()

    @pl.loop(0, n_half)
    def _(q):
        for d in range(2):
            ring(p1, r1, s1, q1, d, q).wait_send()
            ring(p2, r2, s2, q2, d, q).wait_send()
            for n in range(LEGS):
                last_leg(d, q, n).wait_send()
        for jc in range(CORES):
            for n in range(LEGS):
                hop(q, jc, n, core, chip * CORES + jc).wait_send()
        store(q).wait()


def solution(mesh):
    n_stages = mesh.shape['pp']
    n_ep = mesh.shape['ep']
    group_axes = ('data', 'pp')

    def device_step(expert_out, expert_id, slot_id, gate, resid, owner, norm_w, w_q, w_k, w_v, w_o):
        dev_index = lax.axis_index('ep')
        n_loc, capacity, model_dim = expert_out.shape[2:]
        cap = capacity // n_ep
        tok_dev, top_k = expert_id.shape[2:]
        seq_dev = owner.shape[1] // n_ep
        seq_len = tok_dev // seq_dev
        assert expert_out.shape[1] == 1 and seq_dev == n_ep
        half = model_dim // CORES
        slot_pad = -(-cap // 16) * 16
        n_half = n_ep // 2
        block = CORES * seq_len

        dims = (n_ep, n_stages, n_loc, cap, slot_pad, seq_len, top_k, half)
        f32, bf16 = jnp.float32, jnp.bfloat16
        assert n_half > 3

        def ringbuf(slots):
            return pltpu.VMEM((2, slots, block, half), f32)

        square = pltpu.VMEM((model_dim, model_dim), bf16)
        dma = pltpu.SemaphoreType.DMA
        z_pairs = pl.pallas_call(
            functools.partial(stage_kernel, dims),
            out_shape=jax.ShapeDtypeStruct((n_ep, seq_len, model_dim), bf16),
            in_specs=[pl.BlockSpec(memory_space=pl.ANY)] * 11,
            out_specs=pl.BlockSpec(memory_space=pl.ANY),
            scratch_shapes=[
                pltpu.VMEM((n_ep, CORES * n_loc, slot_pad, half), bf16),
                pltpu.VMEM((CORES, tok_dev, half), bf16),
                pltpu.VMEM((n_ep, 2 * top_k, tok_dev), f32),
                pltpu.VMEM((top_k, tok_dev), jnp.int32),
                pltpu.VMEM((top_k, tok_dev), jnp.int32),
                pltpu.VMEM((top_k, tok_dev), f32),
                pltpu.VMEM((1, n_ep * seq_dev), jnp.int32),
                pltpu.SMEM((1, n_ep * seq_dev), jnp.int32),
                pltpu.VMEM((tok_dev, 128), f32),
                pltpu.VMEM((3 * tok_dev, CORES * n_loc * slot_pad), bf16),
                ringbuf(n_half), ringbuf(n_half), ringbuf(2), ringbuf(n_half), ringbuf(n_half), ringbuf(n_half), ringbuf(3),
                pltpu.VMEM((n_half, CORES, 2, seq_len, half), bf16),
                pltpu.VMEM((n_ep, seq_len, model_dim), bf16),
                pltpu.VMEM((1, model_dim), f32),
                square, square, square, square,
                pltpu.VMEM((2 * seq_len, model_dim), bf16),
                pltpu.VMEM((2 * seq_len, model_dim), bf16),
                dma((n_ep,)), dma((n_ep,)), dma((n_ep,)),
                dma, dma, dma,
                dma((3,)), dma((n_ep - 1,)), dma((n_ep,)),
                dma, dma, dma,
                dma((2, n_half)), dma((2, n_half)), dma((2, n_half, LEGS)),
                dma((2, n_half)), dma((2, n_half)), dma((2, n_half, LEGS)),
                dma((n_half, CORES, LEGS)), dma((CORES, n_half, LEGS)), dma((4, n_half)), dma((n_half,)), dma,
            ],
            compiler_params=pltpu.CompilerParams(collective_id=0, has_side_effects=True, vmem_limit_bytes=67043328),
            name='stage',
        )(owner, expert_id[0, 0].T, slot_id[0, 0].T, gate[0, 0].T, expert_out[0, 0], resid[0, 0],
          norm_w, w_q[0], w_k[0], w_v[0], w_o[0])
        source = lax.dynamic_slice_in_dim(owner[0], dev_index * seq_dev, seq_dev) // seq_dev
        z_owned = z_pairs.at[source % n_half * 2 + source // n_half].get(mode='promise_in_bounds', unique_indices=True)
        return z_owned.reshape(1, 1, tok_dev, model_dim)

    tok_spec = P(group_axes, None, 'ep', None)
    weight_spec = P('pp', None, None)
    in_specs = (P(group_axes, None, 'ep', None, None), tok_spec, tok_spec, tok_spec, tok_spec, P(group_axes, None), P('pp', None), weight_spec, weight_spec, weight_spec, weight_spec)
    return jax.shard_map(device_step, mesh=mesh, in_specs=in_specs, out_specs=tok_spec, check_vma=False)
```

```python
import functools

import jax
import jax.numpy as jnp
from jax import lax
from jax.experimental import pallas as pl
from jax.experimental.pallas import tpu as pltpu
from jax.sharding import PartitionSpec as P

HEAD_DIM = 128
NORM_EPS = 1e-6
MESH = pl.DeviceIdType.MESH
CORES = 2


def stage_kernel(dims, owner_ref, id_ref, slot_ref, gate_ref, out_ref, resid_ref, norm_ref, q_ref, k_ref, v_ref, o_ref, z_ref,
                   obuf, hbuf, routes, ids, slots, gates, owners, goes, comes, table, wterm,
                   p1, p2, p3, r1, r2, r3, own, ysend, yland, norm, wq, wk, wv, wo, xs, mix,
                   o_loc, o_snd, o_rcv, h_loc, h_snd, h_rcv, t_loc, t_snd, t_rcv, w_snd, w_rcv, w_loc,
                   s1, s2, s3, q1, q2, q3, ys, yr, wt, zs, n_loc_sem, c_loc):
    n_ep, n_st, n_loc, cap, slot_pad, seq_len, top_k, half = dims
    n_chip = n_ep // CORES
    n_half = n_ep // 2
    tok_dev = n_ep * seq_len
    me = lax.axis_index('ep')
    rank = lax.axis_index('pp')
    core = lax.rem(me, CORES)
    chip = me // CORES
    sib = me + 1 - 2 * core
    nxt = lax.rem(rank + 1, n_st)
    prv = lax.rem(rank + n_st - 1, n_st)
    side = [lax.rem(me + n_ep - CORES, n_ep), lax.rem(me + CORES, n_ep)]
    my_cols = pl.ds(pl.multiple_of(core * half, 128), half)
    sib_cols = pl.ds(pl.multiple_of((1 - core) * half, 128), half)
    order = [q + n_half * ab for q in range(n_half) for ab in range(2)]

    small = [pltpu.make_async_copy(src, dst, t_loc.at[i])
             for i, (src, dst) in enumerate(((id_ref, ids), (slot_ref, slots), (gate_ref, gates)))]
    for copy in small:
        copy.start()
    barrier = pltpu.get_barrier_semaphore()
    for k in range(1, n_ep):
        pl.semaphore_signal(barrier, inc=1, device_id={'ep': lax.rem(me + k, n_ep)}, device_id_type=MESH)
    for other in (nxt, prv):
        for jc in range(CORES):
            pl.semaphore_signal(barrier, inc=1, device_id={'pp': other, 'ep': chip * CORES + jc}, device_id_type=MESH)
    for h in order:
        pltpu.make_async_copy(out_ref.at[:, pl.ds(h * cap, cap), my_cols],
                              obuf.at[h, pl.ds(core * n_loc, n_loc), pl.ds(0, cap)], o_loc.at[h]).start()
    h_copy = pltpu.make_async_copy(resid_ref.at[:, my_cols], hbuf.at[core], h_loc)
    h_copy.start()
    model = CORES * half
    strip = model // n_half

    def weight(i, part):
        src, dst = ((q_ref, wq), (k_ref, wk), (v_ref, wv), (o_ref, wo))[i]
        rows = pl.ds(part * strip, strip)
        return pltpu.make_async_copy(src.at[rows], dst.at[rows], wt.at[i, part])

    norm_copy = pltpu.make_async_copy(norm_ref, norm, n_loc_sem)
    norm_copy.start()
    comes_copy = pltpu.make_async_copy(owner_ref, comes, c_loc)
    comes_copy.start()
    for copy in small:
        copy.wait()
    key = jnp.where(slots[...] >= 0, ids[...] * slot_pad + slots[...] - me * cap, -1)
    routes[me, :top_k] = key.astype(jnp.float32)
    routes[me, top_k:] = gates[...]
    if slot_pad > cap:
        for h in range(n_ep):
            obuf[h, :, cap:, :] = jnp.zeros((CORES * n_loc, slot_pad - cap, half), jnp.bfloat16)
    pl.semaphore_wait(barrier, n_ep - 1 + 2 * CORES)

    w_out = pltpu.make_async_remote_copy(owner_ref, owners, w_snd, w_rcv, device_id={'pp': prv}, device_id_type=MESH)
    w_out.start()
    t_out = []
    for k in (n_chip, n_chip - 1, n_chip + 1, 2, n_ep - 2, 1, n_ep - 1):
        peer = lax.rem(me + k, n_ep)
        t_out.append(pltpu.make_async_remote_copy(routes.at[me], routes.at[me], t_snd.at[k - 1], t_rcv.at[me],
                                                  device_id={'ep': peer}, device_id_type=MESH))
        t_out[-1].start()

    def o_out(h):
        return pltpu.make_async_remote_copy(out_ref.at[:, pl.ds(pl.multiple_of(h * cap, 8), cap), sib_cols],
                                            obuf.at[h, pl.ds(core * n_loc, n_loc), pl.ds(0, cap)],
                                            o_snd.at[h], o_rcv.at[h],
                                            device_id={'ep': sib}, device_id_type=MESH)

    h_out = pltpu.make_async_remote_copy(resid_ref.at[:, sib_cols], hbuf.at[core], h_snd, h_rcv,
                                         device_id={'ep': sib}, device_id_type=MESH)
    for ab in range(2):
        o_out(n_half * ab).start()
    h_out.start()

    w_out.wait_recv()
    goes_copy = pltpu.make_async_copy(owners, goes, w_loc)
    goes_copy.start()
    goes_copy.wait()

    def o_wait(h):
        pltpu.make_async_copy(out_ref.at[:, pl.ds(0, cap), my_cols],
                              obuf.at[h, pl.ds(core * n_loc, n_loc), pl.ds(0, cap)], o_loc.at[h]).wait()
        pltpu.make_async_remote_copy(out_ref.at[:, pl.ds(0, cap), sib_cols],
                                     obuf.at[h, pl.ds((1 - core) * n_loc, n_loc), pl.ds(0, cap)],
                                     o_snd.at[h], o_rcv.at[h],
                                     device_id={'ep': sib}, device_id_type=MESH).wait_recv()

    def ring(src, dst, snd, rcv, d, q):
        return pltpu.make_async_remote_copy(src.at[d, q], dst.at[d, q], snd.at[d, q], rcv.at[d, q],
                                            device_id={'ep': side[d]}, device_id_type=MESH)

    depth = CORES * n_loc * slot_pad
    width = min(256, half)
    tile = min(512, half)
    n_sub = model // tile
    leg = half // n_sub
    lane = lax.broadcasted_iota(jnp.int32, (seq_len, depth), 1).astype(jnp.float32)
    block = CORES * seq_len
    per = n_chip * CORES // 2

    def partial(q, ab):
        h = q + n_half * ab

        @pl.when(h != me)
        def _():
            pltpu.make_async_remote_copy(routes.at[h], routes.at[h], t_snd.at[0], t_rcv.at[h],
                                         device_id={'ep': h}, device_id_type=MESH).wait_recv()
        rows = routes[h]
        rows = jnp.concatenate([rows, jnp.zeros((128 - rows.shape[0], tok_dev), jnp.float32)], axis=0)
        table[...] = rows.T
        step = 1 - 2 * ab
        dest = [chip + 2, chip + n_chip + step, chip + n_chip - step, chip]
        picks = []
        for r in range(n_chip):
            for jc in range(CORES):
                j = lax.rem(dest[r], n_chip) * CORES + jc
                pick = 0
                for b in range(n_ep):
                    seq = goes[0, j * n_ep + b] - h * n_ep
                    pick = jnp.where(jnp.logical_and(seq >= 0, seq < n_ep), seq, pick)
                picks.append(pick)

        def chosen(pick, load):
            got = load(0)
            for s in range(1, n_ep):
                got = jnp.where(pick == s, load(s), got)
            return got

        base = (chip * depth).astype(jnp.float32)
        dsts = [p1.at[ab, q], p2.at[1 - ab, q], p3.at[ab, lax.rem(q, 2)], own.at[ab, lax.rem(q, 3)]]
        for part in range(2):
            mine = picks[part * per:(part + 1) * per]
            for b, pick in enumerate(mine):
                rt = chosen(pick, lambda s: table[s * seq_len:(s + 1) * seq_len, :])
                w = jnp.zeros((seq_len, depth), jnp.float32)
                for j in range(top_k):
                    key = rt[:, j:j + 1] - base
                    w = jnp.where(lane == key, rt[:, top_k + j:top_k + j + 1], w)
                hi = w.astype(jnp.bfloat16)
                rest = w - hi.astype(jnp.float32)
                mid = rest.astype(jnp.bfloat16)
                low = (rest - mid.astype(jnp.float32)).astype(jnp.bfloat16)
                for t, term in enumerate((hi, mid, low)):
                    wterm[pl.ds((t * per + b) * seq_len, seq_len), :] = term
            if part == 0:
                o_wait(h)

            @pl.loop(0, half // width)
            def _(n):
                cols = pl.ds(pl.multiple_of(n * width, width), width)
                slots_in = obuf[h, :, :, cols].reshape(depth, width)
                res = jnp.dot(wterm[...], slots_in, preferred_element_type=jnp.float32)
                span = per * seq_len
                res = res[:span] + (res[span:2 * span] + res[2 * span:])
                for r in range(2):
                    dsts[2 * part + r][:, cols] = res[r * block:(r + 1) * block]

            @pl.when(h // CORES == chip)
            def _():
                hc = lax.rem(h, CORES)
                if part == 0:
                    @pl.when(hc == 0)
                    def _():
                        h_copy.wait()
                        h_out.wait_recv()

                @pl.loop(0, half // width)
                def _(n):
                    cols = pl.ds(pl.multiple_of(n * width, width), width)
                    for b, pick in enumerate(mine):
                        dst = dsts[2 * part + b // CORES]
                        rs = slice((b % CORES) * seq_len, (b % CORES + 1) * seq_len)
                        held = chosen(pick, lambda s: hbuf[hc, s * seq_len:(s + 1) * seq_len, cols].astype(jnp.float32))
                        dst[rs, cols] = dst[rs, cols] + held

            if part == 0:
                for d in range(2):
                    @pl.when(jnp.logical_and(ab == d, q <= 1))
                    def _():
                        ring(p1, r1, s1, q1, d, q).start()

                    @pl.when(jnp.logical_and(ab == d, q == 0))
                    def _():
                        ring(p2, r2, s2, q2, 1 - d, q).start()

    def o_out_wait(h):
        pltpu.make_async_remote_copy(out_ref.at[:, pl.ds(0, cap), sib_cols],
                                     obuf.at[h, pl.ds(core * n_loc, n_loc), pl.ds(0, cap)],
                                     o_snd.at[h], o_rcv.at[h],
                                     device_id={'ep': sib}, device_id_type=MESH).wait_send()

    def sub(n):
        return pl.ds(pl.multiple_of(n * leg, leg), leg)

    def last_leg(d, q, n):
        return pltpu.make_async_remote_copy(r1.at[d, q, :, sub(n)], r3.at[d, q, :, sub(n)], s3.at[d, q, n], q3.at[d, q, n],
                                            device_id={'ep': side[d]}, device_id_type=MESH)

    def hop(q, jc, n, c, to):
        cols = pl.ds(pl.multiple_of(c * half + n * leg, leg), leg)
        return pltpu.make_async_remote_copy(ysend.at[q, jc, :, :, sub(n)], yland.at[pl.ds(2 * q, 2), :, cols],
                                            ys.at[q, jc, n], yr.at[c, q, n],
                                            device_id={'pp': nxt, 'ep': to}, device_id_type=MESH)

    def finish(q, n):
        @pl.when(n == 0)
        def _():
            for d in range(2):
                ring(p2, r2, s2, q2, d, q).wait_recv()
        cols = sub(n)
        for d in range(2):
            last_leg(d, q, n).wait_recv()
        for ab in range(2):
            total = own[ab, lax.rem(q, 3), :, cols] + (r3[ab, q, :, cols] + r2[1 - ab, q, :, cols])
            rounded = total.astype(jnp.bfloat16)
            for jc in range(CORES):
                ysend[q, jc, ab, :, cols] = rounded[jc * seq_len:(jc + 1) * seq_len]
        for jc in range(CORES):
            hop(q, jc, n, core, chip * CORES + jc).start()

    n_tok = 2 * seq_len
    row = lax.broadcasted_iota(jnp.int32, (n_tok, n_tok), 0)
    col = lax.broadcasted_iota(jnp.int32, (n_tok, n_tok), 1)
    causal = jnp.logical_and(row >= col, row // seq_len == col // seq_len)

    def normalise(q):
        for c in range(CORES):
            for n in range(n_sub):
                hop(q, 0, n, c, me).wait_recv()
        for ab in range(2):
            y = yland[2 * q + ab].astype(jnp.float32)
            inv = lax.rsqrt(jnp.mean(y * y, axis=-1, keepdims=True) + NORM_EPS)
            xs[ab * seq_len:(ab + 1) * seq_len, :] = (y * inv * norm[...]).astype(jnp.bfloat16)

    def attend(n):
        cols = pl.ds(pl.multiple_of(n * tile, tile), tile)
        x = xs[...]
        qt, kt, vt = (jnp.dot(x, w[:, cols], preferred_element_type=jnp.float32).astype(jnp.bfloat16) for w in (wq, wk, wv))
        for hd in range(tile // HEAD_DIM):
            hs = slice(hd * HEAD_DIM, (hd + 1) * HEAD_DIM)
            scores = lax.dot_general(qt[:, hs], kt[:, hs], (((1,), (1,)), ((), ())), preferred_element_type=jnp.float32)
            scores = jnp.where(causal, scores * (HEAD_DIM ** -0.5), -1e30)
            raised = jnp.exp(scores - jnp.max(scores, axis=-1, keepdims=True))
            probs = (raised / jnp.sum(raised, axis=-1, keepdims=True)).astype(jnp.bfloat16)
            mixed = jnp.dot(probs, vt[:, hs], preferred_element_type=jnp.float32).astype(jnp.bfloat16)
            mix[:, pl.ds(pl.multiple_of(n * tile + hd * HEAD_DIM, HEAD_DIM), HEAD_DIM)] = mixed

    def project(q):
        @pl.loop(0, CORES)
        def _(c):
            @pl.loop(0, half // tile)
            def _(n):
                cols = pl.ds(pl.multiple_of(c * half + n * tile, tile), tile)
                out = jnp.dot(mix[...], wo[:, cols], preferred_element_type=jnp.float32).astype(jnp.bfloat16).astype(jnp.float32)
                z = []
                for ab in range(2):
                    y = yland[2 * q + ab, :, cols].astype(jnp.float32)
                    z.append((y + out[ab * seq_len:(ab + 1) * seq_len]).astype(jnp.bfloat16))
                cols = pl.ds(pl.multiple_of(n * tile, tile), tile)
                for b in range(n_ep):
                    home = comes[0, me * n_ep + b] // n_ep
                    rs = pl.ds(b * seq_len, seq_len)
                    hbuf[c, rs, cols] = jnp.where(home == q, z[0], jnp.where(home == q + n_half, z[1], hbuf[c, rs, cols]))

    def store(c):
        return pltpu.make_async_copy(hbuf.at[c], z_ref.at[:, pl.ds(c * half, half)], zs.at[c])

    def last(q):
        for d in range(2):
            ring(p1, r1, s1, q1, d, q).wait_recv()
            r1[d, q] = p3[d, lax.rem(q, 2)] + r1[d, q]
            for n in range(n_sub):
                last_leg(d, q, n).start()

    def first(q):
        for d in range(2):
            ring(p1, r1, s1, q1, d, q).start()
        for d in range(2):
            ring(p2, r2, s2, q2, d, q).start()

    @pl.loop(0, n_half + 3)
    def _(it):
        @pl.when(it < n_half)
        def _():
            @pl.loop(0, 2)
            def _(ab):
                partial(it, ab)

                @pl.when(jnp.logical_and(ab == 0, it < n_half - 1))
                def _():
                    for other in range(2):
                        o_out(it + 1 + n_half * other).start()

        @pl.when(it == 1)
        def _():
            last(0)
            for d in range(2):
                ring(p2, r2, s2, q2, d, 1).start()
            last(1)

        @pl.when(it == 2)
        def _():
            first(2)

        for i in range(4):
            @pl.when(it == (0, 1, 1, 2)[i])
            def _():
                for part in range(n_half):
                    weight(i, part).start()

        @pl.when(it == 3)
        def _():
            norm_copy.wait()
            comes_copy.wait()
            for i in range(3):
                for part in range(n_half):
                    weight(i, part).wait()

        @pl.when(it >= 3)
        def _():
            normalise(it - 3)

        @pl.loop(0, n_sub)
        def _(n):
            @pl.when(it >= 3)
            def _():
                attend(n)

            @pl.when(jnp.logical_and(it >= 2, it < n_half + 2))
            def _():
                finish(it - 2, n)

        @pl.when(it == 3)
        def _():
            for part in range(n_half):
                weight(3, part).wait()
            last(2)
            first(3)

        @pl.when(it == n_half)
        def _():
            w_out.wait_send()
            h_out.wait_send()
            for copy in t_out:
                copy.wait_send()

            @pl.loop(0, n_ep)
            def _(h):
                o_out_wait(h)

        @pl.when(it >= 3)
        def _():
            project(it - 3)

        @pl.when(it == 4)
        def _():
            last(3)

    for c in range(CORES):
        store(c).start()

    @pl.loop(0, n_half)
    def _(q):
        for d in range(2):
            ring(p1, r1, s1, q1, d, q).wait_send()
            ring(p2, r2, s2, q2, d, q).wait_send()
            for n in range(n_sub):
                last_leg(d, q, n).wait_send()
        for jc in range(CORES):
            for n in range(n_sub):
                hop(q, jc, n, core, chip * CORES + jc).wait_send()
    for c in range(CORES):
        store(c).wait()


def solution(mesh):
    n_stages = mesh.shape['pp']
    n_ep = mesh.shape['ep']
    group_axes = ('data', 'pp')

    def device_step(expert_out, expert_id, slot_id, gate, resid, owner, norm_w, w_q, w_k, w_v, w_o):
        n_loc, capacity, model_dim = expert_out.shape[2:]
        cap = capacity // n_ep
        tok_dev, top_k = expert_id.shape[2:]
        seq_dev = owner.shape[1] // n_ep
        seq_len = tok_dev // seq_dev
        assert expert_out.shape[1] == 1 and seq_dev == n_ep
        half = model_dim // CORES
        slot_pad = -(-cap // 16) * 16
        n_half = n_ep // 2
        block = CORES * seq_len

        dims = (n_ep, n_stages, n_loc, cap, slot_pad, seq_len, top_k, half)
        f32, bf16 = jnp.float32, jnp.bfloat16
        n_sub = model_dim // min(512, half)
        assert n_half == 4

        def ringbuf(slots):
            return pltpu.VMEM((2, slots, block, half), f32)

        square = pltpu.VMEM((model_dim, model_dim), bf16)
        dma = pltpu.SemaphoreType.DMA
        z_owned = pl.pallas_call(
            functools.partial(stage_kernel, dims),
            out_shape=jax.ShapeDtypeStruct((tok_dev, model_dim), bf16),
            in_specs=[pl.BlockSpec(memory_space=pl.ANY)] * 11,
            out_specs=pl.BlockSpec(memory_space=pl.ANY),
            scratch_shapes=[
                pltpu.VMEM((n_ep, CORES * n_loc, slot_pad, half), bf16),
                pltpu.VMEM((CORES, tok_dev, half), bf16),
                pltpu.VMEM((n_ep, 2 * top_k, tok_dev), f32),
                pltpu.VMEM((top_k, tok_dev), jnp.int32),
                pltpu.VMEM((top_k, tok_dev), jnp.int32),
                pltpu.VMEM((top_k, tok_dev), f32),
                pltpu.VMEM((1, n_ep * seq_dev), jnp.int32),
                pltpu.SMEM((1, n_ep * seq_dev), jnp.int32),
                pltpu.SMEM((1, n_ep * seq_dev), jnp.int32),
                pltpu.VMEM((tok_dev, 128), f32),
                pltpu.VMEM((3 * tok_dev // 2, CORES * n_loc * slot_pad), bf16),
                ringbuf(n_half), ringbuf(n_half), ringbuf(2), ringbuf(n_half), ringbuf(n_half), ringbuf(n_half), ringbuf(3),
                pltpu.VMEM((n_half, CORES, 2, seq_len, half), bf16),
                pltpu.VMEM((n_ep, seq_len, model_dim), bf16),
                pltpu.VMEM((1, model_dim), f32),
                square, square, square, square,
                pltpu.VMEM((2 * seq_len, model_dim), bf16),
                pltpu.VMEM((2 * seq_len, model_dim), bf16),
                dma((n_ep,)), dma((n_ep,)), dma((n_ep,)),
                dma, dma, dma,
                dma((3,)), dma((n_ep - 1,)), dma((n_ep,)),
                dma, dma, dma,
                dma((2, n_half)), dma((2, n_half)), dma((2, n_half, n_sub)),
                dma((2, n_half)), dma((2, n_half)), dma((2, n_half, n_sub)),
                dma((n_half, CORES, n_sub)), dma((CORES, n_half, n_sub)), dma((4, n_half)), dma((CORES,)), dma, dma,
            ],
            compiler_params=pltpu.CompilerParams(collective_id=0, has_side_effects=True, vmem_limit_bytes=67043328),
            name='stage',
        )(owner, expert_id[0, 0].T, slot_id[0, 0].T, gate[0, 0].T, expert_out[0, 0], resid[0, 0],
          norm_w, w_q[0], w_k[0], w_v[0], w_o[0])
        return z_owned.reshape(1, 1, tok_dev, model_dim)

    tok_spec = P(group_axes, None, 'ep', None)
    weight_spec = P('pp', None, None)
    in_specs = (P(group_axes, None, 'ep', None, None), tok_spec, tok_spec, tok_spec, tok_spec, P(group_axes, None), P('pp', None), weight_spec, weight_spec, weight_spec, weight_spec)
    return jax.shard_map(device_step, mesh=mesh, in_specs=in_specs, out_specs=tok_spec, check_vma=False)
```

```python
import functools

import jax
import jax.numpy as jnp
from jax import lax
from jax.experimental import pallas as pl
from jax.experimental.pallas import tpu as pltpu
from jax.sharding import PartitionSpec as P

HEAD_DIM = 128
NORM_EPS = 1e-6
MESH = pl.DeviceIdType.MESH
CORES = 2


def stage_kernel(dims, owner_ref, id_ref, slot_ref, gate_ref, out_ref, resid_ref, norm_ref, q_ref, k_ref, v_ref, o_ref, z_ref,
                   obuf, hbuf, ids, slots, gates, owners, goes, comes, table, wterm,
                   p1, p2, p3, r1, r2, r3, own, ysend, yland, norm, wq, wk, wv, wo, xs, mix,
                   o_loc, o_snd, o_rcv, h_loc, h_snd, h_rcv, t_loc, t_snd, t_rcv, w_snd, w_rcv, w_loc,
                   s1, s2, s3, q1, q2, q3, ys, yr, wt, zs, n_loc_sem, c_loc):
    n_ep, n_st, n_loc, cap, slot_pad, seq_len, top_k, half = dims
    n_chip = n_ep // CORES
    n_half = n_ep // 2
    tok_dev = n_ep * seq_len
    me = lax.axis_index('ep')
    rank = lax.axis_index('pp')
    core = lax.rem(me, CORES)
    chip = me // CORES
    sib = me + 1 - 2 * core
    nxt = lax.rem(rank + 1, n_st)
    prv = lax.rem(rank + n_st - 1, n_st)
    side = [lax.rem(me + n_ep - CORES, n_ep), lax.rem(me + CORES, n_ep)]
    my_cols = pl.ds(pl.multiple_of(core * half, 128), half)
    sib_cols = pl.ds(pl.multiple_of((1 - core) * half, 128), half)
    order = [q + n_half * ab for q in range(n_half) for ab in range(2)]

    raw = ((id_ref, ids), (slot_ref, slots), (gate_ref, gates))
    for i, (src, dst) in enumerate(raw):
        pltpu.make_async_copy(src, dst.at[me], t_loc.at[i]).start()
    barrier = pltpu.get_barrier_semaphore()
    for k in range(1, n_ep):
        pl.semaphore_signal(barrier, inc=1, device_id={'ep': lax.rem(me + k, n_ep)}, device_id_type=MESH)
    for other in (nxt, prv):
        for jc in range(CORES):
            pl.semaphore_signal(barrier, inc=1, device_id={'pp': other, 'ep': chip * CORES + jc}, device_id_type=MESH)
    def o_in(h):
        return pltpu.make_async_copy(out_ref.at[:, pl.ds(h * cap, cap), my_cols],
                                     obuf.at[h, pl.ds(core * n_loc, n_loc), pl.ds(0, cap)], o_loc.at[h])

    for h in order[:2]:
        o_in(h).start()
    h_copy = pltpu.make_async_copy(resid_ref.at[:, my_cols], hbuf.at[core], h_loc)
    h_copy.start()
    model = CORES * half
    strip = model // n_half

    def weight(i, part):
        src, dst = ((q_ref, wq), (k_ref, wk), (v_ref, wv), (o_ref, wo))[i]
        rows = pl.ds(part * strip, strip)
        return pltpu.make_async_copy(src.at[rows], dst.at[rows], wt.at[i, part])

    norm_copy = pltpu.make_async_copy(norm_ref, norm, n_loc_sem)
    norm_copy.start()
    comes_copy = pltpu.make_async_copy(owner_ref, comes, c_loc)
    comes_copy.start()
    for i in range(4):
        for part in range(n_half):
            weight(i, part).start()
    for h in order[2:]:
        o_in(h).start()
    if slot_pad > cap:
        for h in range(n_ep):
            obuf[h, :, cap:, :] = jnp.zeros((CORES * n_loc, slot_pad - cap, half), jnp.bfloat16)
    pl.semaphore_wait(barrier, n_ep - 1 + 2 * CORES)

    w_out = pltpu.make_async_remote_copy(owner_ref, owners, w_snd, w_rcv, device_id={'pp': prv}, device_id_type=MESH)
    w_out.start()
    def route(i, k, home, peer):
        src, dst = raw[i]
        return pltpu.make_async_remote_copy(src, dst.at[home], t_snd.at[i, k - 1], t_rcv.at[i, home],
                                            device_id={'ep': peer}, device_id_type=MESH)

    t_out = [route(i, k, me, lax.rem(me + k, n_ep))
             for k in (n_chip, n_chip - 1, n_chip + 1, 2, n_ep - 2, 1, n_ep - 1) for i in range(3)]
    for copy in t_out:
        copy.start()

    def o_out(h):
        return pltpu.make_async_remote_copy(out_ref.at[:, pl.ds(pl.multiple_of(h * cap, 8), cap), sib_cols],
                                            obuf.at[h, pl.ds(core * n_loc, n_loc), pl.ds(0, cap)],
                                            o_snd.at[h], o_rcv.at[h],
                                            device_id={'ep': sib}, device_id_type=MESH)

    h_out = pltpu.make_async_remote_copy(resid_ref.at[:, sib_cols], hbuf.at[core], h_snd, h_rcv,
                                         device_id={'ep': sib}, device_id_type=MESH)
    for ab in range(2):
        o_out(n_half * ab).start()
    h_out.start()

    w_out.wait_recv()
    goes_copy = pltpu.make_async_copy(owners, goes, w_loc)
    goes_copy.start()
    goes_copy.wait()

    def o_wait(h):
        pltpu.make_async_copy(out_ref.at[:, pl.ds(0, cap), my_cols],
                              obuf.at[h, pl.ds(core * n_loc, n_loc), pl.ds(0, cap)], o_loc.at[h]).wait()
        pltpu.make_async_remote_copy(out_ref.at[:, pl.ds(0, cap), sib_cols],
                                     obuf.at[h, pl.ds((1 - core) * n_loc, n_loc), pl.ds(0, cap)],
                                     o_snd.at[h], o_rcv.at[h],
                                     device_id={'ep': sib}, device_id_type=MESH).wait_recv()

    def ring(src, dst, snd, rcv, d, q):
        return pltpu.make_async_remote_copy(src.at[d, q], dst.at[d, q], snd.at[d, q], rcv.at[d, q],
                                            device_id={'ep': side[d]}, device_id_type=MESH)

    depth = CORES * n_loc * slot_pad
    width = min(256, half)
    tile = min(512, half)
    n_sub = model // tile
    leg = half // n_sub
    lane = lax.broadcasted_iota(jnp.int32, (seq_len, depth), 1).astype(jnp.float32)
    block = CORES * seq_len
    per = n_chip * CORES // 2

    def partial(q, ab):
        h = q + n_half * ab

        @pl.when(h != me)
        def _():
            for i in range(3):
                route(i, 1, h, h).wait_recv()

        @pl.when(h == me)
        def _():
            for i, (src, dst) in enumerate(raw):
                pltpu.make_async_copy(src, dst.at[me], t_loc.at[i]).wait()

        key = jnp.where(slots[h] >= 0, ids[h] * slot_pad + slots[h] - h * cap, -1).astype(jnp.float32)
        rows = jnp.concatenate([key, gates[h], jnp.zeros((128 - 2 * top_k, tok_dev), jnp.float32)], axis=0)
        table[...] = rows.T
        step = 1 - 2 * ab
        dest = [chip + 2, chip + n_chip + step, chip + n_chip - step, chip]
        picks = []
        for r in range(n_chip):
            for jc in range(CORES):
                j = lax.rem(dest[r], n_chip) * CORES + jc
                pick = 0
                for b in range(n_ep):
                    seq = goes[0, j * n_ep + b] - h * n_ep
                    pick = jnp.where(jnp.logical_and(seq >= 0, seq < n_ep), seq, pick)
                picks.append(pick)

        def chosen(pick, load):
            got = load(0)
            for s in range(1, n_ep):
                got = jnp.where(pick == s, load(s), got)
            return got

        base = (chip * depth).astype(jnp.float32)
        dsts = [p1.at[ab, q], p2.at[1 - ab, q], p3.at[ab, lax.rem(q, 2)], own.at[ab, lax.rem(q, 3)]]
        for part in range(2):
            mine = picks[part * per:(part + 1) * per]
            for b, pick in enumerate(mine):
                rt = chosen(pick, lambda s: table[s * seq_len:(s + 1) * seq_len, :])
                w = jnp.zeros((seq_len, depth), jnp.float32)
                for j in range(top_k):
                    key = rt[:, j:j + 1] - base
                    w = jnp.where(lane == key, rt[:, top_k + j:top_k + j + 1], w)
                hi = w.astype(jnp.bfloat16)
                rest = w - hi.astype(jnp.float32)
                mid = rest.astype(jnp.bfloat16)
                low = (rest - mid.astype(jnp.float32)).astype(jnp.bfloat16)
                for t, term in enumerate((hi, mid, low)):
                    wterm[pl.ds((t * per + b) * seq_len, seq_len), :] = term
            if part == 0:
                o_wait(h)

            @pl.loop(0, half // width)
            def _(n):
                cols = pl.ds(pl.multiple_of(n * width, width), width)
                slots_in = obuf[h, :, :, cols].reshape(depth, width)
                res = jnp.dot(wterm[...], slots_in, preferred_element_type=jnp.float32)
                span = per * seq_len
                res = res[:span] + (res[span:2 * span] + res[2 * span:])
                for r in range(2):
                    dsts[2 * part + r][:, cols] = res[r * block:(r + 1) * block]

            @pl.when(h // CORES == chip)
            def _():
                hc = lax.rem(h, CORES)
                if part == 0:
                    @pl.when(hc == 0)
                    def _():
                        h_copy.wait()
                        h_out.wait_recv()

                @pl.loop(0, half // width)
                def _(n):
                    cols = pl.ds(pl.multiple_of(n * width, width), width)
                    for b, pick in enumerate(mine):
                        dst = dsts[2 * part + b // CORES]
                        rs = slice((b % CORES) * seq_len, (b % CORES + 1) * seq_len)
                        held = chosen(pick, lambda s: hbuf[hc, s * seq_len:(s + 1) * seq_len, cols].astype(jnp.float32))
                        dst[rs, cols] = dst[rs, cols] + held

            if part == 0:
                for d in range(2):
                    @pl.when(jnp.logical_and(ab == d, q <= 1))
                    def _():
                        ring(p1, r1, s1, q1, d, q).start()

                    @pl.when(jnp.logical_and(ab == d, q == 0))
                    def _():
                        ring(p2, r2, s2, q2, 1 - d, q).start()

    def o_out_wait(h):
        pltpu.make_async_remote_copy(out_ref.at[:, pl.ds(0, cap), sib_cols],
                                     obuf.at[h, pl.ds(core * n_loc, n_loc), pl.ds(0, cap)],
                                     o_snd.at[h], o_rcv.at[h],
                                     device_id={'ep': sib}, device_id_type=MESH).wait_send()

    def sub(n):
        return pl.ds(pl.multiple_of(n * leg, leg), leg)

    def last_leg(d, q, n):
        return pltpu.make_async_remote_copy(r1.at[d, q, :, sub(n)], r3.at[d, q, :, sub(n)], s3.at[d, q, n], q3.at[d, q, n],
                                            device_id={'ep': side[d]}, device_id_type=MESH)

    def hop(q, jc, n, c, to):
        cols = pl.ds(pl.multiple_of(c * half + n * leg, leg), leg)
        return pltpu.make_async_remote_copy(ysend.at[q, jc, :, :, sub(n)], yland.at[pl.ds(2 * q, 2), :, cols],
                                            ys.at[q, jc, n], yr.at[c, q, n],
                                            device_id={'pp': nxt, 'ep': to}, device_id_type=MESH)

    def finish(q, n):
        @pl.when(n == 0)
        def _():
            for d in range(2):
                ring(p2, r2, s2, q2, d, q).wait_recv()
        cols = sub(n)
        for d in range(2):
            last_leg(d, q, n).wait_recv()
        for ab in range(2):
            total = own[ab, lax.rem(q, 3), :, cols] + (r3[ab, q, :, cols] + r2[1 - ab, q, :, cols])
            rounded = total.astype(jnp.bfloat16)
            for jc in range(CORES):
                ysend[q, jc, ab, :, cols] = rounded[jc * seq_len:(jc + 1) * seq_len]
        for jc in range(CORES):
            hop(q, jc, n, core, chip * CORES + jc).start()

    n_tok = 2 * seq_len
    row = lax.broadcasted_iota(jnp.int32, (n_tok, n_tok), 0)
    col = lax.broadcasted_iota(jnp.int32, (n_tok, n_tok), 1)
    causal = jnp.logical_and(row >= col, row // seq_len == col // seq_len)

    def normalise(q):
        for c in range(CORES):
            for n in range(n_sub):
                hop(q, 0, n, c, me).wait_recv()
        for ab in range(2):
            y = yland[2 * q + ab].astype(jnp.float32)
            inv = lax.rsqrt(jnp.mean(y * y, axis=-1, keepdims=True) + NORM_EPS)
            xs[ab * seq_len:(ab + 1) * seq_len, :] = (y * inv * norm[...]).astype(jnp.bfloat16)

    def attend(n):
        cols = pl.ds(pl.multiple_of(n * tile, tile), tile)
        x = xs[...]
        qt, kt, vt = (jnp.dot(x, w[:, cols], preferred_element_type=jnp.float32).astype(jnp.bfloat16) for w in (wq, wk, wv))
        for hd in range(tile // HEAD_DIM):
            hs = slice(hd * HEAD_DIM, (hd + 1) * HEAD_DIM)
            scores = lax.dot_general(qt[:, hs], kt[:, hs], (((1,), (1,)), ((), ())), preferred_element_type=jnp.float32)
            scores = jnp.where(causal, scores * (HEAD_DIM ** -0.5), -1e30)
            raised = jnp.exp(scores - jnp.max(scores, axis=-1, keepdims=True))
            probs = (raised / jnp.sum(raised, axis=-1, keepdims=True)).astype(jnp.bfloat16)
            mixed = jnp.dot(probs, vt[:, hs], preferred_element_type=jnp.float32).astype(jnp.bfloat16)
            mix[:, pl.ds(pl.multiple_of(n * tile + hd * HEAD_DIM, HEAD_DIM), HEAD_DIM)] = mixed

    def project(q):
        @pl.loop(0, CORES)
        def _(c):
            @pl.loop(0, half // tile)
            def _(n):
                cols = pl.ds(pl.multiple_of(c * half + n * tile, tile), tile)
                out = jnp.dot(mix[...], wo[:, cols], preferred_element_type=jnp.float32).astype(jnp.bfloat16).astype(jnp.float32)
                z = []
                for ab in range(2):
                    y = yland[2 * q + ab, :, cols].astype(jnp.float32)
                    z.append((y + out[ab * seq_len:(ab + 1) * seq_len]).astype(jnp.bfloat16))
                cols = pl.ds(pl.multiple_of(n * tile, tile), tile)
                for b in range(n_ep):
                    home = comes[0, me * n_ep + b] // n_ep
                    rs = pl.ds(b * seq_len, seq_len)
                    hbuf[c, rs, cols] = jnp.where(home == q, z[0], jnp.where(home == q + n_half, z[1], hbuf[c, rs, cols]))

    def store(c):
        return pltpu.make_async_copy(hbuf.at[c], z_ref.at[:, pl.ds(c * half, half)], zs.at[c])

    def last(q):
        for d in range(2):
            ring(p1, r1, s1, q1, d, q).wait_recv()
            r1[d, q] = p3[d, lax.rem(q, 2)] + r1[d, q]
            for n in range(n_sub):
                last_leg(d, q, n).start()

    def first(q):
        for d in range(2):
            ring(p1, r1, s1, q1, d, q).start()
        for d in range(2):
            ring(p2, r2, s2, q2, d, q).start()

    @pl.loop(0, n_half + 3)
    def _(it):
        @pl.when(it < n_half)
        def _():
            @pl.loop(0, 2)
            def _(ab):
                partial(it, ab)

                @pl.when(jnp.logical_and(ab == 0, it < n_half - 1))
                def _():
                    for other in range(2):
                        o_out(it + 1 + n_half * other).start()

        @pl.when(it == 1)
        def _():
            last(0)
            for d in range(2):
                ring(p2, r2, s2, q2, d, 1).start()
            last(1)

        @pl.when(it == 2)
        def _():
            first(2)

        @pl.when(it == 3)
        def _():
            norm_copy.wait()
            comes_copy.wait()
            for i in range(3):
                for part in range(n_half):
                    weight(i, part).wait()

        @pl.when(it >= 3)
        def _():
            normalise(it - 3)

        @pl.loop(0, n_sub)
        def _(n):
            @pl.when(it >= 3)
            def _():
                attend(n)

            @pl.when(jnp.logical_and(it >= 2, it < n_half + 2))
            def _():
                finish(it - 2, n)

        @pl.when(it == 3)
        def _():
            for part in range(n_half):
                weight(3, part).wait()
            last(2)
            first(3)

        @pl.when(it == n_half)
        def _():
            w_out.wait_send()
            h_out.wait_send()
            for copy in t_out:
                copy.wait_send()

            @pl.loop(0, n_ep)
            def _(h):
                o_out_wait(h)

        @pl.when(it >= 3)
        def _():
            project(it - 3)

        @pl.when(it == 4)
        def _():
            last(3)

    for c in range(CORES):
        store(c).start()

    @pl.loop(0, n_half)
    def _(q):
        for d in range(2):
            ring(p1, r1, s1, q1, d, q).wait_send()
            ring(p2, r2, s2, q2, d, q).wait_send()
            for n in range(n_sub):
                last_leg(d, q, n).wait_send()
        for jc in range(CORES):
            for n in range(n_sub):
                hop(q, jc, n, core, chip * CORES + jc).wait_send()
    for c in range(CORES):
        store(c).wait()


def solution(mesh):
    n_stages = mesh.shape['pp']
    n_ep = mesh.shape['ep']
    group_axes = ('data', 'pp')

    def device_step(expert_out, expert_id, slot_id, gate, resid, owner, norm_w, w_q, w_k, w_v, w_o):
        n_loc, capacity, model_dim = expert_out.shape[2:]
        cap = capacity // n_ep
        tok_dev, top_k = expert_id.shape[2:]
        seq_dev = owner.shape[1] // n_ep
        seq_len = tok_dev // seq_dev
        assert expert_out.shape[1] == 1 and seq_dev == n_ep
        half = model_dim // CORES
        slot_pad = -(-cap // 16) * 16
        n_half = n_ep // 2
        block = CORES * seq_len

        dims = (n_ep, n_stages, n_loc, cap, slot_pad, seq_len, top_k, half)
        f32, bf16 = jnp.float32, jnp.bfloat16
        n_sub = model_dim // min(512, half)
        assert n_half == 4

        def ringbuf(slots):
            return pltpu.VMEM((2, slots, block, half), f32)

        square = pltpu.VMEM((model_dim, model_dim), bf16)
        dma = pltpu.SemaphoreType.DMA
        z_owned = pl.pallas_call(
            functools.partial(stage_kernel, dims),
            out_shape=jax.ShapeDtypeStruct((tok_dev, model_dim), bf16),
            in_specs=[pl.BlockSpec(memory_space=pl.ANY)] * 11,
            out_specs=pl.BlockSpec(memory_space=pl.ANY),
            scratch_shapes=[
                pltpu.VMEM((n_ep, CORES * n_loc, slot_pad, half), bf16),
                pltpu.VMEM((CORES, tok_dev, half), bf16),
                pltpu.VMEM((n_ep, top_k, tok_dev), jnp.int32),
                pltpu.VMEM((n_ep, top_k, tok_dev), jnp.int32),
                pltpu.VMEM((n_ep, top_k, tok_dev), f32),
                pltpu.VMEM((1, n_ep * seq_dev), jnp.int32),
                pltpu.SMEM((1, n_ep * seq_dev), jnp.int32),
                pltpu.SMEM((1, n_ep * seq_dev), jnp.int32),
                pltpu.VMEM((tok_dev, 128), f32),
                pltpu.VMEM((3 * tok_dev // 2, CORES * n_loc * slot_pad), bf16),
                ringbuf(n_half), ringbuf(n_half), ringbuf(2), ringbuf(n_half), ringbuf(n_half), ringbuf(n_half), ringbuf(3),
                pltpu.VMEM((n_half, CORES, 2, seq_len, half), bf16),
                pltpu.VMEM((n_ep, seq_len, model_dim), bf16),
                pltpu.VMEM((1, model_dim), f32),
                square, square, square, square,
                pltpu.VMEM((2 * seq_len, model_dim), bf16),
                pltpu.VMEM((2 * seq_len, model_dim), bf16),
                dma((n_ep,)), dma((n_ep,)), dma((n_ep,)),
                dma, dma, dma,
                dma((3,)), dma((3, n_ep - 1)), dma((3, n_ep)),
                dma, dma, dma,
                dma((2, n_half)), dma((2, n_half)), dma((2, n_half, n_sub)),
                dma((2, n_half)), dma((2, n_half)), dma((2, n_half, n_sub)),
                dma((n_half, CORES, n_sub)), dma((CORES, n_half, n_sub)), dma((4, n_half)), dma((CORES,)), dma, dma,
            ],
            compiler_params=pltpu.CompilerParams(collective_id=0, has_side_effects=True, vmem_limit_bytes=67043328),
            name='stage',
        )(owner, expert_id[0, 0].T, slot_id[0, 0].T, gate[0, 0].T, expert_out[0, 0], resid[0, 0],
          norm_w, w_q[0], w_k[0], w_v[0], w_o[0])
        return z_owned.reshape(1, 1, tok_dev, model_dim)

    tok_spec = P(group_axes, None, 'ep', None)
    weight_spec = P('pp', None, None)
    in_specs = (P(group_axes, None, 'ep', None, None), tok_spec, tok_spec, tok_spec, tok_spec, P(group_axes, None), P('pp', None), weight_spec, weight_spec, weight_spec, weight_spec)
    return jax.shard_map(device_step, mesh=mesh, in_specs=in_specs, out_specs=tok_spec, check_vma=False)
```

```python
import functools

import jax
import jax.numpy as jnp
from jax import lax
from jax.experimental import pallas as pl
from jax.experimental.pallas import tpu as pltpu
from jax.sharding import PartitionSpec as P

HEAD_DIM = 128
NORM_EPS = 1e-6
MESH = pl.DeviceIdType.MESH
CORES = 2


def stage_kernel(dims, owner_ref, id_ref, slot_ref, gate_ref, out_ref, resid_ref, norm_ref, q_ref, k_ref, v_ref, o_ref, z_ref,
                   obuf, hbuf, ids, slots, gates, owners, goes, comes, table, wterm,
                   p1, p2, p3, r1, r2, r3, own, ysend, yland, norm, wq, wk, wv, wo, xs, mix,
                   o_loc, o_snd, o_rcv, h_loc, h_snd, h_rcv, t_loc, t_snd, t_rcv, w_snd, w_rcv, w_loc,
                   s1, s2, s3, q1, q2, q3, ys, yr, wt, zs, n_loc_sem, c_loc):
    n_ep, n_st, n_loc, cap, slot_pad, seq_len, top_k, half = dims
    n_chip = n_ep // CORES
    n_half = n_ep // 2
    tok_dev = n_ep * seq_len
    me = lax.axis_index('ep')
    rank = lax.axis_index('pp')
    core = lax.rem(me, CORES)
    chip = me // CORES
    sib = me + 1 - 2 * core
    nxt = lax.rem(rank + 1, n_st)
    prv = lax.rem(rank + n_st - 1, n_st)
    side = [lax.rem(me + n_ep - CORES, n_ep), lax.rem(me + CORES, n_ep)]
    my_cols = pl.ds(pl.multiple_of(core * half, 128), half)
    sib_cols = pl.ds(pl.multiple_of((1 - core) * half, 128), half)
    order = [q + n_half * ab for q in range(n_half) for ab in range(2)]

    raw = ((id_ref, ids), (slot_ref, slots), (gate_ref, gates))
    for i, (src, dst) in enumerate(raw):
        pltpu.make_async_copy(src, dst.at[me], t_loc.at[i]).start()
    barrier = pltpu.get_barrier_semaphore()
    for k in range(1, n_ep):
        pl.semaphore_signal(barrier, inc=1, device_id={'ep': lax.rem(me + k, n_ep)}, device_id_type=MESH)
    for other in (nxt, prv):
        for jc in range(CORES):
            pl.semaphore_signal(barrier, inc=1, device_id={'pp': other, 'ep': chip * CORES + jc}, device_id_type=MESH)
    def o_in(h):
        return pltpu.make_async_copy(out_ref.at[:, pl.ds(h * cap, cap), my_cols],
                                     obuf.at[h, pl.ds(core * n_loc, n_loc), pl.ds(0, cap)], o_loc.at[h])

    for h in order[:2]:
        o_in(h).start()
    h_copy = pltpu.make_async_copy(resid_ref.at[:, my_cols], hbuf.at[core], h_loc)
    h_copy.start()
    model = CORES * half
    strip = model // n_half

    def weight(i, part):
        src, dst = ((q_ref, wq), (k_ref, wk), (v_ref, wv), (o_ref, wo))[i]
        rows = pl.ds(part * strip, strip)
        return pltpu.make_async_copy(src.at[rows], dst.at[rows], wt.at[i, part])

    norm_copy = pltpu.make_async_copy(norm_ref, norm, n_loc_sem)
    norm_copy.start()
    comes_copy = pltpu.make_async_copy(owner_ref, comes, c_loc)
    comes_copy.start()
    for h in order[2:]:
        o_in(h).start()
    for i in range(2):
        for part in range(n_half):
            weight(i, part).start()
    if slot_pad > cap:
        for h in range(n_ep):
            obuf[h, :, cap:, :] = jnp.zeros((CORES * n_loc, slot_pad - cap, half), jnp.bfloat16)
    pl.semaphore_wait(barrier, n_ep - 1 + 2 * CORES)

    w_out = pltpu.make_async_remote_copy(owner_ref, owners, w_snd, w_rcv, device_id={'pp': prv}, device_id_type=MESH)
    w_out.start()
    def route(i, k, home, peer):
        src, dst = raw[i]
        return pltpu.make_async_remote_copy(src, dst.at[home], t_snd.at[i, k - 1], t_rcv.at[i, home],
                                            device_id={'ep': peer}, device_id_type=MESH)

    t_out = [route(i, k, me, lax.rem(me + k, n_ep))
             for k in (n_chip, n_chip - 1, n_chip + 1, 2, n_ep - 2, 1, n_ep - 1) for i in range(3)]
    for copy in t_out:
        copy.start()

    def o_out(h):
        return pltpu.make_async_remote_copy(out_ref.at[:, pl.ds(pl.multiple_of(h * cap, 8), cap), sib_cols],
                                            obuf.at[h, pl.ds(core * n_loc, n_loc), pl.ds(0, cap)],
                                            o_snd.at[h], o_rcv.at[h],
                                            device_id={'ep': sib}, device_id_type=MESH)

    h_out = pltpu.make_async_remote_copy(resid_ref.at[:, sib_cols], hbuf.at[core], h_snd, h_rcv,
                                         device_id={'ep': sib}, device_id_type=MESH)
    for ab in range(2):
        o_out(n_half * ab).start()
    h_out.start()

    w_out.wait_recv()
    goes_copy = pltpu.make_async_copy(owners, goes, w_loc)
    goes_copy.start()
    goes_copy.wait()

    def o_wait(h):
        pltpu.make_async_copy(out_ref.at[:, pl.ds(0, cap), my_cols],
                              obuf.at[h, pl.ds(core * n_loc, n_loc), pl.ds(0, cap)], o_loc.at[h]).wait()
        pltpu.make_async_remote_copy(out_ref.at[:, pl.ds(0, cap), sib_cols],
                                     obuf.at[h, pl.ds((1 - core) * n_loc, n_loc), pl.ds(0, cap)],
                                     o_snd.at[h], o_rcv.at[h],
                                     device_id={'ep': sib}, device_id_type=MESH).wait_recv()

    def ring(src, dst, snd, rcv, d, q):
        return pltpu.make_async_remote_copy(src.at[d, q], dst.at[d, q], snd.at[d, q], rcv.at[d, q],
                                            device_id={'ep': side[d]}, device_id_type=MESH)

    depth = CORES * n_loc * slot_pad
    width = min(256, half)
    tile = min(512, half)
    n_sub = model // tile
    leg = half // n_sub
    lane = lax.broadcasted_iota(jnp.int32, (seq_len, depth), 1).astype(jnp.float32)
    block = CORES * seq_len
    per = n_chip * CORES // 2

    def partial(q, ab):
        h = q + n_half * ab

        @pl.when(h != me)
        def _():
            for i in range(3):
                route(i, 1, h, h).wait_recv()

        @pl.when(h == me)
        def _():
            for i, (src, dst) in enumerate(raw):
                pltpu.make_async_copy(src, dst.at[me], t_loc.at[i]).wait()

        key = jnp.where(slots[h] >= 0, ids[h] * slot_pad + slots[h] - h * cap, -1).astype(jnp.float32)
        rows = jnp.concatenate([key, gates[h], jnp.zeros((128 - 2 * top_k, tok_dev), jnp.float32)], axis=0)
        table[...] = rows.T
        step = 1 - 2 * ab
        dest = [chip + 2, chip + n_chip + step, chip + n_chip - step, chip]
        picks = []
        for r in range(n_chip):
            for jc in range(CORES):
                j = lax.rem(dest[r], n_chip) * CORES + jc
                pick = 0
                for b in range(n_ep):
                    seq = goes[0, j * n_ep + b] - h * n_ep
                    pick = jnp.where(jnp.logical_and(seq >= 0, seq < n_ep), seq, pick)
                picks.append(pick)

        def chosen(pick, load):
            got = load(0)
            for s in range(1, n_ep):
                got = jnp.where(pick == s, load(s), got)
            return got

        base = (chip * depth).astype(jnp.float32)
        dsts = [p1.at[ab, q], p2.at[1 - ab, q], p3.at[ab, lax.rem(q, 2)], own.at[ab, lax.rem(q, 3)]]
        for part in range(2):
            mine = picks[part * per:(part + 1) * per]
            for b, pick in enumerate(mine):
                rt = chosen(pick, lambda s: table[s * seq_len:(s + 1) * seq_len, :])
                w = jnp.zeros((seq_len, depth), jnp.float32)
                for j in range(top_k):
                    key = rt[:, j:j + 1] - base
                    w = jnp.where(lane == key, rt[:, top_k + j:top_k + j + 1], w)
                hi = w.astype(jnp.bfloat16)
                rest = w - hi.astype(jnp.float32)
                mid = rest.astype(jnp.bfloat16)
                low = (rest - mid.astype(jnp.float32)).astype(jnp.bfloat16)
                for t, term in enumerate((hi, mid, low)):
                    wterm[pl.ds((t * per + b) * seq_len, seq_len), :] = term
            if part == 0:
                o_wait(h)

            @pl.loop(0, half // width)
            def _(n):
                cols = pl.ds(pl.multiple_of(n * width, width), width)
                slots_in = obuf[h, :, :, cols].reshape(depth, width)
                res = jnp.dot(wterm[...], slots_in, preferred_element_type=jnp.float32)
                span = per * seq_len
                res = res[:span] + (res[span:2 * span] + res[2 * span:])
                for r in range(2):
                    dsts[2 * part + r][:, cols] = res[r * block:(r + 1) * block]

            @pl.when(h // CORES == chip)
            def _():
                hc = lax.rem(h, CORES)
                if part == 0:
                    @pl.when(hc == 0)
                    def _():
                        h_copy.wait()
                        h_out.wait_recv()

                @pl.loop(0, half // width)
                def _(n):
                    cols = pl.ds(pl.multiple_of(n * width, width), width)
                    for b, pick in enumerate(mine):
                        dst = dsts[2 * part + b // CORES]
                        rs = slice((b % CORES) * seq_len, (b % CORES + 1) * seq_len)
                        held = chosen(pick, lambda s: hbuf[hc, s * seq_len:(s + 1) * seq_len, cols].astype(jnp.float32))
                        dst[rs, cols] = dst[rs, cols] + held

            if part == 0:
                for d in range(2):
                    @pl.when(jnp.logical_and(ab == d, q <= 1))
                    def _():
                        ring(p1, r1, s1, q1, d, q).start()

                    @pl.when(jnp.logical_and(ab == d, q == 0))
                    def _():
                        ring(p2, r2, s2, q2, 1 - d, q).start()

    def o_out_wait(h):
        pltpu.make_async_remote_copy(out_ref.at[:, pl.ds(0, cap), sib_cols],
                                     obuf.at[h, pl.ds(core * n_loc, n_loc), pl.ds(0, cap)],
                                     o_snd.at[h], o_rcv.at[h],
                                     device_id={'ep': sib}, device_id_type=MESH).wait_send()

    def sub(n):
        return pl.ds(pl.multiple_of(n * leg, leg), leg)

    def last_leg(d, q, n):
        return pltpu.make_async_remote_copy(r1.at[d, q, :, sub(n)], r3.at[d, q, :, sub(n)], s3.at[d, q, n], q3.at[d, q, n],
                                            device_id={'ep': side[d]}, device_id_type=MESH)

    def hop(q, jc, n, c, to):
        cols = pl.ds(pl.multiple_of(c * half + n * leg, leg), leg)
        return pltpu.make_async_remote_copy(ysend.at[q, jc, :, :, sub(n)], yland.at[pl.ds(2 * q, 2), :, cols],
                                            ys.at[q, jc, n], yr.at[c, q, n],
                                            device_id={'pp': nxt, 'ep': to}, device_id_type=MESH)

    def finish(q, n):
        @pl.when(n == 0)
        def _():
            for d in range(2):
                ring(p2, r2, s2, q2, d, q).wait_recv()
        cols = sub(n)
        for d in range(2):
            last_leg(d, q, n).wait_recv()
        for ab in range(2):
            total = own[ab, lax.rem(q, 3), :, cols] + (r3[ab, q, :, cols] + r2[1 - ab, q, :, cols])
            rounded = total.astype(jnp.bfloat16)
            for jc in range(CORES):
                ysend[q, jc, ab, :, cols] = rounded[jc * seq_len:(jc + 1) * seq_len]
        for jc in range(CORES):
            hop(q, jc, n, core, chip * CORES + jc).start()

    n_tok = 2 * seq_len
    n_row = tile // HEAD_DIM * n_tok
    row = lax.broadcasted_iota(jnp.int32, (n_row, n_tok), 0) % n_tok
    col = lax.broadcasted_iota(jnp.int32, (n_row, n_tok), 1)
    causal = jnp.logical_and(row >= col, row // seq_len == col // seq_len)

    def normalise(q):
        for c in range(CORES):
            for n in range(n_sub):
                hop(q, 0, n, c, me).wait_recv()
        for ab in range(2):
            y = yland[2 * q + ab].astype(jnp.float32)
            inv = lax.rsqrt(jnp.mean(y * y, axis=-1, keepdims=True) + NORM_EPS)
            xs[ab * seq_len:(ab + 1) * seq_len, :] = (y * inv * norm[...]).astype(jnp.bfloat16)

    def queries(n):
        cols = pl.ds(n * tile if isinstance(n, int) else pl.multiple_of(n * tile, tile), tile)
        x = xs[...]
        return [jnp.dot(x, w[:, cols], preferred_element_type=jnp.float32).astype(jnp.bfloat16) for w in (wq, wk, wv)]

    def attend(n, qkv):
        cols = pl.ds(n * tile if isinstance(n, int) else pl.multiple_of(n * tile, tile), tile)
        qt, kt, vt = qkv
        heads = [slice(hd * HEAD_DIM, (hd + 1) * HEAD_DIM) for hd in range(tile // HEAD_DIM)]
        scores = jnp.concatenate([lax.dot_general(qt[:, hs], kt[:, hs], (((1,), (1,)), ((), ())),
                                                  preferred_element_type=jnp.float32) for hs in heads], axis=0)
        scores = jnp.where(causal, scores * (HEAD_DIM ** -0.5), -1e30)
        raised = jnp.exp(scores - jnp.max(scores, axis=-1, keepdims=True))
        probs = (raised / jnp.sum(raised, axis=-1, keepdims=True)).astype(jnp.bfloat16)
        mixed = [jnp.dot(probs[i * n_tok:(i + 1) * n_tok], vt[:, hs], preferred_element_type=jnp.float32)
                 for i, hs in enumerate(heads)]
        mix[:, cols] = jnp.concatenate(mixed, axis=1).astype(jnp.bfloat16)

    def store(c):
        return pltpu.make_async_copy(hbuf.at[c], z_ref.at[:, pl.ds(pl.multiple_of(c * half, 128), half)], zs.at[c])

    def project(q):
        @pl.loop(0, CORES)
        def _(c):
            @pl.loop(0, half // tile)
            def _(n):
                cols = pl.ds(pl.multiple_of(c * half + n * tile, tile), tile)
                out = jnp.dot(mix[...], wo[:, cols], preferred_element_type=jnp.float32).astype(jnp.bfloat16).astype(jnp.float32)
                z = []
                for ab in range(2):
                    y = yland[2 * q + ab, :, cols].astype(jnp.float32)
                    z.append((y + out[ab * seq_len:(ab + 1) * seq_len]).astype(jnp.bfloat16))
                cols = pl.ds(pl.multiple_of(n * tile, tile), tile)
                for b in range(n_ep):
                    home = comes[0, me * n_ep + b] // n_ep
                    rs = pl.ds(b * seq_len, seq_len)
                    hbuf[c, rs, cols] = jnp.where(home == q, z[0], jnp.where(home == q + n_half, z[1], hbuf[c, rs, cols]))

            @pl.when(q == n_half - 1)
            def _():
                store(c).start()

    def last(q):
        for d in range(2):
            ring(p1, r1, s1, q1, d, q).wait_recv()
            r1[d, q] = p3[d, lax.rem(q, 2)] + r1[d, q]
            for n in range(n_sub):
                last_leg(d, q, n).start()

    def first(q):
        for d in range(2):
            ring(p1, r1, s1, q1, d, q).start()
        for d in range(2):
            ring(p2, r2, s2, q2, d, q).start()

    @pl.loop(0, n_half + 3)
    def _(it):
        @pl.when(it < n_half)
        def _():
            @pl.loop(0, 2)
            def _(ab):
                partial(it, ab)

                @pl.when(jnp.logical_and(ab == 0, it < n_half - 1))
                def _():
                    for other in range(2):
                        o_out(it + 1 + n_half * other).start()

        @pl.when(it == 1)
        def _():
            last(0)
            for d in range(2):
                ring(p2, r2, s2, q2, d, 1).start()
            last(1)

        @pl.when(it == 2)
        def _():
            first(2)

        for i in range(2, 4):
            @pl.when(it == i - 1)
            def _():
                for part in range(n_half):
                    weight(i, part).start()

        @pl.when(it == 3)
        def _():
            norm_copy.wait()
            comes_copy.wait()
            for i in range(3):
                for part in range(n_half):
                    weight(i, part).wait()

        @pl.when(it >= 3)
        def _():
            normalise(it - 3)

        @pl.when(it == n_half + 2)
        def _():
            ahead = queries(0)
            for n in range(n_sub):
                now, ahead = ahead, queries(n + 1) if n + 1 < n_sub else None
                attend(n, now)

        @pl.loop(0, n_sub)
        def _(n):
            @pl.when(jnp.logical_and(it >= 3, it < n_half + 2))
            def _():
                attend(n, queries(n))

            @pl.when(jnp.logical_and(it >= 2, it < n_half + 2))
            def _():
                finish(it - 2, n)

        @pl.when(it == 3)
        def _():
            for part in range(n_half):
                weight(3, part).wait()
            last(2)
            first(3)

        @pl.when(it == n_half)
        def _():
            w_out.wait_send()
            h_out.wait_send()
            for copy in t_out:
                copy.wait_send()

            @pl.loop(0, n_ep)
            def _(h):
                o_out_wait(h)

        @pl.when(it >= 3)
        def _():
            project(it - 3)

        @pl.when(it == 4)
        def _():
            last(3)

    @pl.loop(0, n_half)
    def _(q):
        for d in range(2):
            ring(p1, r1, s1, q1, d, q).wait_send()
            ring(p2, r2, s2, q2, d, q).wait_send()
            for n in range(n_sub):
                last_leg(d, q, n).wait_send()
        for jc in range(CORES):
            for n in range(n_sub):
                hop(q, jc, n, core, chip * CORES + jc).wait_send()
    for c in range(CORES):
        store(c).wait()


def solution(mesh):
    n_stages = mesh.shape['pp']
    n_ep = mesh.shape['ep']
    group_axes = ('data', 'pp')

    def device_step(expert_out, expert_id, slot_id, gate, resid, owner, norm_w, w_q, w_k, w_v, w_o):
        n_loc, capacity, model_dim = expert_out.shape[2:]
        cap = capacity // n_ep
        tok_dev, top_k = expert_id.shape[2:]
        seq_dev = owner.shape[1] // n_ep
        seq_len = tok_dev // seq_dev
        assert expert_out.shape[1] == 1 and seq_dev == n_ep
        half = model_dim // CORES
        slot_pad = -(-cap // 16) * 16
        n_half = n_ep // 2
        block = CORES * seq_len

        dims = (n_ep, n_stages, n_loc, cap, slot_pad, seq_len, top_k, half)
        f32, bf16 = jnp.float32, jnp.bfloat16
        n_sub = model_dim // min(512, half)
        assert n_half == 4

        def ringbuf(slots):
            return pltpu.VMEM((2, slots, block, half), f32)

        square = pltpu.VMEM((model_dim, model_dim), bf16)
        dma = pltpu.SemaphoreType.DMA
        z_owned = pl.pallas_call(
            functools.partial(stage_kernel, dims),
            out_shape=jax.ShapeDtypeStruct((tok_dev, model_dim), bf16),
            in_specs=[pl.BlockSpec(memory_space=pl.ANY)] * 11,
            out_specs=pl.BlockSpec(memory_space=pl.ANY),
            scratch_shapes=[
                pltpu.VMEM((n_ep, CORES * n_loc, slot_pad, half), bf16),
                pltpu.VMEM((CORES, tok_dev, half), bf16),
                pltpu.VMEM((n_ep, top_k, tok_dev), jnp.int32),
                pltpu.VMEM((n_ep, top_k, tok_dev), jnp.int32),
                pltpu.VMEM((n_ep, top_k, tok_dev), f32),
                pltpu.VMEM((1, n_ep * seq_dev), jnp.int32),
                pltpu.SMEM((1, n_ep * seq_dev), jnp.int32),
                pltpu.SMEM((1, n_ep * seq_dev), jnp.int32),
                pltpu.VMEM((tok_dev, 128), f32),
                pltpu.VMEM((3 * tok_dev // 2, CORES * n_loc * slot_pad), bf16),
                ringbuf(n_half), ringbuf(n_half), ringbuf(2), ringbuf(n_half), ringbuf(n_half), ringbuf(n_half), ringbuf(3),
                pltpu.VMEM((n_half, CORES, 2, seq_len, half), bf16),
                pltpu.VMEM((n_ep, seq_len, model_dim), bf16),
                pltpu.VMEM((1, model_dim), f32),
                square, square, square, square,
                pltpu.VMEM((2 * seq_len, model_dim), bf16),
                pltpu.VMEM((2 * seq_len, model_dim), bf16),
                dma((n_ep,)), dma((n_ep,)), dma((n_ep,)),
                dma, dma, dma,
                dma((3,)), dma((3, n_ep - 1)), dma((3, n_ep)),
                dma, dma, dma,
                dma((2, n_half)), dma((2, n_half)), dma((2, n_half, n_sub)),
                dma((2, n_half)), dma((2, n_half)), dma((2, n_half, n_sub)),
                dma((n_half, CORES, n_sub)), dma((CORES, n_half, n_sub)), dma((4, n_half)), dma((CORES,)), dma, dma,
            ],
            compiler_params=pltpu.CompilerParams(collective_id=0, has_side_effects=True, vmem_limit_bytes=67043328),
            name='stage',
        )(owner, expert_id[0, 0].T, slot_id[0, 0].T, gate[0, 0].T, expert_out[0, 0], resid[0, 0],
          norm_w, w_q[0], w_k[0], w_v[0], w_o[0])
        return z_owned.reshape(1, 1, tok_dev, model_dim)

    tok_spec = P(group_axes, None, 'ep', None)
    weight_spec = P('pp', None, None)
    in_specs = (P(group_axes, None, 'ep', None, None), tok_spec, tok_spec, tok_spec, tok_spec, P(group_axes, None), P('pp', None), weight_spec, weight_spec, weight_spec, weight_spec)
    return jax.shard_map(device_step, mesh=mesh, in_specs=in_specs, out_specs=tok_spec, check_vma=False)
```

```python
import functools

import jax
import jax.numpy as jnp
from jax import lax
from jax.experimental import pallas as pl
from jax.experimental.pallas import tpu as pltpu
from jax.sharding import PartitionSpec as P

HEAD_DIM = 128
NORM_EPS = 1e-6
MESH = pl.DeviceIdType.MESH
CORES = 2


def stage_kernel(dims, owner_ref, id_ref, slot_ref, gate_ref, out_ref, resid_ref, norm_ref, q_ref, k_ref, v_ref, o_ref, z_ref,
                   obuf, hbuf, ids, slots, gates, owners, goes, comes, table, wterm,
                   p1, p2, p3, r1, r2, r3, own, ysend, yland, norm, wq, wk, wv, wo, xs, mix,
                   o_loc, o_snd, o_rcv, h_loc, h_snd, h_rcv, t_loc, t_snd, t_rcv, w_snd, w_rcv, w_loc,
                   s1, s2, s3, q1, q2, q3, ys, yr, wt, zs, n_loc_sem, c_loc):
    n_ep, n_st, n_loc, cap, slot_pad, seq_len, top_k, half = dims
    n_chip = n_ep // CORES
    n_half = n_ep // 2
    tok_dev = n_ep * seq_len
    me = lax.axis_index('ep')
    rank = lax.axis_index('pp')
    core = lax.rem(me, CORES)
    chip = me // CORES
    sib = me + 1 - 2 * core
    nxt = lax.rem(rank + 1, n_st)
    prv = lax.rem(rank + n_st - 1, n_st)
    side = [lax.rem(me + n_ep - CORES, n_ep), lax.rem(me + CORES, n_ep)]
    my_cols = pl.ds(pl.multiple_of(core * half, 128), half)
    sib_cols = pl.ds(pl.multiple_of((1 - core) * half, 128), half)
    order = [q + n_half * ab for q in range(n_half) for ab in range(2)]

    raw = ((id_ref, ids), (slot_ref, slots), (gate_ref, gates))
    for i, (src, dst) in enumerate(raw):
        pltpu.make_async_copy(src, dst.at[me], t_loc.at[i]).start()
    barrier = pltpu.get_barrier_semaphore()
    for k in range(1, n_ep):
        pl.semaphore_signal(barrier, inc=1, device_id={'ep': lax.rem(me + k, n_ep)}, device_id_type=MESH)
    for other in (nxt, prv):
        for jc in range(CORES):
            pl.semaphore_signal(barrier, inc=1, device_id={'pp': other, 'ep': chip * CORES + jc}, device_id_type=MESH)
    def o_in(h):
        return pltpu.make_async_copy(out_ref.at[:, pl.ds(h * cap, cap), my_cols],
                                     obuf.at[h, pl.ds(core * n_loc, n_loc), pl.ds(0, cap)], o_loc.at[h])

    for h in order[:2]:
        o_in(h).start()
    h_copy = pltpu.make_async_copy(resid_ref.at[:, my_cols], hbuf.at[core], h_loc)
    h_copy.start()
    model = CORES * half
    strip = model // n_half

    def weight(i, part):
        src, dst = ((q_ref, wq), (k_ref, wk), (v_ref, wv), (o_ref, wo))[i]
        rows = pl.ds(part * strip, strip)
        return pltpu.make_async_copy(src.at[rows], dst.at[rows], wt.at[i, part])

    norm_copy = pltpu.make_async_copy(norm_ref, norm, n_loc_sem)
    norm_copy.start()
    comes_copy = pltpu.make_async_copy(owner_ref, comes, c_loc)
    comes_copy.start()
    def fill(first, stop):
        for i in range(first, stop):
            weight(i // n_half, i % n_half).start()

    fill(0, 3)
    if slot_pad > cap:
        for h in range(n_ep):
            obuf[h, :, cap:, :] = jnp.zeros((CORES * n_loc, slot_pad - cap, half), jnp.bfloat16)
    pl.semaphore_wait(barrier, n_ep - 1 + 2 * CORES)

    w_out = pltpu.make_async_remote_copy(owner_ref, owners, w_snd, w_rcv, device_id={'pp': prv}, device_id_type=MESH)
    w_out.start()
    def route(i, k, home, peer):
        src, dst = raw[i]
        return pltpu.make_async_remote_copy(src, dst.at[home], t_snd.at[i, k - 1], t_rcv.at[i, home],
                                            device_id={'ep': peer}, device_id_type=MESH)

    t_out = [route(i, k, me, lax.rem(me + k, n_ep))
             for k in (n_chip, n_chip - 1, n_chip + 1, 2, n_ep - 2, 1, n_ep - 1) for i in range(3)]
    for copy in t_out:
        copy.start()

    def o_out(h):
        return pltpu.make_async_remote_copy(out_ref.at[:, pl.ds(pl.multiple_of(h * cap, 8), cap), sib_cols],
                                            obuf.at[h, pl.ds(core * n_loc, n_loc), pl.ds(0, cap)],
                                            o_snd.at[h], o_rcv.at[h],
                                            device_id={'ep': sib}, device_id_type=MESH)

    h_out = pltpu.make_async_remote_copy(resid_ref.at[:, sib_cols], hbuf.at[core], h_snd, h_rcv,
                                         device_id={'ep': sib}, device_id_type=MESH)
    for ab in range(2):
        o_out(n_half * ab).start()
    h_out.start()

    fill(3, 7)
    w_out.wait_recv()
    goes_copy = pltpu.make_async_copy(owners, goes, w_loc)
    goes_copy.start()
    for h in order[2:4]:
        o_in(h).start()
    fill(7, 9)
    goes_copy.wait()

    def o_wait(h):
        pltpu.make_async_copy(out_ref.at[:, pl.ds(0, cap), my_cols],
                              obuf.at[h, pl.ds(core * n_loc, n_loc), pl.ds(0, cap)], o_loc.at[h]).wait()
        pltpu.make_async_remote_copy(out_ref.at[:, pl.ds(0, cap), sib_cols],
                                     obuf.at[h, pl.ds((1 - core) * n_loc, n_loc), pl.ds(0, cap)],
                                     o_snd.at[h], o_rcv.at[h],
                                     device_id={'ep': sib}, device_id_type=MESH).wait_recv()

    def ring(src, dst, snd, rcv, d, q):
        return pltpu.make_async_remote_copy(src.at[d, q], dst.at[d, q], snd.at[d, q], rcv.at[d, q],
                                            device_id={'ep': side[d]}, device_id_type=MESH)

    depth = CORES * n_loc * slot_pad
    width = min(256, half)
    tile = min(512, half)
    n_sub = model // tile
    leg = half // n_sub
    lane = lax.broadcasted_iota(jnp.int32, (seq_len, depth), 1).astype(jnp.float32)
    block = CORES * seq_len
    per = n_chip * CORES // 2

    def partial(q, ab):
        h = q + n_half * ab

        @pl.when(h != me)
        def _():
            for i in range(3):
                route(i, 1, h, h).wait_recv()

        @pl.when(h == me)
        def _():
            for i, (src, dst) in enumerate(raw):
                pltpu.make_async_copy(src, dst.at[me], t_loc.at[i]).wait()

        key = jnp.where(slots[h] >= 0, ids[h] * slot_pad + slots[h] - h * cap, -1).astype(jnp.float32)
        rows = jnp.concatenate([key, gates[h], jnp.zeros((128 - 2 * top_k, tok_dev), jnp.float32)], axis=0)
        table[...] = rows.T
        step = 1 - 2 * ab
        dest = [chip + 2, chip + n_chip + step, chip + n_chip - step, chip]
        picks = []
        for r in range(n_chip):
            for jc in range(CORES):
                j = lax.rem(dest[r], n_chip) * CORES + jc
                pick = 0
                for b in range(n_ep):
                    seq = goes[0, j * n_ep + b] - h * n_ep
                    pick = jnp.where(jnp.logical_and(seq >= 0, seq < n_ep), seq, pick)
                picks.append(pick)

        def chosen(pick, load):
            got = load(0)
            for s in range(1, n_ep):
                got = jnp.where(pick == s, load(s), got)
            return got

        base = (chip * depth).astype(jnp.float32)
        dsts = [p1.at[ab, q], p2.at[1 - ab, q], p3.at[ab, lax.rem(q, 2)], own.at[ab, lax.rem(q, 3)]]
        for part in range(2):
            mine = picks[part * per:(part + 1) * per]
            for b, pick in enumerate(mine):
                rt = chosen(pick, lambda s: table[s * seq_len:(s + 1) * seq_len, :])
                w = jnp.zeros((seq_len, depth), jnp.float32)
                for j in range(top_k):
                    key = rt[:, j:j + 1] - base
                    w = jnp.where(lane == key, rt[:, top_k + j:top_k + j + 1], w)
                hi = w.astype(jnp.bfloat16)
                rest = w - hi.astype(jnp.float32)
                mid = rest.astype(jnp.bfloat16)
                low = (rest - mid.astype(jnp.float32)).astype(jnp.bfloat16)
                for t, term in enumerate((hi, mid, low)):
                    wterm[pl.ds((t * per + b) * seq_len, seq_len), :] = term
            if part == 0:
                o_wait(h)

            @pl.loop(0, half // width)
            def _(n):
                cols = pl.ds(pl.multiple_of(n * width, width), width)
                slots_in = obuf[h, :, :, cols].reshape(depth, width)
                res = jnp.dot(wterm[...], slots_in, preferred_element_type=jnp.float32)
                span = per * seq_len
                res = res[:span] + (res[span:2 * span] + res[2 * span:])
                for r in range(2):
                    dsts[2 * part + r][:, cols] = res[r * block:(r + 1) * block]

            @pl.when(h // CORES == chip)
            def _():
                hc = lax.rem(h, CORES)
                if part == 0:
                    @pl.when(hc == 0)
                    def _():
                        h_copy.wait()
                        h_out.wait_recv()

                @pl.loop(0, half // width)
                def _(n):
                    cols = pl.ds(pl.multiple_of(n * width, width), width)
                    for b, pick in enumerate(mine):
                        dst = dsts[2 * part + b // CORES]
                        rs = slice((b % CORES) * seq_len, (b % CORES + 1) * seq_len)
                        held = chosen(pick, lambda s: hbuf[hc, s * seq_len:(s + 1) * seq_len, cols].astype(jnp.float32))
                        dst[rs, cols] = dst[rs, cols] + held

            if part == 0:
                for d in range(2):
                    @pl.when(jnp.logical_and(ab == d, q <= 1))
                    def _():
                        ring(p1, r1, s1, q1, d, q).start()

                    @pl.when(jnp.logical_and(ab == d, q == 0))
                    def _():
                        ring(p2, r2, s2, q2, 1 - d, q).start()

    def o_out_wait(h):
        pltpu.make_async_remote_copy(out_ref.at[:, pl.ds(0, cap), sib_cols],
                                     obuf.at[h, pl.ds(core * n_loc, n_loc), pl.ds(0, cap)],
                                     o_snd.at[h], o_rcv.at[h],
                                     device_id={'ep': sib}, device_id_type=MESH).wait_send()

    def sub(n):
        return pl.ds(pl.multiple_of(n * leg, leg), leg)

    def last_leg(d, q, n):
        return pltpu.make_async_remote_copy(r1.at[d, q, :, sub(n)], r3.at[d, q, :, sub(n)], s3.at[d, q, n], q3.at[d, q, n],
                                            device_id={'ep': side[d]}, device_id_type=MESH)

    def hop(q, jc, n, c, to):
        cols = pl.ds(pl.multiple_of(c * half + n * leg, leg), leg)
        return pltpu.make_async_remote_copy(ysend.at[q, jc, :, :, sub(n)], yland.at[pl.ds(2 * q, 2), :, cols],
                                            ys.at[q, jc, n], yr.at[c, q, n],
                                            device_id={'pp': nxt, 'ep': to}, device_id_type=MESH)

    def finish(q, n):
        @pl.when(n == 0)
        def _():
            for d in range(2):
                ring(p2, r2, s2, q2, d, q).wait_recv()
        cols = sub(n)
        for d in range(2):
            last_leg(d, q, n).wait_recv()
        for ab in range(2):
            total = own[ab, lax.rem(q, 3), :, cols] + (r3[ab, q, :, cols] + r2[1 - ab, q, :, cols])
            rounded = total.astype(jnp.bfloat16)
            for jc in range(CORES):
                ysend[q, jc, ab, :, cols] = rounded[jc * seq_len:(jc + 1) * seq_len]
        for jc in range(CORES):
            hop(q, jc, n, core, chip * CORES + jc).start()

    n_tok = 2 * seq_len
    n_row = tile // HEAD_DIM * n_tok
    row = lax.broadcasted_iota(jnp.int32, (n_row, n_tok), 0) % n_tok
    col = lax.broadcasted_iota(jnp.int32, (n_row, n_tok), 1)
    causal = jnp.logical_and(row >= col, row // seq_len == col // seq_len)

    def normalise(q):
        for c in range(CORES):
            for n in range(n_sub):
                hop(q, 0, n, c, me).wait_recv()
        for ab in range(2):
            y = yland[2 * q + ab].astype(jnp.float32)
            inv = lax.rsqrt(jnp.mean(y * y, axis=-1, keepdims=True) + NORM_EPS)
            xs[ab * seq_len:(ab + 1) * seq_len, :] = (y * inv * norm[...]).astype(jnp.bfloat16)

    def queries(n):
        cols = pl.ds(n * tile if isinstance(n, int) else pl.multiple_of(n * tile, tile), tile)
        x = xs[...]
        return [jnp.dot(x, w[:, cols], preferred_element_type=jnp.float32).astype(jnp.bfloat16) for w in (wq, wk, wv)]

    def attend(n, qkv):
        cols = pl.ds(n * tile if isinstance(n, int) else pl.multiple_of(n * tile, tile), tile)
        qt, kt, vt = qkv
        heads = [slice(hd * HEAD_DIM, (hd + 1) * HEAD_DIM) for hd in range(tile // HEAD_DIM)]
        scores = jnp.concatenate([lax.dot_general(qt[:, hs], kt[:, hs], (((1,), (1,)), ((), ())),
                                                  preferred_element_type=jnp.float32) for hs in heads], axis=0)
        scores = jnp.where(causal, scores * (HEAD_DIM ** -0.5), -1e30)
        raised = jnp.exp(scores - jnp.max(scores, axis=-1, keepdims=True))
        probs = (raised / jnp.sum(raised, axis=-1, keepdims=True)).astype(jnp.bfloat16)
        mixed = [jnp.dot(probs[i * n_tok:(i + 1) * n_tok], vt[:, hs], preferred_element_type=jnp.float32)
                 for i, hs in enumerate(heads)]
        mix[:, cols] = jnp.concatenate(mixed, axis=1).astype(jnp.bfloat16)

    def store(c):
        return pltpu.make_async_copy(hbuf.at[c], z_ref.at[:, pl.ds(pl.multiple_of(c * half, 128), half)], zs.at[c])

    def project_tile(q, c, n):
        def at(start):
            return pl.ds(start if isinstance(start, int) else pl.multiple_of(start, tile), tile)

        cols = at(c * half + n * tile)
        out = jnp.dot(mix[...], wo[:, cols], preferred_element_type=jnp.float32).astype(jnp.bfloat16).astype(jnp.float32)
        z = []
        for ab in range(2):
            y = yland[2 * q + ab, :, cols].astype(jnp.float32)
            z.append((y + out[ab * seq_len:(ab + 1) * seq_len]).astype(jnp.bfloat16))
        cols = at(n * tile)
        for b in range(n_ep):
            home = comes[0, me * n_ep + b] // n_ep
            rs = pl.ds(b * seq_len, seq_len)
            hbuf[c, rs, cols] = jnp.where(home == q, z[0], jnp.where(home == q + n_half, z[1], hbuf[c, rs, cols]))

    def project(q):
        @pl.loop(0, CORES)
        def _(c):
            @pl.loop(0, half // tile)
            def _(n):
                project_tile(q, c, n)

    def project_last():
        for c in range(CORES):
            for n in range(half // tile):
                project_tile(n_half - 1, c, n)
            store(c).start()

    def last(q):
        for d in range(2):
            ring(p1, r1, s1, q1, d, q).wait_recv()
            r1[d, q] = p3[d, lax.rem(q, 2)] + r1[d, q]
            for n in range(n_sub):
                last_leg(d, q, n).start()

    def first(q):
        for d in range(2):
            ring(p1, r1, s1, q1, d, q).start()
        for d in range(2):
            ring(p2, r2, s2, q2, d, q).start()

    @pl.loop(0, n_half + 3)
    def _(it):
        @pl.when(it < n_half)
        def _():
            @pl.loop(0, 2)
            def _(ab):
                partial(it, ab)

                @pl.when(jnp.logical_and(ab == 0, it < n_half - 1))
                def _():
                    for other in range(2):
                        o_out(it + 1 + n_half * other).start()

        @pl.when(it == 1)
        def _():
            last(0)
            for d in range(2):
                ring(p2, r2, s2, q2, d, 1).start()
            last(1)

        @pl.when(it == 2)
        def _():
            first(2)

        @pl.when(it == 0)
        def _():
            for h in order[4:]:
                o_in(h).start()

        @pl.when(it == 1)
        def _():
            fill(9, 12)

        @pl.when(it == 2)
        def _():
            fill(12, 16)

        @pl.when(it == 3)
        def _():
            norm_copy.wait()
            comes_copy.wait()
            for i in range(3):
                for part in range(n_half):
                    weight(i, part).wait()

        @pl.when(it >= 3)
        def _():
            normalise(it - 3)

        @pl.when(it == n_half + 2)
        def _():
            ahead = queries(0)
            for n in range(n_sub):
                now, ahead = ahead, queries(n + 1) if n + 1 < n_sub else None
                attend(n, now)

        @pl.loop(0, n_sub)
        def _(n):
            @pl.when(jnp.logical_and(it >= 3, it < n_half + 2))
            def _():
                attend(n, queries(n))

            @pl.when(jnp.logical_and(it >= 2, it < n_half + 2))
            def _():
                finish(it - 2, n)

        @pl.when(it == 3)
        def _():
            for part in range(n_half):
                weight(3, part).wait()
            last(2)
            first(3)

        @pl.when(it == n_half)
        def _():
            w_out.wait_send()
            h_out.wait_send()
            for copy in t_out:
                copy.wait_send()

            @pl.loop(0, n_ep)
            def _(h):
                o_out_wait(h)

        @pl.when(jnp.logical_and(it >= 3, it < n_half + 2))
        def _():
            project(it - 3)

        @pl.when(it == n_half + 2)
        def _():
            project_last()

        @pl.when(it == 4)
        def _():
            last(3)

    @pl.loop(0, n_half)
    def _(q):
        for d in range(2):
            ring(p1, r1, s1, q1, d, q).wait_send()
            ring(p2, r2, s2, q2, d, q).wait_send()
            for n in range(n_sub):
                last_leg(d, q, n).wait_send()
        for jc in range(CORES):
            for n in range(n_sub):
                hop(q, jc, n, core, chip * CORES + jc).wait_send()
    for c in range(CORES):
        store(c).wait()


def solution(mesh):
    n_stages = mesh.shape['pp']
    n_ep = mesh.shape['ep']
    group_axes = ('data', 'pp')

    def device_step(expert_out, expert_id, slot_id, gate, resid, owner, norm_w, w_q, w_k, w_v, w_o):
        n_loc, capacity, model_dim = expert_out.shape[2:]
        cap = capacity // n_ep
        tok_dev, top_k = expert_id.shape[2:]
        seq_dev = owner.shape[1] // n_ep
        seq_len = tok_dev // seq_dev
        assert expert_out.shape[1] == 1 and seq_dev == n_ep
        half = model_dim // CORES
        slot_pad = -(-cap // 16) * 16
        n_half = n_ep // 2
        block = CORES * seq_len

        dims = (n_ep, n_stages, n_loc, cap, slot_pad, seq_len, top_k, half)
        f32, bf16 = jnp.float32, jnp.bfloat16
        n_sub = model_dim // min(512, half)
        assert n_half == 4

        def ringbuf(slots):
            return pltpu.VMEM((2, slots, block, half), f32)

        square = pltpu.VMEM((model_dim, model_dim), bf16)
        dma = pltpu.SemaphoreType.DMA
        z_owned = pl.pallas_call(
            functools.partial(stage_kernel, dims),
            out_shape=jax.ShapeDtypeStruct((tok_dev, model_dim), bf16),
            in_specs=[pl.BlockSpec(memory_space=pl.ANY)] * 11,
            out_specs=pl.BlockSpec(memory_space=pl.ANY),
            scratch_shapes=[
                pltpu.VMEM((n_ep, CORES * n_loc, slot_pad, half), bf16),
                pltpu.VMEM((CORES, tok_dev, half), bf16),
                pltpu.VMEM((n_ep, top_k, tok_dev), jnp.int32),
                pltpu.VMEM((n_ep, top_k, tok_dev), jnp.int32),
                pltpu.VMEM((n_ep, top_k, tok_dev), f32),
                pltpu.VMEM((1, n_ep * seq_dev), jnp.int32),
                pltpu.SMEM((1, n_ep * seq_dev), jnp.int32),
                pltpu.SMEM((1, n_ep * seq_dev), jnp.int32),
                pltpu.VMEM((tok_dev, 128), f32),
                pltpu.VMEM((3 * tok_dev // 2, CORES * n_loc * slot_pad), bf16),
                ringbuf(n_half), ringbuf(n_half), ringbuf(2), ringbuf(n_half), ringbuf(n_half), ringbuf(n_half), ringbuf(3),
                pltpu.VMEM((n_half, CORES, 2, seq_len, half), bf16),
                pltpu.VMEM((n_ep, seq_len, model_dim), bf16),
                pltpu.VMEM((1, model_dim), f32),
                square, square, square, square,
                pltpu.VMEM((2 * seq_len, model_dim), bf16),
                pltpu.VMEM((2 * seq_len, model_dim), bf16),
                dma((n_ep,)), dma((n_ep,)), dma((n_ep,)),
                dma, dma, dma,
                dma((3,)), dma((3, n_ep - 1)), dma((3, n_ep)),
                dma, dma, dma,
                dma((2, n_half)), dma((2, n_half)), dma((2, n_half, n_sub)),
                dma((2, n_half)), dma((2, n_half)), dma((2, n_half, n_sub)),
                dma((n_half, CORES, n_sub)), dma((CORES, n_half, n_sub)), dma((4, n_half)), dma((CORES,)), dma, dma,
            ],
            compiler_params=pltpu.CompilerParams(collective_id=0, has_side_effects=True, vmem_limit_bytes=67043328),
            name='stage',
        )(owner, expert_id[0, 0].T, slot_id[0, 0].T, gate[0, 0].T, expert_out[0, 0], resid[0, 0],
          norm_w, w_q[0], w_k[0], w_v[0], w_o[0])
        return z_owned.reshape(1, 1, tok_dev, model_dim)

    tok_spec = P(group_axes, None, 'ep', None)
    weight_spec = P('pp', None, None)
    in_specs = (P(group_axes, None, 'ep', None, None), tok_spec, tok_spec, tok_spec, tok_spec, P(group_axes, None), P('pp', None), weight_spec, weight_spec, weight_spec, weight_spec)
    return jax.shard_map(device_step, mesh=mesh, in_specs=in_specs, out_specs=tok_spec, check_vma=False)
```

```python
import functools

import jax
import jax.numpy as jnp
from jax import lax
from jax.experimental import pallas as pl
from jax.experimental.pallas import tpu as pltpu
from jax.sharding import PartitionSpec as P

HEAD_DIM = 128
NORM_EPS = 1e-6
MESH = pl.DeviceIdType.MESH
CORES = 2


def stage_kernel(dims, owner_ref, id_ref, slot_ref, gate_ref, out_ref, resid_ref, norm_ref, q_ref, k_ref, v_ref, o_ref, z_ref,
                   obuf, hbuf, ids, slots, gates, owners, goes, comes, table, wterm,
                   p1, p2, p3, r1, r2, r3, own, ysend, yland, norm, wq, wk, wv, wo, xs, mix,
                   o_loc, o_snd, o_rcv, h_loc, h_snd, h_rcv, t_loc, t_snd, t_rcv, w_snd, w_rcv, w_loc,
                   s1, s2, s3, q1, q2, q3, ys, yr, wt, zs, n_loc_sem, c_loc):
    n_ep, n_st, n_loc, cap, slot_pad, seq_len, top_k, half = dims
    n_chip = n_ep // CORES
    n_half = n_ep // 2
    tok_dev = n_ep * seq_len
    me = lax.axis_index('ep')
    rank = lax.axis_index('pp')
    core = lax.rem(me, CORES)
    chip = me // CORES
    sib = me + 1 - 2 * core
    nxt = lax.rem(rank + 1, n_st)
    prv = lax.rem(rank + n_st - 1, n_st)
    side = [lax.rem(me + n_ep - CORES, n_ep), lax.rem(me + CORES, n_ep)]
    my_cols = pl.ds(pl.multiple_of(core * half, 128), half)
    sib_cols = pl.ds(pl.multiple_of((1 - core) * half, 128), half)
    order = [q + n_half * ab for q in range(n_half) for ab in range(2)]

    raw = ((id_ref, ids), (slot_ref, slots), (gate_ref, gates))
    for i, (src, dst) in enumerate(raw):
        pltpu.make_async_copy(src, dst.at[me], t_loc.at[i]).start()
    barrier = pltpu.get_barrier_semaphore()
    for k in range(1, n_ep):
        pl.semaphore_signal(barrier, inc=1, device_id={'ep': lax.rem(me + k, n_ep)}, device_id_type=MESH)
    for other in (nxt, prv):
        for jc in range(CORES):
            pl.semaphore_signal(barrier, inc=1, device_id={'pp': other, 'ep': chip * CORES + jc}, device_id_type=MESH)
    def o_in(h):
        return pltpu.make_async_copy(out_ref.at[:, pl.ds(h * cap, cap), my_cols],
                                     obuf.at[h, pl.ds(core * n_loc, n_loc), pl.ds(0, cap)], o_loc.at[h])

    for h in order[:2]:
        o_in(h).start()
    h_copy = pltpu.make_async_copy(resid_ref.at[:, my_cols], hbuf.at[core], h_loc)
    h_copy.start()
    model = CORES * half
    strip = model // n_half

    def weight(i, part):
        src, dst = ((q_ref, wq), (k_ref, wk), (v_ref, wv), (o_ref, wo))[i]
        rows = pl.ds(part * strip, strip)
        return pltpu.make_async_copy(src.at[rows], dst.at[rows], wt.at[i, part])

    norm_copy = pltpu.make_async_copy(norm_ref, norm, n_loc_sem)
    norm_copy.start()
    comes_copy = pltpu.make_async_copy(owner_ref, comes, c_loc)
    comes_copy.start()
    def fill(first, stop):
        for i in range(first, stop):
            weight(i // n_half, i % n_half).start()

    fill(0, 3)
    if slot_pad > cap:
        for h in range(n_ep):
            obuf[h, :, cap:, :] = jnp.zeros((CORES * n_loc, slot_pad - cap, half), jnp.bfloat16)
    pl.semaphore_wait(barrier, n_ep - 1 + 2 * CORES)

    w_out = pltpu.make_async_remote_copy(owner_ref, owners, w_snd, w_rcv, device_id={'pp': prv}, device_id_type=MESH)
    w_out.start()
    def route(i, k, home, peer):
        src, dst = raw[i]
        return pltpu.make_async_remote_copy(src, dst.at[home], t_snd.at[i, k - 1], t_rcv.at[i, home],
                                            device_id={'ep': peer}, device_id_type=MESH)

    t_out = [route(i, k, me, lax.rem(me + k, n_ep))
             for k in (n_chip, n_chip - 1, n_chip + 1, 2, n_ep - 2, 1, n_ep - 1) for i in range(3)]
    for copy in t_out:
        copy.start()

    def o_out(h):
        return pltpu.make_async_remote_copy(out_ref.at[:, pl.ds(pl.multiple_of(h * cap, 8), cap), sib_cols],
                                            obuf.at[h, pl.ds(core * n_loc, n_loc), pl.ds(0, cap)],
                                            o_snd.at[h], o_rcv.at[h],
                                            device_id={'ep': sib}, device_id_type=MESH)

    h_out = pltpu.make_async_remote_copy(resid_ref.at[:, sib_cols], hbuf.at[core], h_snd, h_rcv,
                                         device_id={'ep': sib}, device_id_type=MESH)
    for ab in range(2):
        o_out(n_half * ab).start()
    h_out.start()

    fill(3, 7)
    w_out.wait_recv()
    goes_copy = pltpu.make_async_copy(owners, goes, w_loc)
    goes_copy.start()
    for h in order[2:4]:
        o_in(h).start()
    fill(7, 9)
    goes_copy.wait()

    def o_wait(h):
        pltpu.make_async_copy(out_ref.at[:, pl.ds(0, cap), my_cols],
                              obuf.at[h, pl.ds(core * n_loc, n_loc), pl.ds(0, cap)], o_loc.at[h]).wait()
        pltpu.make_async_remote_copy(out_ref.at[:, pl.ds(0, cap), sib_cols],
                                     obuf.at[h, pl.ds((1 - core) * n_loc, n_loc), pl.ds(0, cap)],
                                     o_snd.at[h], o_rcv.at[h],
                                     device_id={'ep': sib}, device_id_type=MESH).wait_recv()

    def ring(src, dst, snd, rcv, d, q):
        return pltpu.make_async_remote_copy(src.at[d, q], dst.at[d, q], snd.at[d, q], rcv.at[d, q],
                                            device_id={'ep': side[d]}, device_id_type=MESH)

    depth = CORES * n_loc * slot_pad
    width = min(256, half)
    tile = min(512, half)
    n_sub = model // tile
    per_seq = n_sub // CORES
    leg = seq_len // per_seq
    lane = lax.broadcasted_iota(jnp.int32, (seq_len, depth), 1).astype(jnp.float32)
    block = CORES * seq_len
    per = n_chip * CORES // 2

    def partial(q, ab):
        h = q + n_half * ab

        @pl.when(h != me)
        def _():
            for i in range(3):
                route(i, 1, h, h).wait_recv()

        @pl.when(h == me)
        def _():
            for i, (src, dst) in enumerate(raw):
                pltpu.make_async_copy(src, dst.at[me], t_loc.at[i]).wait()

        key = jnp.where(slots[h] >= 0, ids[h] * slot_pad + slots[h] - h * cap, -1).astype(jnp.float32)
        rows = jnp.concatenate([key, gates[h], jnp.zeros((128 - 2 * top_k, tok_dev), jnp.float32)], axis=0)
        table[...] = rows.T
        step = 1 - 2 * ab
        dest = [chip + 2, chip + n_chip + step, chip + n_chip - step, chip]
        picks = []
        for r in range(n_chip):
            for jc in range(CORES):
                j = lax.rem(dest[r], n_chip) * CORES + jc
                pick = 0
                for b in range(n_ep):
                    seq = goes[0, j * n_ep + b] - h * n_ep
                    pick = jnp.where(jnp.logical_and(seq >= 0, seq < n_ep), seq, pick)
                picks.append(pick)

        def chosen(pick, load):
            got = load(0)
            for s in range(1, n_ep):
                got = jnp.where(pick == s, load(s), got)
            return got

        base = (chip * depth).astype(jnp.float32)
        dsts = [p1.at[ab, q], p2.at[1 - ab, q], p3.at[ab, lax.rem(q, 2)], own.at[ab, lax.rem(q, 3)]]
        for part in range(2):
            mine = picks[part * per:(part + 1) * per]
            for b, pick in enumerate(mine):
                rt = chosen(pick, lambda s: table[s * seq_len:(s + 1) * seq_len, :])
                w = jnp.zeros((seq_len, depth), jnp.float32)
                for j in range(top_k):
                    key = rt[:, j:j + 1] - base
                    w = jnp.where(lane == key, rt[:, top_k + j:top_k + j + 1], w)
                hi = w.astype(jnp.bfloat16)
                rest = w - hi.astype(jnp.float32)
                mid = rest.astype(jnp.bfloat16)
                low = (rest - mid.astype(jnp.float32)).astype(jnp.bfloat16)
                for t, term in enumerate((hi, mid, low)):
                    wterm[pl.ds((t * per + b) * seq_len, seq_len), :] = term
            if part == 0:
                o_wait(h)

            @pl.loop(0, half // width)
            def _(n):
                cols = pl.ds(pl.multiple_of(n * width, width), width)
                slots_in = obuf[h, :, :, cols].reshape(depth, width)
                res = jnp.dot(wterm[...], slots_in, preferred_element_type=jnp.float32)
                span = per * seq_len
                res = res[:span] + (res[span:2 * span] + res[2 * span:])
                for r in range(2):
                    dsts[2 * part + r][:, cols] = res[r * block:(r + 1) * block]

            @pl.when(h // CORES == chip)
            def _():
                hc = lax.rem(h, CORES)
                if part == 0:
                    @pl.when(hc == 0)
                    def _():
                        h_copy.wait()
                        h_out.wait_recv()

                @pl.loop(0, half // width)
                def _(n):
                    cols = pl.ds(pl.multiple_of(n * width, width), width)
                    for b, pick in enumerate(mine):
                        dst = dsts[2 * part + b // CORES]
                        rs = slice((b % CORES) * seq_len, (b % CORES + 1) * seq_len)
                        held = chosen(pick, lambda s: hbuf[hc, s * seq_len:(s + 1) * seq_len, cols].astype(jnp.float32))
                        dst[rs, cols] = dst[rs, cols] + held

            if part == 0:
                for d in range(2):
                    @pl.when(jnp.logical_and(ab == d, q <= 1))
                    def _():
                        ring(p1, r1, s1, q1, d, q).start()

                    @pl.when(jnp.logical_and(ab == d, q == 0))
                    def _():
                        ring(p2, r2, s2, q2, 1 - d, q).start()

    def o_out_wait(h):
        pltpu.make_async_remote_copy(out_ref.at[:, pl.ds(0, cap), sib_cols],
                                     obuf.at[h, pl.ds(core * n_loc, n_loc), pl.ds(0, cap)],
                                     o_snd.at[h], o_rcv.at[h],
                                     device_id={'ep': sib}, device_id_type=MESH).wait_send()

    def sub(n):
        return pl.ds(pl.multiple_of(n * leg, leg), leg)

    def last_leg(d, q, n):
        return pltpu.make_async_remote_copy(r1.at[d, q, sub(n)], r3.at[d, q, sub(n)], s3.at[d, q, n], q3.at[d, q, n],
                                            device_id={'ep': side[d]}, device_id_type=MESH)

    def hop(q, jc, m, c, to):
        return pltpu.make_async_remote_copy(ysend.at[q, jc, :, sub(m)],
                                            yland.at[pl.ds(2 * q, 2), sub(m), pl.ds(pl.multiple_of(c * half, 128), half)],
                                            ys.at[q, jc, m], yr.at[c, q, m],
                                            device_id={'pp': nxt, 'ep': to}, device_id_type=MESH)

    def finish(q, n):
        @pl.when(n == 0)
        def _():
            for d in range(2):
                ring(p2, r2, s2, q2, d, q).wait_recv()
        rows = sub(n)
        jc, m = lax.div(n, per_seq), lax.rem(n, per_seq)
        for d in range(2):
            last_leg(d, q, n).wait_recv()
        for ab in range(2):
            total = own[ab, lax.rem(q, 3), rows] + (r3[ab, q, rows] + r2[1 - ab, q, rows])
            ysend[q, jc, ab, sub(m)] = total.astype(jnp.bfloat16)
        hop(q, jc, m, core, chip * CORES + jc).start()

    n_tok = 2 * seq_len
    n_row = tile // HEAD_DIM * n_tok
    row = lax.broadcasted_iota(jnp.int32, (n_row, n_tok), 0) % n_tok
    col = lax.broadcasted_iota(jnp.int32, (n_row, n_tok), 1)
    causal = jnp.logical_and(row >= col, row // seq_len == col // seq_len)

    def normalise(q):
        for c in range(CORES):
            for m in range(per_seq):
                hop(q, 0, m, c, me).wait_recv()
        for ab in range(2):
            y = yland[2 * q + ab].astype(jnp.float32)
            inv = lax.rsqrt(jnp.mean(y * y, axis=-1, keepdims=True) + NORM_EPS)
            xs[ab * seq_len:(ab + 1) * seq_len, :] = (y * inv * norm[...]).astype(jnp.bfloat16)

    def queries(n):
        cols = pl.ds(n * tile if isinstance(n, int) else pl.multiple_of(n * tile, tile), tile)
        x = xs[...]
        return [jnp.dot(x, w[:, cols], preferred_element_type=jnp.float32).astype(jnp.bfloat16) for w in (wq, wk, wv)]

    def attend(n, qkv):
        cols = pl.ds(n * tile if isinstance(n, int) else pl.multiple_of(n * tile, tile), tile)
        qt, kt, vt = qkv
        heads = [slice(hd * HEAD_DIM, (hd + 1) * HEAD_DIM) for hd in range(tile // HEAD_DIM)]
        scores = jnp.concatenate([lax.dot_general(qt[:, hs], kt[:, hs], (((1,), (1,)), ((), ())),
                                                  preferred_element_type=jnp.float32) for hs in heads], axis=0)
        scores = jnp.where(causal, scores * (HEAD_DIM ** -0.5), -1e30)
        raised = jnp.exp(scores - jnp.max(scores, axis=-1, keepdims=True))
        probs = (raised / jnp.sum(raised, axis=-1, keepdims=True)).astype(jnp.bfloat16)
        mixed = [jnp.dot(probs[i * n_tok:(i + 1) * n_tok], vt[:, hs], preferred_element_type=jnp.float32)
                 for i, hs in enumerate(heads)]
        mix[:, cols] = jnp.concatenate(mixed, axis=1).astype(jnp.bfloat16)

    def store(c):
        return pltpu.make_async_copy(hbuf.at[c], z_ref.at[:, pl.ds(pl.multiple_of(c * half, 128), half)], zs.at[c])

    def project_tile(q, c, n):
        def at(start):
            return pl.ds(start if isinstance(start, int) else pl.multiple_of(start, tile), tile)

        cols = at(c * half + n * tile)
        out = jnp.dot(mix[...], wo[:, cols], preferred_element_type=jnp.float32).astype(jnp.bfloat16).astype(jnp.float32)
        z = []
        for ab in range(2):
            y = yland[2 * q + ab, :, cols].astype(jnp.float32)
            z.append((y + out[ab * seq_len:(ab + 1) * seq_len]).astype(jnp.bfloat16))
        cols = at(n * tile)
        for b in range(n_ep):
            home = comes[0, me * n_ep + b] // n_ep
            rs = pl.ds(b * seq_len, seq_len)
            hbuf[c, rs, cols] = jnp.where(home == q, z[0], jnp.where(home == q + n_half, z[1], hbuf[c, rs, cols]))

    def project(q):
        @pl.loop(0, CORES)
        def _(c):
            @pl.loop(0, half // tile)
            def _(n):
                project_tile(q, c, n)

    def project_last():
        for c in range(CORES):
            for n in range(half // tile):
                project_tile(n_half - 1, c, n)
            store(c).start()

    def last(q):
        for d in range(2):
            ring(p1, r1, s1, q1, d, q).wait_recv()
            r1[d, q] = p3[d, lax.rem(q, 2)] + r1[d, q]
            for n in range(n_sub):
                last_leg(d, q, n).start()

    def first(q):
        for d in range(2):
            ring(p1, r1, s1, q1, d, q).start()
        for d in range(2):
            ring(p2, r2, s2, q2, d, q).start()

    @pl.loop(0, n_half + 3)
    def _(it):
        @pl.when(it < n_half)
        def _():
            @pl.loop(0, 2)
            def _(ab):
                partial(it, ab)

                @pl.when(jnp.logical_and(ab == 0, it < n_half - 1))
                def _():
                    for other in range(2):
                        o_out(it + 1 + n_half * other).start()

        @pl.when(it == 1)
        def _():
            last(0)
            for d in range(2):
                ring(p2, r2, s2, q2, d, 1).start()
            last(1)

        @pl.when(it == 2)
        def _():
            first(2)

        @pl.when(it == 0)
        def _():
            for h in order[4:]:
                o_in(h).start()

        @pl.when(it == 1)
        def _():
            fill(9, 12)

        @pl.when(it == 2)
        def _():
            fill(12, 16)

        @pl.when(it == 3)
        def _():
            norm_copy.wait()
            comes_copy.wait()
            for i in range(3):
                for part in range(n_half):
                    weight(i, part).wait()

        @pl.when(it >= 3)
        def _():
            normalise(it - 3)

        @pl.when(it == n_half + 2)
        def _():
            ahead = queries(0)
            for n in range(n_sub):
                now, ahead = ahead, queries(n + 1) if n + 1 < n_sub else None
                attend(n, now)

        @pl.loop(0, n_sub)
        def _(n):
            @pl.when(jnp.logical_and(it >= 3, it < n_half + 2))
            def _():
                attend(n, queries(n))

            @pl.when(jnp.logical_and(it >= 2, it < n_half + 2))
            def _():
                finish(it - 2, n)

        @pl.when(it == 3)
        def _():
            for part in range(n_half):
                weight(3, part).wait()
            last(2)
            first(3)

        @pl.when(it == n_half)
        def _():
            w_out.wait_send()
            h_out.wait_send()
            for copy in t_out:
                copy.wait_send()

            @pl.loop(0, n_ep)
            def _(h):
                o_out_wait(h)

        @pl.when(jnp.logical_and(it >= 3, it < n_half + 2))
        def _():
            project(it - 3)

        @pl.when(it == n_half + 2)
        def _():
            project_last()

        @pl.when(it == 4)
        def _():
            last(3)

    @pl.loop(0, n_half)
    def _(q):
        for d in range(2):
            ring(p1, r1, s1, q1, d, q).wait_send()
            ring(p2, r2, s2, q2, d, q).wait_send()
            for n in range(n_sub):
                last_leg(d, q, n).wait_send()
        for jc in range(CORES):
            for m in range(per_seq):
                hop(q, jc, m, core, chip * CORES + jc).wait_send()
    for c in range(CORES):
        store(c).wait()


def solution(mesh):
    n_stages = mesh.shape['pp']
    n_ep = mesh.shape['ep']
    group_axes = ('data', 'pp')

    def device_step(expert_out, expert_id, slot_id, gate, resid, owner, norm_w, w_q, w_k, w_v, w_o):
        n_loc, capacity, model_dim = expert_out.shape[2:]
        cap = capacity // n_ep
        tok_dev, top_k = expert_id.shape[2:]
        seq_dev = owner.shape[1] // n_ep
        seq_len = tok_dev // seq_dev
        assert expert_out.shape[1] == 1 and seq_dev == n_ep
        half = model_dim // CORES
        slot_pad = -(-cap // 16) * 16
        n_half = n_ep // 2
        block = CORES * seq_len

        dims = (n_ep, n_stages, n_loc, cap, slot_pad, seq_len, top_k, half)
        f32, bf16 = jnp.float32, jnp.bfloat16
        n_sub = model_dim // min(512, half)
        assert n_half == 4

        def ringbuf(slots):
            return pltpu.VMEM((2, slots, block, half), f32)

        square = pltpu.VMEM((model_dim, model_dim), bf16)
        dma = pltpu.SemaphoreType.DMA
        z_owned = pl.pallas_call(
            functools.partial(stage_kernel, dims),
            out_shape=jax.ShapeDtypeStruct((tok_dev, model_dim), bf16),
            in_specs=[pl.BlockSpec(memory_space=pl.ANY)] * 11,
            out_specs=pl.BlockSpec(memory_space=pl.ANY),
            scratch_shapes=[
                pltpu.VMEM((n_ep, CORES * n_loc, slot_pad, half), bf16),
                pltpu.VMEM((CORES, tok_dev, half), bf16),
                pltpu.VMEM((n_ep, top_k, tok_dev), jnp.int32),
                pltpu.VMEM((n_ep, top_k, tok_dev), jnp.int32),
                pltpu.VMEM((n_ep, top_k, tok_dev), f32),
                pltpu.VMEM((1, n_ep * seq_dev), jnp.int32),
                pltpu.SMEM((1, n_ep * seq_dev), jnp.int32),
                pltpu.SMEM((1, n_ep * seq_dev), jnp.int32),
                pltpu.VMEM((tok_dev, 128), f32),
                pltpu.VMEM((3 * tok_dev // 2, CORES * n_loc * slot_pad), bf16),
                ringbuf(n_half), ringbuf(n_half), ringbuf(2), ringbuf(n_half), ringbuf(n_half), ringbuf(n_half), ringbuf(3),
                pltpu.VMEM((n_half, CORES, 2, seq_len, half), bf16),
                pltpu.VMEM((n_ep, seq_len, model_dim), bf16),
                pltpu.VMEM((1, model_dim), f32),
                square, square, square, square,
                pltpu.VMEM((2 * seq_len, model_dim), bf16),
                pltpu.VMEM((2 * seq_len, model_dim), bf16),
                dma((n_ep,)), dma((n_ep,)), dma((n_ep,)),
                dma, dma, dma,
                dma((3,)), dma((3, n_ep - 1)), dma((3, n_ep)),
                dma, dma, dma,
                dma((2, n_half)), dma((2, n_half)), dma((2, n_half, n_sub)),
                dma((2, n_half)), dma((2, n_half)), dma((2, n_half, n_sub)),
                dma((n_half, CORES, n_sub // CORES)), dma((CORES, n_half, n_sub // CORES)), dma((4, n_half)), dma((CORES,)), dma, dma,
            ],
            compiler_params=pltpu.CompilerParams(collective_id=0, has_side_effects=True, vmem_limit_bytes=67043328),
            name='stage',
        )(owner, expert_id[0, 0].T, slot_id[0, 0].T, gate[0, 0].T, expert_out[0, 0], resid[0, 0],
          norm_w, w_q[0], w_k[0], w_v[0], w_o[0])
        return z_owned.reshape(1, 1, tok_dev, model_dim)

    tok_spec = P(group_axes, None, 'ep', None)
    weight_spec = P('pp', None, None)
    in_specs = (P(group_axes, None, 'ep', None, None), tok_spec, tok_spec, tok_spec, tok_spec, P(group_axes, None), P('pp', None), weight_spec, weight_spec, weight_spec, weight_spec)
    return jax.shard_map(device_step, mesh=mesh, in_specs=in_specs, out_specs=tok_spec, check_vma=False)
```
